32 devices in a mesh: gx: 4 (over y, x), gy: 2 (over core), gz: 4 (over z).
Axes of the slice: x: 2, y: 2, z: 4, core: 2. Of those that a mesh axis runs over, the one named last changes fastest.
Arguments:
- spectrum: float32 [3, 2, 16, 16, 2048], P(None, None, ('gy', 'gx'), None, 'gz'), may hold values from -0.3125 to 0.3125
- theta: float32 [16, 16, 8192], P('gy', 'gz', 'gx'), may hold values from -6 to 6
- section_sum: float32 [16, 16, 8192], P('gy', 'gz', 'gx'), may hold values from -6 to 6
- seg_offset: int32 [4], replicated, may hold values from 0 to 2560, as said below
- seg_length: int32 [4], replicated, may hold values from 512 to 1536, as said below
- stencil_index: int32 [8, 8192], replicated, may hold values from 0 to 1535, as said below
- stencil_weight: float32 [8, 8192], replicated, may hold values from 0 to 0.25
Outputs:
- theta_next: float32 [16, 16, 8192], P('gy', 'gz', 'gx')
- section_next: float32 [16, 16, 8192], P('gy', 'gz', 'gx')
The draws below stay inside these ranges and needn't reach their ends.
Inputs may be any that keep to these rules, and one draw needn't show every extreme that they name: `seg_length`: some block's segment holds exactly 1536 cells. For every block i, seg_offset[i] + 1536 <= 4096. `stencil_index`: positions count from the start of the segment of the scalar cell's x block; taps at or past that segment's length are padding.
All inputs are finite; a program needn't handle non-finite values.
Results may differ from the reference program's by a relative error of at most 0.00005.
Values sent between devices are 32-bit elements; how exact they have to be, the bound alone decides.
A program may use at most 64 MiB of HBM per device.

```python
import jax
import jax.numpy as jnp
from jax import lax

TAPS = 8
NVX = 4096
K = 2048
NSX = 8192
NSY = 16
NSZ = 16
MAXSEG = 1536
N_GX = 4


def segments_drawn(key):
    base_key = jax.random.fold_in(key, 7)
    length_key, longest_key = jax.random.split(base_key)
    lengths = jax.random.randint(length_key, (N_GX,), MAXSEG // 3, MAXSEG + 1, dtype=jnp.int32)
    longest = jax.random.randint(longest_key, (), 0, N_GX, dtype=jnp.int32)
    block_number = jnp.arange(N_GX, dtype=jnp.int32)
    lengths = jnp.where(block_number == longest, MAXSEG, lengths)
    centers = block_number * (NVX // N_GX) + NVX // (2 * N_GX)
    offsets = jnp.clip(centers - lengths // 2, 0, NVX - MAXSEG)
    return (offsets.astype(jnp.int32), lengths.astype(jnp.int32))


def draw_seg_offset(key, part):
    return segments_drawn(key)[0]


def draw_seg_length(key, part):
    return segments_drawn(key)[1]


def draw_stencil_index(key, part):
    offsets, lengths = segments_drawn(key)
    block_cells = NSX // N_GX
    cell_index = jnp.arange(NSX, dtype=jnp.int32)
    within = cell_index % block_cells
    owner_block = cell_index // block_cells
    owner_length = jnp.sum(jnp.where(owner_block[:, None] == jnp.arange(N_GX, dtype=jnp.int32)[None, :], lengths[None, :], 0), axis=1)
    jitter = jax.random.randint(jax.random.fold_in(key, 13), (NSX,), 0, 3, dtype=jnp.int32)
    anchor = within * owner_length // block_cells + jitter
    tap_shift = jnp.arange(TAPS, dtype=jnp.int32)[:, None] - TAPS // 2 + 1
    return jnp.clip(anchor[None, :] + tap_shift, 0, MAXSEG - 1).astype(jnp.int32)


def level_of(rng, extent, shards, least, top_value):
    def one(position, shards_of):
        heights = jax.random.uniform(jax.random.fold_in(jax.random.fold_in(rng, 6), position), (shards_of,), jnp.float32, least / len(shards), top_value / len(shards))
        return jnp.repeat(jnp.exp(heights), extent[position] // shards_of).reshape((-1,) + (1,) * (len(extent) - position - 1))

    factor_of = one(*shards[0])
    for cut in shards[1:]:
        factor_of = factor_of * one(*cut)
    return factor_of


def scatter_about(rng, extent, spread, most, cuts=(), kind=jnp.bfloat16):
    entries = jax.random.normal(rng, extent, jnp.float32) * spread
    if len(cuts) > 0:
        entries = level_of(rng, extent, cuts, -0.22, 0.18) * entries
    return jnp.clip(entries, min=-most, max=most).astype(kind)


def setup_inputs(seed: int = 0) -> dict:
    seeds = jax.random.split(jax.random.key(seed), 8)
    return {
        "spectrum": scatter_about(seeds[0], (3, 2, NSY, NSZ, K), ((2.0 / NVX) ** 0.5), 0.3125, ((2, 8), (4, 4)), jnp.float32),
        "theta": scatter_about(seeds[1], (NSY, NSZ, NSX), 1.0, 6.0, ((0, 2), (1, 4), (2, 4)), jnp.float32),
        "section_sum": scatter_about(seeds[2], (NSY, NSZ, NSX), 0.5, 6.0, ((0, 2), (1, 4), (2, 4)), jnp.float32),
        "seg_offset": draw_seg_offset(jax.random.fold_in(seeds[7], 71), 0),
        "seg_length": draw_seg_length(jax.random.fold_in(seeds[7], 71), 0),
        "stencil_index": draw_stencil_index(jax.random.fold_in(seeds[7], 71), 0),
        "stencil_weight": jnp.clip(jax.random.uniform(seeds[6], (TAPS, NSX), jnp.float32, 0.0, 0.25), 0.0, 0.25),
    }


first_coeffs = (0.8, -0.2, 4.0 / 105.0, -1.0 / 280.0)
second_coeffs = (1.6, -0.2, 8.0 / 315.0, -1.0 / 560.0)
center_coeff = -205.0 / 72.0
diffusivity = 0.15
time_step = 0.4
section_keep = -5.0 / 9.0
section_gain = 15.0 / 16.0


def reference(spectrum, theta, section_sum, seg_offset, seg_length, stencil_index, stencil_weight):
    line_length = 2 * spectrum.shape[-1]
    scalar_cells = theta.shape[2]
    block_cells = scalar_cells // N_GX
    block_of = (jnp.arange(scalar_cells, dtype=jnp.int32) // block_cells).astype(jnp.int32)
    start_of = seg_offset[block_of]
    length_of = seg_length[block_of]
    absolute = (start_of[None, :] + stencil_index).astype(jnp.int32)
    live_weight = jnp.where(stencil_index < length_of[None, :], stencil_weight, 0.0)
    theta_cycle = jnp.concatenate([theta[-4:], theta, theta[:4]], axis=0)

    def one_row(row_index):
        coeffs = spectrum[:, 0, row_index] + 1j * spectrum[:, 1, row_index]
        velocity = line_length * jnp.real(jnp.fft.ifft(coeffs, n=line_length, axis=-1))
        carried = jnp.zeros((3, theta.shape[1], scalar_cells), jnp.float32)
        for tap_number in range(stencil_index.shape[0]):
            carried = carried + live_weight[tap_number] * jnp.take(velocity, absolute[tap_number], axis=-1)
        slab = lax.dynamic_slice_in_dim(theta_cycle, row_index, 9, 0)
        center = slab[4]
        grad_x = jnp.zeros_like(center)
        grad_y = jnp.zeros_like(center)
        grad_z = jnp.zeros_like(center)
        laplace = 3.0 * center_coeff * center
        for reach in range(1, 5):
            ahead_x = jnp.roll(center, -reach, axis=1)
            behind_x = jnp.roll(center, reach, axis=1)
            ahead_z = jnp.roll(center, -reach, axis=0)
            behind_z = jnp.roll(center, reach, axis=0)
            ahead_y = slab[4 + reach]
            behind_y = slab[4 - reach]
            first = first_coeffs[reach - 1]
            second = second_coeffs[reach - 1]
            grad_x = grad_x + first * (ahead_x - behind_x)
            grad_y = grad_y + first * (ahead_y - behind_y)
            grad_z = grad_z + first * (ahead_z - behind_z)
            laplace = laplace + second * (ahead_x + behind_x + ahead_y + behind_y + ahead_z + behind_z)
        change = -(carried[0] * grad_x + carried[1] * grad_y + carried[2] * grad_z) + diffusivity * laplace
        register = lax.dynamic_index_in_dim(section_sum, row_index, 0, keepdims=False)
        section_next = section_keep * register + time_step * change
        return center + section_gain * section_next, section_next

    theta_next, section_next = lax.map(one_row, jnp.arange(theta.shape[0], dtype=jnp.int32))
    return theta_next, section_next
```

```python
import functools
import math

import jax
import jax.numpy as jnp
import numpy as np
from jax import lax
from jax.experimental import pallas as pl
from jax.experimental.pallas import tpu as pltpu
from jax.sharding import PartitionSpec as P

MESH = pl.DeviceIdType.MESH
VMEM = pltpu.VMEM
LANES = 128
HALO = 4
TILE = 8
WIDTH = 512

first_coeffs = (0.8, -0.2, 4.0 / 105.0, -1.0 / 280.0)
second_coeffs = (1.6, -0.2, 8.0 / 315.0, -1.0 / 560.0)
center_coeff = -205.0 / 72.0
diffusivity = 0.15
time_step = 0.4
section_keep = -5.0 / 9.0
section_gain = 15.0 / 16.0


def whole_vmem(count):
    return [pl.BlockSpec(memory_space=VMEM)] * count


def rotate(value, turn):
    re, im = value
    cosine, sine = math.cos(2 * math.pi * turn), math.sin(2 * math.pi * turn)
    quarter = turn * 4 % 4
    if quarter == 0:
        return re, im
    if quarter == 1:
        return -im, re
    if quarter == 2:
        return -re, -im
    if quarter == 3:
        return im, -re
    return re * cosine - im * sine, re * sine + im * cosine


def fft(values):
    count = len(values)
    if count == 1:
        return values
    even = fft(values[0::2])
    odd = fft(values[1::2])
    low, high = [], []
    for x in range(count // 2):
        re, im = rotate(odd[x], x / count)
        low.append((even[x][0] + re, even[x][1] + im))
        high.append((even[x][0] - re, even[x][1] - im))
    return low + high


def split(value):
    top = value.astype(jnp.bfloat16)
    return top, (value - top.astype(jnp.float32)).astype(jnp.bfloat16)


def section_kernel(
    sizes, span,
    offset_ref, length_ref, spec_hbm, theta_hbm, sum_hbm, index_hbm, weight_hbm, twist_hbm, last_hbm,
    theta_out, sum_out,
    spec_ref, theta_ref, sum_ref, index_ref, weight_ref, twist_ref, last_ref,
    modes_send, modes_recv, mixed, velocity, seg_send, seg_recv, matrix_top, matrix_rest, gathered, values,
    grads, part, drift, field, z_back, z_front,
    load_sems, modes_sems, seg_sems, face_sems, deep_sems,
):
    gx, gy, gz = sizes
    here = {axis: lax.axis_index(axis) for axis in ("gx", "gy", "gz")}
    counts = dict(gx=gx, gy=gy, gz=gz)
    ahead = {axis: {axis: lax.rem(here[axis] + 1, counts[axis])} for axis in here}
    behind = {axis: {axis: lax.rem(here[axis] + counts[axis] - 1, counts[axis])} for axis in here}
    me, layer = here["gx"], here["gz"]
    rows, depth, cells = theta_ref.shape
    _, _, own_rows, all_depth, modes = spec_ref.shape
    local_slabs = modes // LANES
    group = own_rows * depth
    slabs = gz * local_slabs
    near = 2 * slabs
    far = 2 * slabs
    taps = index_ref.shape[0]
    lines = rows * depth
    tiles = lines // TILE
    skirt = HALO * depth

    own_columns = pl.ds(pl.multiple_of(me * cells, LANES), cells)
    loads = [
        pltpu.make_async_copy(source, place, load_sems.at[number])
        for number, (source, place) in enumerate(
            [
                (spec_hbm, spec_ref),
                (theta_hbm, theta_ref),
                (index_hbm.at[:, own_columns], index_ref),
                (weight_hbm.at[:, own_columns], weight_ref),
                (twist_hbm, twist_ref),
                (last_hbm, last_ref),
                (sum_hbm, sum_ref),
            ]
        )
    ]
    for load in loads:
        load.start()

    barrier = pltpu.get_barrier_semaphore()
    targets = [{"gx": lax.rem(me + step, gx)} for step in range(1, gx)]
    targets += [{"gz": lax.rem(layer + step, gz)} for step in range(1, gz)]
    targets += [ahead["gy"], behind["gy"]]
    for target in targets:
        pl.semaphore_signal(barrier, inc=1, device_id=target, device_id_type=MESH)

    loads[0].wait()
    for comp in range(3):
        for slab in range(local_slabs):
            for part_of in range(2):
                for row in range(own_rows):
                    held = spec_ref[comp, part_of, row, :, slab * LANES : (slab + 1) * LANES]
                    at = part_of * group + row * depth
                    for peer in range(gz):
                        modes_send[comp, peer, slab, at : at + depth, :] = held[
                            peer * depth : (peer + 1) * depth
                        ]
    pl.semaphore_wait(barrier, len(targets))

    def modes_copy(comp, target):
        return pltpu.make_async_remote_copy(
            src_ref=modes_send.at[comp, target],
            dst_ref=modes_recv.at[comp, layer],
            send_sem=modes_sems.at[0, comp, target],
            recv_sem=modes_sems.at[1, comp, layer],
            device_id={"gz": target},
            device_id_type=MESH,
        )

    def modes_wait(comp, other):
        pltpu.make_async_remote_copy(
            src_ref=modes_send.at[comp, other],
            dst_ref=modes_recv.at[comp, other],
            send_sem=modes_sems.at[0, comp, other],
            recv_sem=modes_sems.at[1, comp, other],
            device_id={"gz": other},
            device_id_type=MESH,
        ).wait()

    def send_modes(comp, distance):
        @pl.when(layer + distance < gz)
        def _():
            modes_copy(comp, layer + distance).start()

        @pl.when(layer >= distance)
        def _():
            modes_copy(comp, layer - distance).start()

    for comp in range(3):
        send_modes(comp, 1)
    for comp in range(3):
        for distance in range(2, gz):
            send_modes(comp, distance)

    def seg_copy(comp, step):
        target = lax.rem(me + step, gx)
        return pltpu.make_async_remote_copy(
            src_ref=seg_send.at[comp, target],
            dst_ref=seg_recv.at[comp, me],
            send_sem=seg_sems.at[0, comp, step - 1],
            recv_sem=seg_sems.at[1, comp, step - 1],
            device_id={"gx": target},
            device_id_type=MESH,
        )

    loads[1].wait()
    for tile in range(tiles):
        at = skirt + tile * TILE
        for half in range(TILE // depth):
            field[at + half * depth : at + (half + 1) * depth, LANES : LANES + cells] = theta_ref[
                tile * (TILE // depth) + half
            ]

    mine = pl.ds(skirt, lines)
    middle = pl.ds(LANES, cells)
    faces = [
        pltpu.make_async_remote_copy(
            src_ref=field.at[source],
            dst_ref=field.at[place],
            send_sem=face_sems.at[0, number],
            recv_sem=face_sems.at[1, number],
            device_id=device,
            device_id_type=MESH,
        )
        for number, (source, place, device) in enumerate(
            [
                ((mine, pl.ds(cells, LANES)), (mine, pl.ds(0, LANES)), ahead["gx"]),
                ((mine, pl.ds(LANES, LANES)), (mine, pl.ds(LANES + cells, LANES)), behind["gx"]),
                ((pl.ds(lines, skirt), middle), (pl.ds(0, skirt), middle), ahead["gy"]),
                ((pl.ds(skirt, skirt), middle), (pl.ds(skirt + lines, skirt), middle), behind["gy"]),
            ]
        )
    ]
    for face in faces:
        face.start()

    def deep_copy(way, tile):
        return pltpu.make_async_remote_copy(
            src_ref=field.at[pl.ds(skirt + tile * TILE, TILE), middle],
            dst_ref=(z_back, z_front)[way].at[pl.ds(tile * TILE, TILE)],
            send_sem=deep_sems.at[0, way, tile],
            recv_sem=deep_sems.at[1, way, tile],
            device_id=(ahead, behind)[way]["gz"],
            device_id_type=MESH,
        )

    for comp in range(3):
        modes_recv[comp, layer] = modes_send[comp, layer]

    loads[2].wait()
    loads[3].wait()
    live_count = length_ref[me]
    begin = offset_ref[me] - jnp.minimum(offset_ref[me] // LANES, far - span) * LANES
    counter = lax.broadcasted_iota(jnp.int32, (LANES, LANES), 0).astype(jnp.float32).astype(jnp.bfloat16)
    counters = [counter[step : step + 16] for step in range(0, LANES, 16)]

    def spread(row):
        return jnp.broadcast_to(row, (16, LANES)).astype(jnp.bfloat16)

    def build(chunk, carry):
        columns = pl.ds(pl.multiple_of(chunk * LANES, LANES), LANES)
        index = index_ref[:, columns]
        live = index < live_count
        weight = jnp.where(live, weight_ref[:, columns], 0.0)
        merged = jnp.zeros_like(weight)
        for tap in range(taps):
            merged = merged + jnp.where(index == index[tap : tap + 1], weight[tap : tap + 1], 0.0)
        high, low = split(merged)
        high, low = high.astype(jnp.float32), low.astype(jnp.float32)
        place = jnp.where(live, index + begin, -1)
        owner = (place >> 7).astype(jnp.float32)
        within = (place & (LANES - 1)).astype(jnp.float32)
        tops = [spread(high[tap : tap + 1]) for tap in range(taps)]
        rests = [spread(low[tap : tap + 1]) for tap in range(taps)]
        owners = [spread(owner[tap : tap + 1]) for tap in range(taps)]
        withins = [spread(within[tap : tap + 1]) for tap in range(taps)]

        def slab_of(slab, inner):
            number = jnp.full((16, LANES), slab, jnp.int32).astype(jnp.float32).astype(jnp.bfloat16)
            close = [
                jnp.where(owners[tap] == number, withins[tap], jnp.bfloat16(-1)) for tap in range(taps)
            ]
            for step in range(LANES // 16):
                top = jnp.zeros((16, LANES), jnp.bfloat16)
                rest = jnp.zeros((16, LANES), jnp.bfloat16)
                for tap in range(taps):
                    hit = counters[step] == close[tap]
                    top = jnp.where(hit, tops[tap], top)
                    rest = jnp.where(hit, rests[tap], rest)
                at = pl.ds(pl.multiple_of(slab * LANES + step * 16, 16), 16)
                matrix_top[chunk, at, :] = top
                matrix_rest[chunk, at, :] = rest
            return inner

        return lax.fori_loop(0, span, slab_of, carry)

    lax.fori_loop(0, cells // LANES, build, 0)

    @pl.when(layer == gz - 1)
    def _():
        for way in (1, 0):
            for tile in range(tiles):
                deep_copy(way, tile).start()

    @pl.when(layer != gz - 1)
    def _():
        for way in (0, 1):
            for tile in range(tiles):
                deep_copy(way, tile).start()

    loads[4].wait()
    loads[5].wait()
    last_both = last_ref[...]
    last_top = last_both[:far]
    dims = (((1,), (1,)), ((), ()))

    def twisted(line):
        re, im = mixed[:, line, :], mixed[:, group + line, :]
        pieces = []
        for quarter in range(LANES // near):
            part_of = slice(quarter * near, (quarter + 1) * near)
            cosine, sine = twist_ref[0, part_of, :], twist_ref[1, part_of, :]
            pieces.append(jnp.concatenate([re * cosine - im * sine, re * sine + im * cosine], axis=1))
        return jnp.concatenate(pieces, axis=0)

    def transform(comp, carry):
        for step in range(1, gz):
            modes_wait(comp, lax.rem(layer + step, gz))

        def arrived(k):
            held = modes_recv[comp, k // local_slabs, k % local_slabs]
            return held[:group], held[group:]

        for parity in range(2):
            mixes = fft([rotate(arrived(k), parity * k / near) for k in range(slabs)])
            for x in range(slabs):
                mixed[2 * x + parity, 0:group, :] = mixes[x][0]
                mixed[2 * x + parity, group:, :] = mixes[x][1]
        for pair in range(group // 2):
            turned = jnp.concatenate([twisted(2 * pair), twisted(2 * pair + 1)], axis=0)
            top, rest = split(turned)
            first = lax.dot_general(last_both, top, dims, preferred_element_type=jnp.float32)
            second = lax.dot_general(last_top, rest, dims, preferred_element_type=jnp.float32)
            total = first[:far] + (first[far:] + second)
            velocity[:, 2 * pair, :] = total[:, :LANES]
            velocity[:, 2 * pair + 1, :] = total[:, LANES:]
        for block in range(gx):
            start = jnp.minimum(offset_ref[block] // LANES, far - span)
            seg_send[comp, block] = velocity[pl.ds(start, span)]
        for step in range(1, gx):
            seg_copy(comp, step).start()
        seg_recv[comp, me] = seg_send[comp, me]
        return carry

    lax.fori_loop(0, 3, transform, 0)

    loads[6].wait()
    for tile in range(tiles):
        for half in range(TILE // depth):
            at = tile * TILE + half * depth
            part[at : at + depth, :] = section_keep * sum_ref[tile * (TILE // depth) + half]
    for face in faces:
        face.wait()
    width = min(WIDTH, cells)
    wide_width = width + 2 * LANES
    low_half = lax.broadcasted_iota(jnp.int32, (TILE, width), 0) < depth

    def plane(block, carry):
        columns = pl.ds(pl.multiple_of(block * width, LANES), width)
        inner = pl.ds(pl.multiple_of(block * width + LANES, LANES), width)
        around = pl.ds(pl.multiple_of(block * width, LANES), wide_width)
        for tile in range(tiles):
            stack = [field[(tile + step) * TILE : (tile + step + 1) * TILE, inner] for step in range(5)]
            turned = [pltpu.roll(held, depth, 0) for held in stack]
            between = [jnp.where(low_half, turned[step], turned[step + 1]) for step in range(4)]
            behind_y = [between[1], stack[1], between[0], stack[0]]
            ahead_y = [between[2], stack[3], between[3], stack[4]]
            wide = field[skirt + tile * TILE : skirt + (tile + 1) * TILE, around]
            grad_x = jnp.zeros((TILE, width), jnp.float32)
            grad_y = jnp.zeros((TILE, width), jnp.float32)
            partial = 3.0 * center_coeff * stack[2]
            for reach in range(1, 5):
                ahead_x = pltpu.roll(wide, wide_width - reach, 1)[:, LANES : LANES + width]
                behind_x = pltpu.roll(wide, reach, 1)[:, LANES : LANES + width]
                up, down = ahead_y[reach - 1], behind_y[reach - 1]
                grad_x = grad_x + first_coeffs[reach - 1] * (ahead_x - behind_x)
                grad_y = grad_y + first_coeffs[reach - 1] * (up - down)
                partial = partial + second_coeffs[reach - 1] * ((ahead_x + behind_x) + (up + down))
            at = slice(tile * TILE, (tile + 1) * TILE)
            grads[0, at, columns] = grad_x
            grads[1, at, columns] = grad_y
            part[at, columns] = part[at, columns] + (time_step * diffusivity) * partial
        return carry

    lax.fori_loop(0, cells // width, plane, 0)

    for comp in range(3):
        for step in range(1, gx):
            seg_copy(comp, step).wait()
    for comp in range(3):
        for block in range(gx):
            at = (comp * gx + block) * group
            for slab in range(span):
                gathered[at : at + group, slab * LANES : (slab + 1) * LANES] = seg_recv[comp, block, slab]
    total = 3 * lines
    top, rest = split(gathered[...])
    values[0:total, :] = top
    values[total:, :] = rest

    def combine(pair, carry):
        top = jnp.concatenate([matrix_top[2 * pair], matrix_top[2 * pair + 1]], axis=1)
        rest = jnp.concatenate([matrix_rest[2 * pair], matrix_rest[2 * pair + 1]], axis=1)
        first = jnp.dot(values[...], top, preferred_element_type=jnp.float32)
        second = jnp.dot(values[0:total, :], rest, preferred_element_type=jnp.float32)
        moved = first[:total] + (first[total:] + second)
        columns = pl.ds(pl.multiple_of(pair * 2 * LANES, 2 * LANES), 2 * LANES)
        carried = moved[:lines] * grads[0, :, columns] + moved[lines : 2 * lines] * grads[1, :, columns]
        part[:, columns] = part[:, columns] - time_step * carried
        drift[:, columns] = time_step * moved[2 * lines :]
        return carry

    lax.fori_loop(0, cells // (2 * LANES), combine, 0)

    place_of = lax.rem(lax.broadcasted_iota(jnp.int32, (TILE, width), 0), depth)
    for tile in range(tiles):
        for way in range(2):
            deep_copy(way, tile).wait()
        at = slice(tile * TILE, (tile + 1) * TILE)

        def finish(block, carry):
            columns = pl.ds(pl.multiple_of(block * width, LANES), width)
            inner = pl.ds(pl.multiple_of(block * width + LANES, LANES), width)
            own = field[skirt + tile * TILE : skirt + (tile + 1) * TILE, inner]
            back, front = z_back[at, columns], z_front[at, columns]
            grad_z = jnp.zeros((TILE, width), jnp.float32)
            partial = jnp.zeros((TILE, width), jnp.float32)
            for reach in range(1, 5):
                up, down = front, back
                if reach < HALO:
                    up = jnp.where(
                        place_of < depth - reach, pltpu.roll(own, TILE - reach, 0), pltpu.roll(front, depth - reach, 0)
                    )
                    down = jnp.where(
                        place_of >= reach, pltpu.roll(own, reach, 0), pltpu.roll(back, depth + reach, 0)
                    )
                grad_z = grad_z + first_coeffs[reach - 1] * (up - down)
                partial = partial + second_coeffs[reach - 1] * (up + down)
            after = (part[at, columns] + (time_step * diffusivity) * partial) - drift[at, columns] * grad_z
            later = own + section_gain * after
            for half in range(TILE // depth):
                row, piece = tile * (TILE // depth) + half, slice(half * depth, (half + 1) * depth)
                sum_out[row, :, columns] = after[piece]
                theta_out[row, :, columns] = later[piece]
            return carry

        lax.fori_loop(0, cells // width, finish, 0)


def put(theta_ref, sum_ref, theta_out, sum_out, sems):
    copies = [
        pltpu.make_async_copy(theta_ref, theta_out, sems.at[0]),
        pltpu.make_async_copy(sum_ref, sum_out, sems.at[1]),
    ]
    for copy in copies:
        copy.start()
    for copy in copies:
        copy.wait()


def body(spectrum, theta, section_sum, seg_offset, seg_length, stencil_index, stencil_weight):
    sizes = tuple(lax.axis_size(axis) for axis in ("gx", "gy", "gz"))
    gx, _, gz = sizes
    _, _, own_rows, all_depth, modes = spectrum.shape
    rows, depth, cells = theta.shape
    taps = stencil_index.shape[0]
    assert depth == HALO and rows * depth % TILE == 0 and cells % min(WIDTH, cells) == 0
    group = own_rows * depth
    slabs = gz * modes // LANES
    length = 2 * slabs * LANES
    far = length // LANES
    span = min(3 * length // (2 * gx) // LANES + 1, far)
    k = np.arange(LANES)
    turn = 2 * np.pi * (np.outer(k, k) % length) / length
    twist = np.stack([np.cos(turn), np.sin(turn)]).astype(np.float32)
    turn = 2 * np.pi * (np.outer(np.arange(far), k) % far) / far
    last = np.concatenate([np.cos(turn), -np.sin(turn)], axis=1).astype(np.float32)
    top = last.astype(jnp.bfloat16)
    rest = (last - top.astype(np.float32)).astype(jnp.bfloat16)
    modes_shape = (3, gz, modes // LANES, 2 * group, LANES)
    seg_shape = (3, gx, span, group, LANES)
    lines = rows * depth
    tiles = lines // TILE
    single = jnp.float32
    held = pl.pallas_call(
        functools.partial(section_kernel, sizes, span),
        out_shape=[VMEM(theta.shape, single)] * 2,
        in_specs=[pl.BlockSpec(memory_space=pltpu.SMEM)] * 2 + [pl.BlockSpec(memory_space=pltpu.HBM)] * 7,
        out_specs=whole_vmem(2),
        scratch_shapes=[
            VMEM(spectrum.shape, single),
            VMEM(theta.shape, single),
            VMEM(theta.shape, single),
            VMEM((taps, cells), jnp.int32),
            VMEM((taps, cells), single),
            VMEM(twist.shape, single),
            VMEM((2 * far, 2 * LANES), jnp.bfloat16),
            VMEM(modes_shape, single),
            VMEM(modes_shape, single),
            VMEM((2 * slabs, 2 * group, LANES), single),
            VMEM((far, group, LANES), single),
            VMEM(seg_shape, single),
            VMEM(seg_shape, single),
            VMEM((cells // LANES, span * LANES, LANES), jnp.bfloat16),
            VMEM((cells // LANES, span * LANES, LANES), jnp.bfloat16),
            VMEM((3 * lines, span * LANES), single),
            VMEM((6 * lines, span * LANES), jnp.bfloat16),
            VMEM((2, lines, cells), single),
            VMEM((lines, cells), single),
            VMEM((lines, cells), single),
            VMEM((lines + 2 * HALO * depth, cells + 2 * LANES), single),
            VMEM((lines, cells), single),
            VMEM((lines, cells), single),
            pltpu.SemaphoreType.DMA((7,)),
            pltpu.SemaphoreType.DMA((2, 3, gz)),
            pltpu.SemaphoreType.DMA((2, 3, gx - 1)),
            pltpu.SemaphoreType.DMA((2, 4)),
            pltpu.SemaphoreType.DMA((2, 2, tiles)),
        ],
        compiler_params=pltpu.CompilerParams(
            collective_id=0, has_side_effects=True, vmem_limit_bytes=40 * 1024 * 1024
        ),
        name="section",
    )(
        seg_offset, seg_length, spectrum, theta, section_sum, stencil_index, stencil_weight,
        jnp.asarray(twist), jnp.asarray(np.concatenate([top, rest], axis=0)),
    )
    return tuple(
        pl.pallas_call(
            put,
            out_shape=[jax.ShapeDtypeStruct(theta.shape, single)] * 2,
            in_specs=whole_vmem(2),
            out_specs=[pl.BlockSpec(memory_space=pltpu.HBM)] * 2,
            scratch_shapes=[pltpu.SemaphoreType.DMA((2,))],
            name="put",
        )(*held)
    )


def solution(mesh):
    placed = (
        P(None, None, ("gy", "gx"), None, "gz"),
        P("gy", "gz", "gx"),
        P("gy", "gz", "gx"),
        P(),
        P(),
        P(),
        P(),
    )
    return jax.shard_map(
        body,
        mesh=mesh,
        in_specs=placed,
        out_specs=(P("gy", "gz", "gx"), P("gy", "gz", "gx")),
        check_vma=False,
    )
```

```python
import functools
import math

import jax
import jax.numpy as jnp
import numpy as np
from jax import lax
from jax.experimental import pallas as pl
from jax.experimental.pallas import tpu as pltpu
from jax.sharding import PartitionSpec as P

MESH = pl.DeviceIdType.MESH
VMEM = pltpu.VMEM
LANES = 128
HALO = 4
TILE = 8
WIDTH = 512

first_coeffs = (0.8, -0.2, 4.0 / 105.0, -1.0 / 280.0)
second_coeffs = (1.6, -0.2, 8.0 / 315.0, -1.0 / 560.0)
center_coeff = -205.0 / 72.0
diffusivity = 0.15
time_step = 0.4
section_keep = -5.0 / 9.0
section_gain = 15.0 / 16.0


def whole_vmem(count):
    return [pl.BlockSpec(memory_space=VMEM)] * count


def rotate(value, turn):
    re, im = value
    cosine, sine = math.cos(2 * math.pi * turn), math.sin(2 * math.pi * turn)
    quarter = turn * 4 % 4
    if quarter == 0:
        return re, im
    if quarter == 1:
        return -im, re
    if quarter == 2:
        return -re, -im
    if quarter == 3:
        return im, -re
    return re * cosine - im * sine, re * sine + im * cosine


def fft(values):
    count = len(values)
    if count == 1:
        return values
    even = fft(values[0::2])
    odd = fft(values[1::2])
    low, high = [], []
    for x in range(count // 2):
        re, im = rotate(odd[x], x / count)
        low.append((even[x][0] + re, even[x][1] + im))
        high.append((even[x][0] - re, even[x][1] - im))
    return low + high


def split(value):
    top = value.astype(jnp.bfloat16)
    return top, (value - top.astype(jnp.float32)).astype(jnp.bfloat16)


def section_kernel(
    sizes, span,
    offset_ref, length_ref, spec_hbm, theta_hbm, sum_hbm, index_hbm, weight_hbm, twist_hbm, last_hbm,
    theta_out, sum_out,
    spec_ref, theta_ref, sum_ref, index_ref, weight_ref, twist_ref, last_ref,
    modes_send, modes_recv, mixed, velocity, seg_send, seg_recv, matrix_top, matrix_rest, gathered, values,
    grads, part, drift, field, z_back, z_front,
    load_sems, modes_sems, seg_sems, face_sems, deep_sems,
):
    gx, gy, gz = sizes
    here = {axis: lax.axis_index(axis) for axis in ("gx", "gy", "gz")}
    counts = dict(gx=gx, gy=gy, gz=gz)
    ahead = {axis: {axis: lax.rem(here[axis] + 1, counts[axis])} for axis in here}
    behind = {axis: {axis: lax.rem(here[axis] + counts[axis] - 1, counts[axis])} for axis in here}
    me, layer = here["gx"], here["gz"]
    rows, depth, cells = theta_ref.shape
    _, _, own_rows, all_depth, modes = spec_ref.shape
    local_slabs = modes // LANES
    group = own_rows * depth
    slabs = gz * local_slabs
    near = 2 * slabs
    far = 2 * slabs
    taps = index_ref.shape[0]
    lines = rows * depth
    tiles = lines // TILE
    skirt = HALO * depth

    own_columns = pl.ds(pl.multiple_of(me * cells, LANES), cells)
    loads = [
        pltpu.make_async_copy(source, place, load_sems.at[number])
        for number, (source, place) in enumerate(
            [
                (spec_hbm, spec_ref),
                (theta_hbm, theta_ref),
                (index_hbm.at[:, own_columns], index_ref),
                (weight_hbm.at[:, own_columns], weight_ref),
                (twist_hbm, twist_ref),
                (last_hbm, last_ref),
                (sum_hbm, sum_ref),
            ]
        )
    ]
    for load in loads:
        load.start()

    barrier = pltpu.get_barrier_semaphore()
    targets = [{"gx": lax.rem(me + step, gx)} for step in range(1, gx)]
    targets += [{"gz": lax.rem(layer + step, gz)} for step in range(1, gz)]
    targets += [ahead["gy"], behind["gy"]]
    for target in targets:
        pl.semaphore_signal(barrier, inc=1, device_id=target, device_id_type=MESH)

    loads[0].wait()
    for comp in range(3):
        for slab in range(local_slabs):
            for part_of in range(2):
                for row in range(own_rows):
                    held = spec_ref[comp, part_of, row, :, slab * LANES : (slab + 1) * LANES]
                    at = part_of * group + row * depth
                    for peer in range(gz):
                        modes_send[comp, peer, slab, at : at + depth, :] = held[
                            peer * depth : (peer + 1) * depth
                        ]
    pl.semaphore_wait(barrier, len(targets))

    def modes_copy(comp, target):
        return pltpu.make_async_remote_copy(
            src_ref=modes_send.at[comp, target],
            dst_ref=modes_recv.at[comp, layer],
            send_sem=modes_sems.at[0, comp, target],
            recv_sem=modes_sems.at[1, comp, layer],
            device_id={"gz": target},
            device_id_type=MESH,
        )

    def modes_wait(comp, other):
        pltpu.make_async_remote_copy(
            src_ref=modes_send.at[comp, other],
            dst_ref=modes_recv.at[comp, other],
            send_sem=modes_sems.at[0, comp, other],
            recv_sem=modes_sems.at[1, comp, other],
            device_id={"gz": other},
            device_id_type=MESH,
        ).wait()

    def send_modes(comp, distance):
        @pl.when(layer + distance < gz)
        def _():
            modes_copy(comp, layer + distance).start()

        @pl.when(layer >= distance)
        def _():
            modes_copy(comp, layer - distance).start()

    for comp in range(3):
        send_modes(comp, 1)
    for comp in range(3):
        for distance in range(2, gz):
            send_modes(comp, distance)

    def seg_copy(comp, step):
        target = lax.rem(me + step, gx)
        return pltpu.make_async_remote_copy(
            src_ref=seg_send.at[comp, target],
            dst_ref=seg_recv.at[comp, me],
            send_sem=seg_sems.at[0, comp, step - 1],
            recv_sem=seg_sems.at[1, comp, step - 1],
            device_id={"gx": target},
            device_id_type=MESH,
        )

    loads[1].wait()
    for tile in range(tiles):
        at = skirt + tile * TILE
        for half in range(TILE // depth):
            field[at + half * depth : at + (half + 1) * depth, LANES : LANES + cells] = theta_ref[
                tile * (TILE // depth) + half
            ]

    mine = pl.ds(skirt, lines)
    middle = pl.ds(LANES, cells)
    faces = [
        pltpu.make_async_remote_copy(
            src_ref=field.at[source],
            dst_ref=field.at[place],
            send_sem=face_sems.at[0, number],
            recv_sem=face_sems.at[1, number],
            device_id=device,
            device_id_type=MESH,
        )
        for number, (source, place, device) in enumerate(
            [
                ((mine, pl.ds(cells, LANES)), (mine, pl.ds(0, LANES)), ahead["gx"]),
                ((mine, pl.ds(LANES, LANES)), (mine, pl.ds(LANES + cells, LANES)), behind["gx"]),
                ((pl.ds(lines, skirt), middle), (pl.ds(0, skirt), middle), ahead["gy"]),
                ((pl.ds(skirt, skirt), middle), (pl.ds(skirt + lines, skirt), middle), behind["gy"]),
            ]
        )
    ]
    for face in faces:
        face.start()

    def deep_copy(way, tile):
        return pltpu.make_async_remote_copy(
            src_ref=field.at[pl.ds(skirt + tile * TILE, TILE), middle],
            dst_ref=(z_back, z_front)[way].at[pl.ds(tile * TILE, TILE)],
            send_sem=deep_sems.at[0, way, tile],
            recv_sem=deep_sems.at[1, way, tile],
            device_id=(ahead, behind)[way]["gz"],
            device_id_type=MESH,
        )

    for comp in range(3):
        modes_recv[comp, layer] = modes_send[comp, layer]

    loads[2].wait()
    loads[3].wait()
    live_count = length_ref[me]
    begin = offset_ref[me] - jnp.minimum(offset_ref[me] // LANES, far - span) * LANES
    counter = lax.broadcasted_iota(jnp.int32, (LANES, LANES), 0).astype(jnp.float32).astype(jnp.bfloat16)
    counters = [counter[step : step + 16] for step in range(0, LANES, 16)]

    def spread(row):
        return jnp.broadcast_to(row, (16, LANES)).astype(jnp.bfloat16)

    def build(chunk, carry):
        columns = pl.ds(pl.multiple_of(chunk * LANES, LANES), LANES)
        index = index_ref[:, columns]
        live = index < live_count
        weight = jnp.where(live, weight_ref[:, columns], 0.0)
        merged = jnp.zeros_like(weight)
        for tap in range(taps):
            merged = merged + jnp.where(index == index[tap : tap + 1], weight[tap : tap + 1], 0.0)
        high, low = split(merged)
        high, low = high.astype(jnp.float32), low.astype(jnp.float32)
        place = jnp.where(live, index + begin, -1)
        owner = (place >> 7).astype(jnp.float32)
        within = (place & (LANES - 1)).astype(jnp.float32)
        tops = [spread(high[tap : tap + 1]) for tap in range(taps)]
        rests = [spread(low[tap : tap + 1]) for tap in range(taps)]
        owners = [spread(owner[tap : tap + 1]) for tap in range(taps)]
        withins = [spread(within[tap : tap + 1]) for tap in range(taps)]

        def slab_of(slab, inner):
            number = jnp.full((16, LANES), slab, jnp.int32).astype(jnp.float32).astype(jnp.bfloat16)
            close = [
                jnp.where(owners[tap] == number, withins[tap], jnp.bfloat16(-1)) for tap in range(taps)
            ]
            for step in range(LANES // 16):
                top = jnp.zeros((16, LANES), jnp.bfloat16)
                rest = jnp.zeros((16, LANES), jnp.bfloat16)
                for tap in range(taps):
                    hit = counters[step] == close[tap]
                    top = jnp.where(hit, tops[tap], top)
                    rest = jnp.where(hit, rests[tap], rest)
                at = pl.ds(pl.multiple_of(slab * LANES + step * 16, 16), 16)
                matrix_top[chunk, at, :] = top
                matrix_rest[chunk, at, :] = rest
            return inner

        return lax.fori_loop(0, span, slab_of, carry)

    lax.fori_loop(0, cells // LANES, build, 0)

    @pl.when(layer == gz - 1)
    def _():
        for way in (1, 0):
            for tile in range(tiles):
                deep_copy(way, tile).start()

    @pl.when(layer != gz - 1)
    def _():
        for way in (0, 1):
            for tile in range(tiles):
                deep_copy(way, tile).start()

    loads[4].wait()
    loads[5].wait()
    last_both = last_ref[...]
    last_top = last_both[:far]
    dims = (((1,), (1,)), ((), ()))

    def twisted(line):
        re, im = mixed[:, line, :], mixed[:, group + line, :]
        pieces = []
        for quarter in range(LANES // near):
            part_of = slice(quarter * near, (quarter + 1) * near)
            cosine, sine = twist_ref[0, part_of, :], twist_ref[1, part_of, :]
            pieces.append(jnp.concatenate([re * cosine - im * sine, re * sine + im * cosine], axis=1))
        return jnp.concatenate(pieces, axis=0)

    def transform(comp, carry):
        for step in range(1, gz):
            modes_wait(comp, lax.rem(layer + step, gz))

        def arrived(k):
            held = modes_recv[comp, k // local_slabs, k % local_slabs]
            return held[:group], held[group:]

        for parity in range(2):
            mixes = fft([rotate(arrived(k), parity * k / near) for k in range(slabs)])
            for x in range(slabs):
                mixed[2 * x + parity, 0:group, :] = mixes[x][0]
                mixed[2 * x + parity, group:, :] = mixes[x][1]
        for pair in range(group // 2):
            turned = jnp.concatenate([twisted(2 * pair), twisted(2 * pair + 1)], axis=0)
            top, rest = split(turned)
            first = lax.dot_general(last_both, top, dims, preferred_element_type=jnp.float32)
            second = lax.dot_general(last_top, rest, dims, preferred_element_type=jnp.float32)
            total = first[:far] + (first[far:] + second)
            velocity[:, 2 * pair, :] = total[:, :LANES]
            velocity[:, 2 * pair + 1, :] = total[:, LANES:]
        for block in range(gx):
            start = jnp.minimum(offset_ref[block] // LANES, far - span)
            seg_send[comp, block] = velocity[pl.ds(start, span)]
        for step in range(1, gx):
            seg_copy(comp, step).start()
        seg_recv[comp, me] = seg_send[comp, me]
        return carry

    lax.fori_loop(0, 3, transform, 0)

    loads[6].wait()
    for tile in range(tiles):
        for half in range(TILE // depth):
            at = tile * TILE + half * depth
            part[at : at + depth, :] = section_keep * sum_ref[tile * (TILE // depth) + half]
    for face in faces:
        face.wait()
    width = min(WIDTH, cells)
    wide_width = width + 2 * LANES
    low_half = lax.broadcasted_iota(jnp.int32, (TILE, width), 0) < depth

    def plane(block, carry):
        columns = pl.ds(pl.multiple_of(block * width, LANES), width)
        inner = pl.ds(pl.multiple_of(block * width + LANES, LANES), width)
        around = pl.ds(pl.multiple_of(block * width, LANES), wide_width)
        for tile in range(tiles):
            stack = [field[(tile + step) * TILE : (tile + step + 1) * TILE, inner] for step in range(5)]
            turned = [pltpu.roll(held, depth, 0) for held in stack]
            between = [jnp.where(low_half, turned[step], turned[step + 1]) for step in range(4)]
            behind_y = [between[1], stack[1], between[0], stack[0]]
            ahead_y = [between[2], stack[3], between[3], stack[4]]
            wide = field[skirt + tile * TILE : skirt + (tile + 1) * TILE, around]
            grad_x = jnp.zeros((TILE, width), jnp.float32)
            grad_y = jnp.zeros((TILE, width), jnp.float32)
            partial = 3.0 * center_coeff * stack[2]
            for reach in range(1, 5):
                ahead_x = pltpu.roll(wide, wide_width - reach, 1)[:, LANES : LANES + width]
                behind_x = pltpu.roll(wide, reach, 1)[:, LANES : LANES + width]
                up, down = ahead_y[reach - 1], behind_y[reach - 1]
                grad_x = grad_x + first_coeffs[reach - 1] * (ahead_x - behind_x)
                grad_y = grad_y + first_coeffs[reach - 1] * (up - down)
                partial = partial + second_coeffs[reach - 1] * ((ahead_x + behind_x) + (up + down))
            at = slice(tile * TILE, (tile + 1) * TILE)
            grads[0, at, columns] = grad_x
            grads[1, at, columns] = grad_y
            part[at, columns] = part[at, columns] + (time_step * diffusivity) * partial
        return carry

    lax.fori_loop(0, cells // width, plane, 0)

    for comp in range(3):
        for step in range(1, gx):
            seg_copy(comp, step).wait()
    for comp in range(3):
        for block in range(gx):
            at = (comp * gx + block) * group
            for slab in range(span):
                gathered[at : at + group, slab * LANES : (slab + 1) * LANES] = seg_recv[comp, block, slab]
    total = 3 * lines
    top, rest = split(gathered[...])
    values[0:total, :] = top
    values[total:, :] = rest

    def combine(pair, carry):
        top = jnp.concatenate([matrix_top[2 * pair], matrix_top[2 * pair + 1]], axis=1)
        rest = jnp.concatenate([matrix_rest[2 * pair], matrix_rest[2 * pair + 1]], axis=1)
        first = jnp.dot(values[...], top, preferred_element_type=jnp.float32)
        second = jnp.dot(values[0:total, :], rest, preferred_element_type=jnp.float32)
        moved = first[:total] + (first[total:] + second)
        columns = pl.ds(pl.multiple_of(pair * 2 * LANES, 2 * LANES), 2 * LANES)
        carried = moved[:lines] * grads[0, :, columns] + moved[lines : 2 * lines] * grads[1, :, columns]
        part[:, columns] = part[:, columns] - time_step * carried
        drift[:, columns] = time_step * moved[2 * lines :]
        return carry

    lax.fori_loop(0, cells // (2 * LANES), combine, 0)

    place_of = lax.rem(lax.broadcasted_iota(jnp.int32, (TILE, width), 0), depth)
    for tile in range(tiles):
        for way in range(2):
            deep_copy(way, tile).wait()
        at = slice(tile * TILE, (tile + 1) * TILE)

        def finish(block, carry):
            columns = pl.ds(pl.multiple_of(block * width, LANES), width)
            inner = pl.ds(pl.multiple_of(block * width + LANES, LANES), width)
            own = field[skirt + tile * TILE : skirt + (tile + 1) * TILE, inner]
            back, front = z_back[at, columns], z_front[at, columns]
            grad_z = jnp.zeros((TILE, width), jnp.float32)
            partial = jnp.zeros((TILE, width), jnp.float32)
            for reach in range(1, 5):
                up, down = front, back
                if reach < HALO:
                    up = jnp.where(
                        place_of < depth - reach, pltpu.roll(own, TILE - reach, 0), pltpu.roll(front, depth - reach, 0)
                    )
                    down = jnp.where(
                        place_of >= reach, pltpu.roll(own, reach, 0), pltpu.roll(back, depth + reach, 0)
                    )
                grad_z = grad_z + first_coeffs[reach - 1] * (up - down)
                partial = partial + second_coeffs[reach - 1] * (up + down)
            after = (part[at, columns] + (time_step * diffusivity) * partial) - drift[at, columns] * grad_z
            later = own + section_gain * after
            for half in range(TILE // depth):
                row, piece = tile * (TILE // depth) + half, slice(half * depth, (half + 1) * depth)
                sum_out[row, :, columns] = after[piece]
                theta_out[row, :, columns] = later[piece]
            return carry

        lax.fori_loop(0, cells // width, finish, 0)


def put(theta_ref, sum_ref, theta_out, sum_out, sems):
    copies = [
        pltpu.make_async_copy(theta_ref, theta_out, sems.at[0]),
        pltpu.make_async_copy(sum_ref, sum_out, sems.at[1]),
    ]
    for copy in copies:
        copy.start()
    for copy in copies:
        copy.wait()


def body(spectrum, theta, section_sum, seg_offset, seg_length, stencil_index, stencil_weight):
    sizes = tuple(lax.axis_size(axis) for axis in ("gx", "gy", "gz"))
    gx, _, gz = sizes
    _, _, own_rows, all_depth, modes = spectrum.shape
    rows, depth, cells = theta.shape
    taps = stencil_index.shape[0]
    assert depth == HALO and rows * depth % TILE == 0 and cells % min(WIDTH, cells) == 0
    group = own_rows * depth
    slabs = gz * modes // LANES
    length = 2 * slabs * LANES
    far = length // LANES
    span = min(3 * length // (2 * gx) // LANES + 1, far)
    k = np.arange(LANES)
    turn = 2 * np.pi * (np.outer(k, k) % length) / length
    twist = np.stack([np.cos(turn), np.sin(turn)]).astype(np.float32)
    turn = 2 * np.pi * (np.outer(np.arange(far), k) % far) / far
    last = np.concatenate([np.cos(turn), -np.sin(turn)], axis=1).astype(np.float32)
    top = last.astype(jnp.bfloat16)
    rest = (last - top.astype(np.float32)).astype(jnp.bfloat16)
    modes_shape = (3, gz, modes // LANES, 2 * group, LANES)
    seg_shape = (3, gx, span, group, LANES)
    lines = rows * depth
    tiles = lines // TILE
    single = jnp.float32
    held = pl.pallas_call(
        functools.partial(section_kernel, sizes, span),
        out_shape=[VMEM(theta.shape, single)] * 2,
        in_specs=[pl.BlockSpec(memory_space=pltpu.SMEM)] * 2 + [pl.BlockSpec(memory_space=pltpu.HBM)] * 7,
        out_specs=whole_vmem(2),
        scratch_shapes=[
            VMEM(spectrum.shape, single),
            VMEM(theta.shape, single),
            VMEM(theta.shape, single),
            VMEM((taps, cells), jnp.int32),
            VMEM((taps, cells), single),
            VMEM(twist.shape, single),
            VMEM((2 * far, 2 * LANES), jnp.bfloat16),
            VMEM(modes_shape, single),
            VMEM(modes_shape, single),
            VMEM((2 * slabs, 2 * group, LANES), single),
            VMEM((far, group, LANES), single),
            VMEM(seg_shape, single),
            VMEM(seg_shape, single),
            VMEM((cells // LANES, span * LANES, LANES), jnp.bfloat16),
            VMEM((cells // LANES, span * LANES, LANES), jnp.bfloat16),
            VMEM((3 * lines, span * LANES), single),
            VMEM((6 * lines, span * LANES), jnp.bfloat16),
            VMEM((2, lines, cells), single),
            VMEM((lines, cells), single),
            VMEM((lines, cells), single),
            VMEM((lines + 2 * HALO * depth, cells + 2 * LANES), single),
            VMEM((lines, cells), single),
            VMEM((lines, cells), single),
            pltpu.SemaphoreType.DMA((7,)),
            pltpu.SemaphoreType.DMA((2, 3, gz)),
            pltpu.SemaphoreType.DMA((2, 3, gx - 1)),
            pltpu.SemaphoreType.DMA((2, 4)),
            pltpu.SemaphoreType.DMA((2, 2, tiles)),
        ],
        compiler_params=pltpu.CompilerParams(
            collective_id=0, has_side_effects=True, vmem_limit_bytes=60 * 1024 * 1024
        ),
        name="section",
    )(
        seg_offset, seg_length, spectrum, theta, section_sum, stencil_index, stencil_weight,
        jnp.asarray(twist), jnp.asarray(np.concatenate([top, rest], axis=0)),
    )
    return tuple(
        pl.pallas_call(
            put,
            out_shape=[jax.ShapeDtypeStruct(theta.shape, single)] * 2,
            in_specs=[pl.BlockSpec(memory_space=pl.ANY)] * 2,
            out_specs=[pl.BlockSpec(memory_space=pltpu.HBM)] * 2,
            scratch_shapes=[pltpu.SemaphoreType.DMA((2,))],
            compiler_params=pltpu.CompilerParams(vmem_limit_bytes=1024 * 1024),
            name="put",
        )(*held)
    )


def solution(mesh):
    placed = (
        P(None, None, ("gy", "gx"), None, "gz"),
        P("gy", "gz", "gx"),
        P("gy", "gz", "gx"),
        P(),
        P(),
        P(),
        P(),
    )
    return jax.shard_map(
        body,
        mesh=mesh,
        in_specs=placed,
        out_specs=(P("gy", "gz", "gx"), P("gy", "gz", "gx")),
        check_vma=False,
    )
```

```python
import functools
import math

import jax
import jax.numpy as jnp
import numpy as np
from jax import lax
from jax.experimental import pallas as pl
from jax.experimental.pallas import tpu as pltpu
from jax.sharding import PartitionSpec as P

MESH = pl.DeviceIdType.MESH
VMEM = pltpu.VMEM
LANES = 128
HALO = 4
TILE = 8
WIDTH = 512

first_coeffs = (0.8, -0.2, 4.0 / 105.0, -1.0 / 280.0)
second_coeffs = (1.6, -0.2, 8.0 / 315.0, -1.0 / 560.0)
center_coeff = -205.0 / 72.0
diffusivity = 0.15
time_step = 0.4
section_keep = -5.0 / 9.0
section_gain = 15.0 / 16.0


def whole_vmem(count):
    return [pl.BlockSpec(memory_space=VMEM)] * count


def rotate(value, turn):
    re, im = value
    cosine, sine = math.cos(2 * math.pi * turn), math.sin(2 * math.pi * turn)
    quarter = turn * 4 % 4
    if quarter == 0:
        return re, im
    if quarter == 1:
        return -im, re
    if quarter == 2:
        return -re, -im
    if quarter == 3:
        return im, -re
    return re * cosine - im * sine, re * sine + im * cosine


def fft(values):
    count = len(values)
    if count == 1:
        return values
    even = fft(values[0::2])
    odd = fft(values[1::2])
    low, high = [], []
    for x in range(count // 2):
        re, im = rotate(odd[x], x / count)
        low.append((even[x][0] + re, even[x][1] + im))
        high.append((even[x][0] - re, even[x][1] - im))
    return low + high


def split(value):
    top = value.astype(jnp.bfloat16)
    return top, (value - top.astype(jnp.float32)).astype(jnp.bfloat16)


def section_kernel(
    sizes, span,
    offset_ref, length_ref, spec_hbm, theta_hbm, sum_hbm, index_hbm, weight_hbm, twist_hbm, last_hbm,
    theta_out, sum_out,
    spec_ref, theta_ref, sum_ref, index_ref, weight_ref, twist_ref, last_ref,
    modes_send, modes_recv, mixed, velocity, seg_send, seg_recv, matrix_top, matrix_rest, gathered, values,
    grads, part, drift, field, z_back, z_front,
    load_sems, modes_sems, seg_sems, face_sems, deep_sems, relay_sems,
):
    gx, gy, gz = sizes
    here = {axis: lax.axis_index(axis) for axis in ("gx", "gy", "gz")}
    counts = dict(gx=gx, gy=gy, gz=gz)
    ahead = {axis: {axis: lax.rem(here[axis] + 1, counts[axis])} for axis in here}
    behind = {axis: {axis: lax.rem(here[axis] + counts[axis] - 1, counts[axis])} for axis in here}
    me, layer = here["gx"], here["gz"]
    rows, depth, cells = theta_ref.shape
    _, _, own_rows, all_depth, modes = spec_ref.shape
    local_slabs = modes // LANES
    group = own_rows * depth
    slabs = gz * local_slabs
    near = 2 * slabs
    far = 2 * slabs
    taps = index_ref.shape[0]
    lines = rows * depth
    tiles = lines // TILE
    skirt = HALO * depth

    own_columns = pl.ds(pl.multiple_of(me * cells, LANES), cells)
    loads = [
        pltpu.make_async_copy(source, place, load_sems.at[number])
        for number, (source, place) in enumerate(
            [
                (spec_hbm, spec_ref),
                (theta_hbm, theta_ref),
                (index_hbm.at[:, own_columns], index_ref),
                (weight_hbm.at[:, own_columns], weight_ref),
                (twist_hbm, twist_ref),
                (last_hbm, last_ref),
                (sum_hbm, sum_ref),
            ]
        )
    ]
    for load in loads:
        load.start()

    barrier = pltpu.get_barrier_semaphore()
    has_up, has_down = layer < gz - 1, layer > 0

    def signal(semaphore, target):
        pl.semaphore_signal(semaphore, inc=1, device_id=target, device_id_type=MESH)

    @pl.when(has_up)
    def _():
        signal(barrier, {"gz": layer + 1})

    @pl.when(has_down)
    def _():
        signal(barrier, {"gz": layer - 1})

    targets = [{"gx": lax.rem(me + step, gx)} for step in range(1, gx)]
    targets += [ahead["gy"], behind["gy"]]
    for target in targets:
        signal(barrier, target)

    loads[0].wait()
    for comp in range(3):
        for slab in range(local_slabs):
            for part_of in range(2):
                for row in range(own_rows):
                    held = spec_ref[comp, part_of, row, :, slab * LANES : (slab + 1) * LANES]
                    at = part_of * group + row * depth
                    for peer in range(gz):
                        modes_send[comp, peer, slab, at : at + depth, :] = held[
                            peer * depth : (peer + 1) * depth
                        ]

    @pl.when(jnp.logical_and(has_up, has_down))
    def _():
        pl.semaphore_wait(barrier, len(targets) + 2)

    @pl.when(jnp.logical_not(jnp.logical_and(has_up, has_down)))
    def _():
        pl.semaphore_wait(barrier, len(targets) + 1)

    def tell(distance):
        @pl.when(jnp.logical_and(has_down, layer + distance - 1 < gz))
        def _():
            signal(relay_sems.at[0, distance], {"gz": layer - 1})

        @pl.when(jnp.logical_and(has_up, layer >= distance - 1))
        def _():
            signal(relay_sems.at[1, distance], {"gz": layer + 1})

    def hear(distance):
        @pl.when(layer + distance < gz)
        def _():
            pl.semaphore_wait(relay_sems.at[0, distance], 1)

        @pl.when(layer >= distance)
        def _():
            pl.semaphore_wait(relay_sems.at[1, distance], 1)

    def modes_copy(comp, target):
        return pltpu.make_async_remote_copy(
            src_ref=modes_send.at[comp, target],
            dst_ref=modes_recv.at[comp, layer],
            send_sem=modes_sems.at[0, comp, target],
            recv_sem=modes_sems.at[1, comp, layer],
            device_id={"gz": target},
            device_id_type=MESH,
        )

    def modes_wait(comp, other):
        pltpu.make_async_remote_copy(
            src_ref=modes_send.at[comp, other],
            dst_ref=modes_recv.at[comp, other],
            send_sem=modes_sems.at[0, comp, other],
            recv_sem=modes_sems.at[1, comp, other],
            device_id={"gz": other},
            device_id_type=MESH,
        ).wait()

    def send_modes(comp, distance):
        @pl.when(layer + distance < gz)
        def _():
            modes_copy(comp, layer + distance).start()

        @pl.when(layer >= distance)
        def _():
            modes_copy(comp, layer - distance).start()

    if gz > 2:
        tell(2)
    for comp in range(3):
        send_modes(comp, 1)
    for distance in range(2, gz):
        hear(distance)
        if distance + 1 < gz:
            tell(distance + 1)
        send_modes(0, distance)
    for comp in range(1, 3):
        for distance in range(2, gz):
            send_modes(comp, distance)

    def seg_copy(comp, step):
        target = lax.rem(me + step, gx)
        return pltpu.make_async_remote_copy(
            src_ref=seg_send.at[comp, target],
            dst_ref=seg_recv.at[comp, me],
            send_sem=seg_sems.at[0, comp, step - 1],
            recv_sem=seg_sems.at[1, comp, step - 1],
            device_id={"gx": target},
            device_id_type=MESH,
        )

    loads[1].wait()
    for tile in range(tiles):
        at = skirt + tile * TILE
        for half in range(TILE // depth):
            field[at + half * depth : at + (half + 1) * depth, LANES : LANES + cells] = theta_ref[
                tile * (TILE // depth) + half
            ]

    mine = pl.ds(skirt, lines)
    middle = pl.ds(LANES, cells)
    faces = [
        pltpu.make_async_remote_copy(
            src_ref=field.at[source],
            dst_ref=field.at[place],
            send_sem=face_sems.at[0, number],
            recv_sem=face_sems.at[1, number],
            device_id=device,
            device_id_type=MESH,
        )
        for number, (source, place, device) in enumerate(
            [
                ((mine, pl.ds(cells, LANES)), (mine, pl.ds(0, LANES)), ahead["gx"]),
                ((mine, pl.ds(LANES, LANES)), (mine, pl.ds(LANES + cells, LANES)), behind["gx"]),
                ((pl.ds(lines, skirt), middle), (pl.ds(0, skirt), middle), ahead["gy"]),
                ((pl.ds(skirt, skirt), middle), (pl.ds(skirt + lines, skirt), middle), behind["gy"]),
            ]
        )
    ]
    for face in faces:
        face.start()

    def deep_copy(way, tile):
        return pltpu.make_async_remote_copy(
            src_ref=field.at[pl.ds(skirt + tile * TILE, TILE), middle],
            dst_ref=(z_back, z_front)[way].at[pl.ds(tile * TILE, TILE)],
            send_sem=deep_sems.at[0, way, tile],
            recv_sem=deep_sems.at[1, way, tile],
            device_id=(ahead, behind)[way]["gz"],
            device_id_type=MESH,
        )

    for comp in range(3):
        modes_recv[comp, layer] = modes_send[comp, layer]

    loads[2].wait()
    loads[3].wait()
    live_count = length_ref[me]
    begin = offset_ref[me] - jnp.minimum(offset_ref[me] // LANES, far - span) * LANES
    counter = lax.broadcasted_iota(jnp.int32, (LANES, LANES), 0).astype(jnp.float32).astype(jnp.bfloat16)
    counters = [counter[step : step + 16] for step in range(0, LANES, 16)]

    def spread(row):
        return jnp.broadcast_to(row, (16, LANES)).astype(jnp.bfloat16)

    def build(chunk, carry):
        columns = pl.ds(pl.multiple_of(chunk * LANES, LANES), LANES)
        index = index_ref[:, columns]
        live = index < live_count
        weight = jnp.where(live, weight_ref[:, columns], 0.0)
        merged = jnp.zeros_like(weight)
        for tap in range(taps):
            merged = merged + jnp.where(index == index[tap : tap + 1], weight[tap : tap + 1], 0.0)
        high, low = split(merged)
        high, low = high.astype(jnp.float32), low.astype(jnp.float32)
        place = jnp.where(live, index + begin, -1)
        owner = (place >> 7).astype(jnp.float32)
        within = (place & (LANES - 1)).astype(jnp.float32)
        tops = [spread(high[tap : tap + 1]) for tap in range(taps)]
        rests = [spread(low[tap : tap + 1]) for tap in range(taps)]
        owners = [spread(owner[tap : tap + 1]) for tap in range(taps)]
        withins = [spread(within[tap : tap + 1]) for tap in range(taps)]

        def slab_of(slab, inner):
            number = jnp.full((16, LANES), slab, jnp.int32).astype(jnp.float32).astype(jnp.bfloat16)
            close = [
                jnp.where(owners[tap] == number, withins[tap], jnp.bfloat16(-1)) for tap in range(taps)
            ]
            for step in range(LANES // 16):
                top = jnp.zeros((16, LANES), jnp.bfloat16)
                rest = jnp.zeros((16, LANES), jnp.bfloat16)
                for tap in range(taps):
                    hit = counters[step] == close[tap]
                    top = jnp.where(hit, tops[tap], top)
                    rest = jnp.where(hit, rests[tap], rest)
                at = pl.ds(pl.multiple_of(slab * LANES + step * 16, 16), 16)
                matrix_top[chunk, at, :] = top
                matrix_rest[chunk, at, :] = rest
            return inner

        return lax.fori_loop(0, span, slab_of, carry)

    chunks = cells // LANES
    early, step_of = chunks * 3 // 8, chunks // 8
    lax.fori_loop(0, early, build, 0)

    @pl.when(layer == gz - 1)
    def _():
        for way in (1, 0):
            for tile in range(tiles):
                deep_copy(way, tile).start()

    @pl.when(layer != gz - 1)
    def _():
        for way in (0, 1):
            for tile in range(tiles):
                deep_copy(way, tile).start()

    loads[4].wait()
    loads[5].wait()
    last_both = last_ref[...]
    last_top = last_both[:far]
    dims = (((1,), (1,)), ((), ()))

    def twisted(line):
        re, im = mixed[:, line, :], mixed[:, group + line, :]
        pieces = []
        for quarter in range(LANES // near):
            part_of = slice(quarter * near, (quarter + 1) * near)
            cosine, sine = twist_ref[0, part_of, :], twist_ref[1, part_of, :]
            pieces.append(jnp.concatenate([re * cosine - im * sine, re * sine + im * cosine], axis=1))
        return jnp.concatenate(pieces, axis=0)

    def transform(comp, carry):
        lax.fori_loop(early + comp * step_of, early + (comp + 1) * step_of, build, 0)
        for step in range(1, gz):
            modes_wait(comp, lax.rem(layer + step, gz))

        def arrived(k):
            held = modes_recv[comp, k // local_slabs, k % local_slabs]
            return held[:group], held[group:]

        for parity in range(2):
            mixes = fft([rotate(arrived(k), parity * k / near) for k in range(slabs)])
            for x in range(slabs):
                mixed[2 * x + parity, 0:group, :] = mixes[x][0]
                mixed[2 * x + parity, group:, :] = mixes[x][1]
        for pair in range(group // 2):
            turned = jnp.concatenate([twisted(2 * pair), twisted(2 * pair + 1)], axis=0)
            top, rest = split(turned)
            first = lax.dot_general(last_both, top, dims, preferred_element_type=jnp.float32)
            second = lax.dot_general(last_top, rest, dims, preferred_element_type=jnp.float32)
            total = first[:far] + (first[far:] + second)
            velocity[:, 2 * pair, :] = total[:, :LANES]
            velocity[:, 2 * pair + 1, :] = total[:, LANES:]
        for block in range(gx):
            start = jnp.minimum(offset_ref[block] // LANES, far - span)
            seg_send[comp, block] = velocity[pl.ds(start, span)]
        for step in range(1, gx):
            seg_copy(comp, step).start()
        seg_recv[comp, me] = seg_send[comp, me]
        return carry

    lax.fori_loop(0, 3, transform, 0)
    lax.fori_loop(early + 3 * step_of, chunks, build, 0)

    loads[6].wait()
    for tile in range(tiles):
        for half in range(TILE // depth):
            at = tile * TILE + half * depth
            part[at : at + depth, :] = section_keep * sum_ref[tile * (TILE // depth) + half]
    for face in faces:
        face.wait()
    width = min(WIDTH, cells)
    wide_width = width + 2 * LANES
    low_half = lax.broadcasted_iota(jnp.int32, (TILE, width), 0) < depth

    def plane(block, carry):
        columns = pl.ds(pl.multiple_of(block * width, LANES), width)
        inner = pl.ds(pl.multiple_of(block * width + LANES, LANES), width)
        around = pl.ds(pl.multiple_of(block * width, LANES), wide_width)
        for tile in range(tiles):
            stack = [field[(tile + step) * TILE : (tile + step + 1) * TILE, inner] for step in range(5)]
            turned = [pltpu.roll(held, depth, 0) for held in stack]
            between = [jnp.where(low_half, turned[step], turned[step + 1]) for step in range(4)]
            behind_y = [between[1], stack[1], between[0], stack[0]]
            ahead_y = [between[2], stack[3], between[3], stack[4]]
            wide = field[skirt + tile * TILE : skirt + (tile + 1) * TILE, around]
            grad_x = jnp.zeros((TILE, width), jnp.float32)
            grad_y = jnp.zeros((TILE, width), jnp.float32)
            partial = 3.0 * center_coeff * stack[2]
            for reach in range(1, 5):
                ahead_x = pltpu.roll(wide, wide_width - reach, 1)[:, LANES : LANES + width]
                behind_x = pltpu.roll(wide, reach, 1)[:, LANES : LANES + width]
                up, down = ahead_y[reach - 1], behind_y[reach - 1]
                grad_x = grad_x + first_coeffs[reach - 1] * (ahead_x - behind_x)
                grad_y = grad_y + first_coeffs[reach - 1] * (up - down)
                partial = partial + second_coeffs[reach - 1] * ((ahead_x + behind_x) + (up + down))
            at = slice(tile * TILE, (tile + 1) * TILE)
            grads[0, at, columns] = grad_x
            grads[1, at, columns] = grad_y
            part[at, columns] = part[at, columns] + (time_step * diffusivity) * partial
        return carry

    lax.fori_loop(0, cells // width, plane, 0)

    for comp in range(3):
        for step in range(1, gx):
            seg_copy(comp, step).wait()
    for comp in range(3):
        for block in range(gx):
            at = (comp * gx + block) * group
            for slab in range(span):
                gathered[at : at + group, slab * LANES : (slab + 1) * LANES] = seg_recv[comp, block, slab]
    total = 3 * lines
    top, rest = split(gathered[...])
    values[0:total, :] = top
    values[total:, :] = rest

    def combine(pair, carry):
        top = jnp.concatenate([matrix_top[2 * pair], matrix_top[2 * pair + 1]], axis=1)
        rest = jnp.concatenate([matrix_rest[2 * pair], matrix_rest[2 * pair + 1]], axis=1)
        first = jnp.dot(values[...], top, preferred_element_type=jnp.float32)
        second = jnp.dot(values[0:total, :], rest, preferred_element_type=jnp.float32)
        moved = first[:total] + (first[total:] + second)
        columns = pl.ds(pl.multiple_of(pair * 2 * LANES, 2 * LANES), 2 * LANES)
        carried = moved[:lines] * grads[0, :, columns] + moved[lines : 2 * lines] * grads[1, :, columns]
        part[:, columns] = part[:, columns] - time_step * carried
        drift[:, columns] = time_step * moved[2 * lines :]
        return carry

    lax.fori_loop(0, cells // (2 * LANES), combine, 0)

    place_of = lax.rem(lax.broadcasted_iota(jnp.int32, (TILE, width), 0), depth)
    for tile in range(tiles):
        for way in range(2):
            deep_copy(way, tile).wait()
        at = slice(tile * TILE, (tile + 1) * TILE)

        def finish(block, carry):
            columns = pl.ds(pl.multiple_of(block * width, LANES), width)
            inner = pl.ds(pl.multiple_of(block * width + LANES, LANES), width)
            own = field[skirt + tile * TILE : skirt + (tile + 1) * TILE, inner]
            back, front = z_back[at, columns], z_front[at, columns]
            grad_z = jnp.zeros((TILE, width), jnp.float32)
            partial = jnp.zeros((TILE, width), jnp.float32)
            for reach in range(1, 5):
                up, down = front, back
                if reach < HALO:
                    up = jnp.where(
                        place_of < depth - reach, pltpu.roll(own, TILE - reach, 0), pltpu.roll(front, depth - reach, 0)
                    )
                    down = jnp.where(
                        place_of >= reach, pltpu.roll(own, reach, 0), pltpu.roll(back, depth + reach, 0)
                    )
                grad_z = grad_z + first_coeffs[reach - 1] * (up - down)
                partial = partial + second_coeffs[reach - 1] * (up + down)
            after = (part[at, columns] + (time_step * diffusivity) * partial) - drift[at, columns] * grad_z
            later = own + section_gain * after
            for half in range(TILE // depth):
                row, piece = tile * (TILE // depth) + half, slice(half * depth, (half + 1) * depth)
                sum_out[row, :, columns] = after[piece]
                theta_out[row, :, columns] = later[piece]
            return carry

        lax.fori_loop(0, cells // width, finish, 0)


def put(theta_ref, sum_ref, theta_out, sum_out, sems):
    copies = [
        pltpu.make_async_copy(theta_ref, theta_out, sems.at[0]),
        pltpu.make_async_copy(sum_ref, sum_out, sems.at[1]),
    ]
    for copy in copies:
        copy.start()
    for copy in copies:
        copy.wait()


def body(spectrum, theta, section_sum, seg_offset, seg_length, stencil_index, stencil_weight):
    sizes = tuple(lax.axis_size(axis) for axis in ("gx", "gy", "gz"))
    gx, _, gz = sizes
    _, _, own_rows, all_depth, modes = spectrum.shape
    rows, depth, cells = theta.shape
    taps = stencil_index.shape[0]
    assert depth == HALO and rows * depth % TILE == 0 and cells % min(WIDTH, cells) == 0
    group = own_rows * depth
    slabs = gz * modes // LANES
    length = 2 * slabs * LANES
    far = length // LANES
    span = min(3 * length // (2 * gx) // LANES + 1, far)
    k = np.arange(LANES)
    turn = 2 * np.pi * (np.outer(k, k) % length) / length
    twist = np.stack([np.cos(turn), np.sin(turn)]).astype(np.float32)
    turn = 2 * np.pi * (np.outer(np.arange(far), k) % far) / far
    last = np.concatenate([np.cos(turn), -np.sin(turn)], axis=1).astype(np.float32)
    top = last.astype(jnp.bfloat16)
    rest = (last - top.astype(np.float32)).astype(jnp.bfloat16)
    modes_shape = (3, gz, modes // LANES, 2 * group, LANES)
    seg_shape = (3, gx, span, group, LANES)
    lines = rows * depth
    tiles = lines // TILE
    single = jnp.float32
    held = pl.pallas_call(
        functools.partial(section_kernel, sizes, span),
        out_shape=[VMEM(theta.shape, single)] * 2,
        in_specs=[pl.BlockSpec(memory_space=pltpu.SMEM)] * 2 + [pl.BlockSpec(memory_space=pltpu.HBM)] * 7,
        out_specs=whole_vmem(2),
        scratch_shapes=[
            VMEM(spectrum.shape, single),
            VMEM(theta.shape, single),
            VMEM(theta.shape, single),
            VMEM((taps, cells), jnp.int32),
            VMEM((taps, cells), single),
            VMEM(twist.shape, single),
            VMEM((2 * far, 2 * LANES), jnp.bfloat16),
            VMEM(modes_shape, single),
            VMEM(modes_shape, single),
            VMEM((2 * slabs, 2 * group, LANES), single),
            VMEM((far, group, LANES), single),
            VMEM(seg_shape, single),
            VMEM(seg_shape, single),
            VMEM((cells // LANES, span * LANES, LANES), jnp.bfloat16),
            VMEM((cells // LANES, span * LANES, LANES), jnp.bfloat16),
            VMEM((3 * lines, span * LANES), single),
            VMEM((6 * lines, span * LANES), jnp.bfloat16),
            VMEM((2, lines, cells), single),
            VMEM((lines, cells), single),
            VMEM((lines, cells), single),
            VMEM((lines + 2 * HALO * depth, cells + 2 * LANES), single),
            VMEM((lines, cells), single),
            VMEM((lines, cells), single),
            pltpu.SemaphoreType.DMA((7,)),
            pltpu.SemaphoreType.DMA((2, 3, gz)),
            pltpu.SemaphoreType.DMA((2, 3, gx - 1)),
            pltpu.SemaphoreType.DMA((2, 4)),
            pltpu.SemaphoreType.DMA((2, 2, tiles)),
            pltpu.SemaphoreType.REGULAR((2, gz)),
        ],
        compiler_params=pltpu.CompilerParams(
            collective_id=0, has_side_effects=True, vmem_limit_bytes=60 * 1024 * 1024
        ),
        name="section",
    )(
        seg_offset, seg_length, spectrum, theta, section_sum, stencil_index, stencil_weight,
        jnp.asarray(twist), jnp.asarray(np.concatenate([top, rest], axis=0)),
    )
    return tuple(
        pl.pallas_call(
            put,
            out_shape=[jax.ShapeDtypeStruct(theta.shape, single)] * 2,
            in_specs=[pl.BlockSpec(memory_space=pl.ANY)] * 2,
            out_specs=[pl.BlockSpec(memory_space=pltpu.HBM)] * 2,
            scratch_shapes=[pltpu.SemaphoreType.DMA((2,))],
            compiler_params=pltpu.CompilerParams(vmem_limit_bytes=1024 * 1024),
            name="put",
        )(*held)
    )


def solution(mesh):
    placed = (
        P(None, None, ("gy", "gx"), None, "gz"),
        P("gy", "gz", "gx"),
        P("gy", "gz", "gx"),
        P(),
        P(),
        P(),
        P(),
    )
    return jax.shard_map(
        body,
        mesh=mesh,
        in_specs=placed,
        out_specs=(P("gy", "gz", "gx"), P("gy", "gz", "gx")),
        check_vma=False,
    )
```

```python
import functools
import math

import jax
import jax.numpy as jnp
import numpy as np
from jax import lax
from jax.experimental import pallas as pl
from jax.experimental.pallas import tpu as pltpu
from jax.sharding import PartitionSpec as P

MESH = pl.DeviceIdType.MESH
VMEM = pltpu.VMEM
LANES = 128
HALO = 4
TILE = 8
WIDTH = 512

first_coeffs = (0.8, -0.2, 4.0 / 105.0, -1.0 / 280.0)
second_coeffs = (1.6, -0.2, 8.0 / 315.0, -1.0 / 560.0)
center_coeff = -205.0 / 72.0
diffusivity = 0.15
time_step = 0.4
section_keep = -5.0 / 9.0
section_gain = 15.0 / 16.0


def whole_vmem(count):
    return [pl.BlockSpec(memory_space=VMEM)] * count


def rotate(value, turn):
    re, im = value
    cosine, sine = math.cos(2 * math.pi * turn), math.sin(2 * math.pi * turn)
    quarter = turn * 4 % 4
    if quarter == 0:
        return re, im
    if quarter == 1:
        return -im, re
    if quarter == 2:
        return -re, -im
    if quarter == 3:
        return im, -re
    return re * cosine - im * sine, re * sine + im * cosine


def fft(values):
    count = len(values)
    if count == 1:
        return values
    even = fft(values[0::2])
    odd = fft(values[1::2])
    low, high = [], []
    for x in range(count // 2):
        re, im = rotate(odd[x], x / count)
        low.append((even[x][0] + re, even[x][1] + im))
        high.append((even[x][0] - re, even[x][1] - im))
    return low + high


def split(value):
    top = value.astype(jnp.bfloat16)
    return top, (value - top.astype(jnp.float32)).astype(jnp.bfloat16)


def section_kernel(
    sizes, span,
    offset_ref, length_ref, spec_hbm, theta_hbm, sum_hbm, index_hbm, weight_hbm, twist_hbm, last_hbm,
    theta_out, sum_out,
    spec_ref, theta_ref, sum_ref, index_ref, weight_ref, twist_ref, last_ref,
    modes_send, modes_recv, mixed, velocity, seg_send, seg_recv, matrix_top, matrix_rest, gathered, values,
    grads, part, drift, field, z_back, z_front,
    load_sems, modes_sems, seg_sems, face_sems, deep_sems,
):
    gx, gy, gz = sizes
    here = {axis: lax.axis_index(axis) for axis in ("gx", "gy", "gz")}
    counts = dict(gx=gx, gy=gy, gz=gz)
    ahead = {axis: {axis: lax.rem(here[axis] + 1, counts[axis])} for axis in here}
    behind = {axis: {axis: lax.rem(here[axis] + counts[axis] - 1, counts[axis])} for axis in here}
    me, layer = here["gx"], here["gz"]
    rows, depth, cells = theta_ref.shape
    _, _, own_rows, all_depth, modes = spec_ref.shape
    local_slabs = modes // LANES
    group = own_rows * depth
    slabs = gz * local_slabs
    near = 2 * slabs
    far = 2 * slabs
    taps = index_ref.shape[0]
    lines = rows * depth
    tiles = lines // TILE
    skirt = HALO * depth

    own_columns = pl.ds(pl.multiple_of(me * cells, LANES), cells)
    loads = [
        pltpu.make_async_copy(source, place, load_sems.at[number])
        for number, (source, place) in enumerate(
            [
                (spec_hbm.at[0], spec_ref.at[0]),
                (spec_hbm.at[1], spec_ref.at[1]),
                (spec_hbm.at[2], spec_ref.at[2]),
                (theta_hbm, theta_ref),
                (index_hbm.at[:, own_columns], index_ref),
                (weight_hbm.at[:, own_columns], weight_ref),
                (twist_hbm, twist_ref),
                (last_hbm, last_ref),
                (sum_hbm, sum_ref),
            ]
        )
    ]
    for load in loads:
        load.start()

    barrier = pltpu.get_barrier_semaphore()
    has_up, has_down = layer < gz - 1, layer > 0
    inner = jnp.logical_and(has_up, has_down)
    per_tile = TILE // depth

    def signal(semaphore, target):
        pl.semaphore_signal(semaphore, inc=1, device_id=target, device_id_type=MESH)

    targets = [{"gx": lax.rem(me + step, gx)} for step in range(1, gx)]
    targets += [{"gz": lax.rem(layer + step, gz)} for step in range(1, gz)]
    targets += [ahead["gy"], behind["gy"]]
    for target in targets:
        signal(barrier, target)

    pl.semaphore_wait(barrier, len(targets))

    def modes_copy(comp, target):
        return pltpu.make_async_remote_copy(
            src_ref=modes_send.at[comp, target],
            dst_ref=modes_recv.at[comp, layer],
            send_sem=modes_sems.at[0, comp, target],
            recv_sem=modes_sems.at[1, comp, layer],
            device_id={"gz": target},
            device_id_type=MESH,
        )

    def modes_wait(comp, other):
        pltpu.make_async_remote_copy(
            src_ref=modes_send.at[comp, other],
            dst_ref=modes_recv.at[comp, other],
            send_sem=modes_sems.at[0, comp, other],
            recv_sem=modes_sems.at[1, comp, other],
            device_id={"gz": other},
            device_id_type=MESH,
        ).wait()

    def send_modes(comp, distance):
        @pl.when(layer + distance < gz)
        def _():
            modes_copy(comp, layer + distance).start()

        @pl.when(layer >= distance)
        def _():
            modes_copy(comp, layer - distance).start()

    def deep_copy(way, tile):
        part_of = pl.ds(tile * per_tile, per_tile)
        return pltpu.make_async_remote_copy(
            src_ref=theta_hbm.at[part_of],
            dst_ref=(z_back, z_front)[way].at[part_of],
            send_sem=deep_sems.at[0, way, tile],
            recv_sem=deep_sems.at[1, way, tile],
            device_id=(ahead, behind)[way]["gz"],
            device_id_type=MESH,
        )

    def send_near(chosen):
        @pl.when(has_up)
        def _():
            for tile in chosen:
                deep_copy(0, tile).start()

        @pl.when(has_down)
        def _():
            for tile in chosen:
                deep_copy(1, tile).start()

    for comp in range(3):
        loads[comp].wait()
        for slab in range(local_slabs):
            for part_of in range(2):
                for row in range(own_rows):
                    held = spec_ref[comp, part_of, row, :, slab * LANES : (slab + 1) * LANES]
                    at = part_of * group + row * depth
                    for peer in range(gz):
                        modes_send[comp, peer, slab, at : at + depth, :] = held[
                            peer * depth : (peer + 1) * depth
                        ]
        for distance in range(gz - 1, 0, -1):
            send_modes(comp, distance)
    send_near(range(tiles))

    @pl.when(jnp.logical_not(inner))
    def _():
        @pl.when(jnp.logical_not(has_up))
        def _():
            for tile in range(tiles):
                deep_copy(0, tile).start()

        @pl.when(jnp.logical_not(has_down))
        def _():
            for tile in range(tiles):
                deep_copy(1, tile).start()

    def seg_copy(comp, step):
        target = lax.rem(me + step, gx)
        return pltpu.make_async_remote_copy(
            src_ref=seg_send.at[comp, target],
            dst_ref=seg_recv.at[comp, me],
            send_sem=seg_sems.at[0, comp, step - 1],
            recv_sem=seg_sems.at[1, comp, step - 1],
            device_id={"gx": target},
            device_id_type=MESH,
        )

    loads[3].wait()
    for tile in range(tiles):
        at = skirt + tile * TILE
        for half in range(per_tile):
            field[at + half * depth : at + (half + 1) * depth, LANES : LANES + cells] = theta_ref[
                tile * (per_tile) + half
            ]

    mine = pl.ds(skirt, lines)
    middle = pl.ds(LANES, cells)
    faces = [
        pltpu.make_async_remote_copy(
            src_ref=field.at[source],
            dst_ref=field.at[place],
            send_sem=face_sems.at[0, number],
            recv_sem=face_sems.at[1, number],
            device_id=device,
            device_id_type=MESH,
        )
        for number, (source, place, device) in enumerate(
            [
                ((mine, pl.ds(cells, LANES)), (mine, pl.ds(0, LANES)), ahead["gx"]),
                ((mine, pl.ds(LANES, LANES)), (mine, pl.ds(LANES + cells, LANES)), behind["gx"]),
                ((pl.ds(lines, skirt), middle), (pl.ds(0, skirt), middle), ahead["gy"]),
                ((pl.ds(skirt, skirt), middle), (pl.ds(skirt + lines, skirt), middle), behind["gy"]),
            ]
        )
    ]
    for face in faces:
        face.start()

    for comp in range(3):
        modes_recv[comp, layer] = modes_send[comp, layer]

    loads[4].wait()
    loads[5].wait()
    live_count = length_ref[me]
    begin = offset_ref[me] - jnp.minimum(offset_ref[me] // LANES, far - span) * LANES
    counter = lax.broadcasted_iota(jnp.int32, (LANES, LANES), 0).astype(jnp.float32).astype(jnp.bfloat16)
    counters = [counter[step : step + 16] for step in range(0, LANES, 16)]

    def spread(row):
        return jnp.broadcast_to(row, (16, LANES)).astype(jnp.bfloat16)

    def build(chunk, carry):
        columns = pl.ds(pl.multiple_of(chunk * LANES, LANES), LANES)
        index = index_ref[:, columns]
        live = index < live_count
        weight = jnp.where(live, weight_ref[:, columns], 0.0)
        merged = jnp.zeros_like(weight)
        for tap in range(taps):
            merged = merged + jnp.where(index == index[tap : tap + 1], weight[tap : tap + 1], 0.0)
        high, low = split(merged)
        high, low = high.astype(jnp.float32), low.astype(jnp.float32)
        place = jnp.where(live, index + begin, -1)
        owner = (place >> 7).astype(jnp.float32)
        within = (place & (LANES - 1)).astype(jnp.float32)
        tops = [spread(high[tap : tap + 1]) for tap in range(taps)]
        rests = [spread(low[tap : tap + 1]) for tap in range(taps)]
        owners = [spread(owner[tap : tap + 1]) for tap in range(taps)]
        withins = [spread(within[tap : tap + 1]) for tap in range(taps)]

        def slab_of(slab, inner):
            number = jnp.full((16, LANES), slab, jnp.int32).astype(jnp.float32).astype(jnp.bfloat16)
            close = [
                jnp.where(owners[tap] == number, withins[tap], jnp.bfloat16(-1)) for tap in range(taps)
            ]
            for step in range(LANES // 16):
                top = jnp.zeros((16, LANES), jnp.bfloat16)
                rest = jnp.zeros((16, LANES), jnp.bfloat16)
                for tap in range(taps):
                    hit = counters[step] == close[tap]
                    top = jnp.where(hit, tops[tap], top)
                    rest = jnp.where(hit, rests[tap], rest)
                at = pl.ds(pl.multiple_of(slab * LANES + step * 16, 16), 16)
                matrix_top[chunk, at, :] = top
                matrix_rest[chunk, at, :] = rest
            return inner

        return lax.fori_loop(0, span, slab_of, carry)

    chunks = cells // LANES
    early, step_of = chunks * 3 // 8, chunks // 8
    lax.fori_loop(0, early, build, 0)

    loads[6].wait()
    loads[7].wait()
    last_both = last_ref[...]
    last_top = last_both[:far]
    dims = (((1,), (1,)), ((), ()))

    def twisted(line):
        re, im = mixed[:, line, :], mixed[:, group + line, :]
        pieces = []
        for quarter in range(LANES // near):
            part_of = slice(quarter * near, (quarter + 1) * near)
            cosine, sine = twist_ref[0, part_of, :], twist_ref[1, part_of, :]
            pieces.append(jnp.concatenate([re * cosine - im * sine, re * sine + im * cosine], axis=1))
        return jnp.concatenate(pieces, axis=0)

    def transform(comp, carry):
        lax.fori_loop(early + comp * step_of, early + (comp + 1) * step_of, build, 0)
        for step in range(1, gz):
            modes_wait(comp, lax.rem(layer + step, gz))

        def arrived(k):
            held = modes_recv[comp, k // local_slabs, k % local_slabs]
            return held[:group], held[group:]

        for parity in range(2):
            mixes = fft([rotate(arrived(k), parity * k / near) for k in range(slabs)])
            for x in range(slabs):
                mixed[2 * x + parity, 0:group, :] = mixes[x][0]
                mixed[2 * x + parity, group:, :] = mixes[x][1]
        for pair in range(group // 2):
            turned = jnp.concatenate([twisted(2 * pair), twisted(2 * pair + 1)], axis=0)
            top, rest = split(turned)
            first = lax.dot_general(last_both, top, dims, preferred_element_type=jnp.float32)
            second = lax.dot_general(last_top, rest, dims, preferred_element_type=jnp.float32)
            total = first[:far] + (first[far:] + second)
            velocity[:, 2 * pair, :] = total[:, :LANES]
            velocity[:, 2 * pair + 1, :] = total[:, LANES:]
        for block in range(gx):
            start = jnp.minimum(offset_ref[block] // LANES, far - span)
            seg_send[comp, block] = velocity[pl.ds(start, span)]
        for step in range(1, gx):
            seg_copy(comp, step).start()
        seg_recv[comp, me] = seg_send[comp, me]
        return carry

    lax.fori_loop(0, 3, transform, 0)
    lax.fori_loop(early + 3 * step_of, chunks, build, 0)

    loads[8].wait()
    for tile in range(tiles):
        for half in range(per_tile):
            at = tile * TILE + half * depth
            part[at : at + depth, :] = section_keep * sum_ref[tile * (per_tile) + half]
    for face in faces:
        face.wait()
    width = min(WIDTH, cells)
    wide_width = width + 2 * LANES
    low_half = lax.broadcasted_iota(jnp.int32, (TILE, width), 0) < depth

    def plane(block, carry):
        columns = pl.ds(pl.multiple_of(block * width, LANES), width)
        inner = pl.ds(pl.multiple_of(block * width + LANES, LANES), width)
        around = pl.ds(pl.multiple_of(block * width, LANES), wide_width)
        for tile in range(tiles):
            stack = [field[(tile + step) * TILE : (tile + step + 1) * TILE, inner] for step in range(5)]
            turned = [pltpu.roll(held, depth, 0) for held in stack]
            between = [jnp.where(low_half, turned[step], turned[step + 1]) for step in range(4)]
            behind_y = [between[1], stack[1], between[0], stack[0]]
            ahead_y = [between[2], stack[3], between[3], stack[4]]
            wide = field[skirt + tile * TILE : skirt + (tile + 1) * TILE, around]
            grad_x = jnp.zeros((TILE, width), jnp.float32)
            grad_y = jnp.zeros((TILE, width), jnp.float32)
            partial = 3.0 * center_coeff * stack[2]
            for reach in range(1, 5):
                ahead_x = pltpu.roll(wide, wide_width - reach, 1)[:, LANES : LANES + width]
                behind_x = pltpu.roll(wide, reach, 1)[:, LANES : LANES + width]
                up, down = ahead_y[reach - 1], behind_y[reach - 1]
                grad_x = grad_x + first_coeffs[reach - 1] * (ahead_x - behind_x)
                grad_y = grad_y + first_coeffs[reach - 1] * (up - down)
                partial = partial + second_coeffs[reach - 1] * ((ahead_x + behind_x) + (up + down))
            at = slice(tile * TILE, (tile + 1) * TILE)
            grads[0, at, columns] = grad_x
            grads[1, at, columns] = grad_y
            part[at, columns] = part[at, columns] + (time_step * diffusivity) * partial
        return carry

    lax.fori_loop(0, cells // width, plane, 0)

    for comp in range(3):
        for step in range(1, gx):
            seg_copy(comp, step).wait()
    for comp in range(3):
        for block in range(gx):
            at = (comp * gx + block) * group
            for slab in range(span):
                gathered[at : at + group, slab * LANES : (slab + 1) * LANES] = seg_recv[comp, block, slab]
    total = 3 * lines
    top, rest = split(gathered[...])
    values[0:total, :] = top
    values[total:, :] = rest

    def combine(pair, carry):
        top = jnp.concatenate([matrix_top[2 * pair], matrix_top[2 * pair + 1]], axis=1)
        rest = jnp.concatenate([matrix_rest[2 * pair], matrix_rest[2 * pair + 1]], axis=1)
        first = jnp.dot(values[...], top, preferred_element_type=jnp.float32)
        second = jnp.dot(values[0:total, :], rest, preferred_element_type=jnp.float32)
        moved = first[:total] + (first[total:] + second)
        columns = pl.ds(pl.multiple_of(pair * 2 * LANES, 2 * LANES), 2 * LANES)
        carried = moved[:lines] * grads[0, :, columns] + moved[lines : 2 * lines] * grads[1, :, columns]
        part[:, columns] = part[:, columns] - time_step * carried
        drift[:, columns] = time_step * moved[2 * lines :]
        return carry

    lax.fori_loop(0, cells // (2 * LANES), combine, 0)

    place_of = lax.rem(lax.broadcasted_iota(jnp.int32, (TILE, width), 0), depth)
    for tile in range(tiles):
        for way in range(2):
            deep_copy(way, tile).wait()
        at = slice(tile * TILE, (tile + 1) * TILE)

        def finish(block, carry):
            columns = pl.ds(pl.multiple_of(block * width, LANES), width)
            inner = pl.ds(pl.multiple_of(block * width + LANES, LANES), width)
            own = field[skirt + tile * TILE : skirt + (tile + 1) * TILE, inner]
            back, front = (
                jnp.concatenate([held[tile * per_tile + half, :, columns] for half in range(per_tile)], axis=0)
                for held in (z_back, z_front)
            )
            grad_z = jnp.zeros((TILE, width), jnp.float32)
            partial = jnp.zeros((TILE, width), jnp.float32)
            for reach in range(1, 5):
                up, down = front, back
                if reach < HALO:
                    up = jnp.where(
                        place_of < depth - reach, pltpu.roll(own, TILE - reach, 0), pltpu.roll(front, depth - reach, 0)
                    )
                    down = jnp.where(
                        place_of >= reach, pltpu.roll(own, reach, 0), pltpu.roll(back, depth + reach, 0)
                    )
                grad_z = grad_z + first_coeffs[reach - 1] * (up - down)
                partial = partial + second_coeffs[reach - 1] * (up + down)
            after = (part[at, columns] + (time_step * diffusivity) * partial) - drift[at, columns] * grad_z
            later = own + section_gain * after
            for half in range(per_tile):
                row, piece = tile * (per_tile) + half, slice(half * depth, (half + 1) * depth)
                sum_out[row, :, columns] = after[piece]
                theta_out[row, :, columns] = later[piece]
            return carry

        lax.fori_loop(0, cells // width, finish, 0)


def put(theta_ref, sum_ref, theta_out, sum_out, sems):
    copies = [
        pltpu.make_async_copy(theta_ref, theta_out, sems.at[0]),
        pltpu.make_async_copy(sum_ref, sum_out, sems.at[1]),
    ]
    for copy in copies:
        copy.start()
    for copy in copies:
        copy.wait()


def body(spectrum, theta, section_sum, seg_offset, seg_length, stencil_index, stencil_weight):
    sizes = tuple(lax.axis_size(axis) for axis in ("gx", "gy", "gz"))
    gx, _, gz = sizes
    _, _, own_rows, all_depth, modes = spectrum.shape
    rows, depth, cells = theta.shape
    taps = stencil_index.shape[0]
    assert depth == HALO and rows * depth % TILE == 0 and cells % min(WIDTH, cells) == 0
    group = own_rows * depth
    slabs = gz * modes // LANES
    length = 2 * slabs * LANES
    far = length // LANES
    span = min(3 * length // (2 * gx) // LANES + 1, far)
    k = np.arange(LANES)
    turn = 2 * np.pi * (np.outer(k, k) % length) / length
    twist = np.stack([np.cos(turn), np.sin(turn)]).astype(np.float32)
    turn = 2 * np.pi * (np.outer(np.arange(far), k) % far) / far
    last = np.concatenate([np.cos(turn), -np.sin(turn)], axis=1).astype(np.float32)
    top = last.astype(jnp.bfloat16)
    rest = (last - top.astype(np.float32)).astype(jnp.bfloat16)
    modes_shape = (3, gz, modes // LANES, 2 * group, LANES)
    seg_shape = (3, gx, span, group, LANES)
    lines = rows * depth
    tiles = lines // TILE
    single = jnp.float32
    held = pl.pallas_call(
        functools.partial(section_kernel, sizes, span),
        out_shape=[VMEM(theta.shape, single)] * 2,
        in_specs=[pl.BlockSpec(memory_space=pltpu.SMEM)] * 2 + [pl.BlockSpec(memory_space=pltpu.HBM)] * 7,
        out_specs=whole_vmem(2),
        scratch_shapes=[
            VMEM(spectrum.shape, single),
            VMEM(theta.shape, single),
            VMEM(theta.shape, single),
            VMEM((taps, cells), jnp.int32),
            VMEM((taps, cells), single),
            VMEM(twist.shape, single),
            VMEM((2 * far, 2 * LANES), jnp.bfloat16),
            VMEM(modes_shape, single),
            VMEM(modes_shape, single),
            VMEM((2 * slabs, 2 * group, LANES), single),
            VMEM((far, group, LANES), single),
            VMEM(seg_shape, single),
            VMEM(seg_shape, single),
            VMEM((cells // LANES, span * LANES, LANES), jnp.bfloat16),
            VMEM((cells // LANES, span * LANES, LANES), jnp.bfloat16),
            VMEM((3 * lines, span * LANES), single),
            VMEM((6 * lines, span * LANES), jnp.bfloat16),
            VMEM((2, lines, cells), single),
            VMEM((lines, cells), single),
            VMEM((lines, cells), single),
            VMEM((lines + 2 * HALO * depth, cells + 2 * LANES), single),
            VMEM(theta.shape, single),
            VMEM(theta.shape, single),
            pltpu.SemaphoreType.DMA((9,)),
            pltpu.SemaphoreType.DMA((2, 3, gz)),
            pltpu.SemaphoreType.DMA((2, 3, gx - 1)),
            pltpu.SemaphoreType.DMA((2, 4)),
            pltpu.SemaphoreType.DMA((2, 2, tiles)),
        ],
        compiler_params=pltpu.CompilerParams(
            collective_id=0, has_side_effects=True, vmem_limit_bytes=60 * 1024 * 1024
        ),
        name="section",
    )(
        seg_offset, seg_length, spectrum, theta, section_sum, stencil_index, stencil_weight,
        jnp.asarray(twist), jnp.asarray(np.concatenate([top, rest], axis=0)),
    )
    return tuple(
        pl.pallas_call(
            put,
            out_shape=[jax.ShapeDtypeStruct(theta.shape, single)] * 2,
            in_specs=[pl.BlockSpec(memory_space=pl.ANY)] * 2,
            out_specs=[pl.BlockSpec(memory_space=pltpu.HBM)] * 2,
            scratch_shapes=[pltpu.SemaphoreType.DMA((2,))],
            compiler_params=pltpu.CompilerParams(vmem_limit_bytes=1024 * 1024),
            name="put",
        )(*held)
    )


def solution(mesh):
    placed = (
        P(None, None, ("gy", "gx"), None, "gz"),
        P("gy", "gz", "gx"),
        P("gy", "gz", "gx"),
        P(),
        P(),
        P(),
        P(),
    )
    return jax.shard_map(
        body,
        mesh=mesh,
        in_specs=placed,
        out_specs=(P("gy", "gz", "gx"), P("gy", "gz", "gx")),
        check_vma=False,
    )
```

```python
import functools
import math

import jax
import jax.numpy as jnp
import numpy as np
from jax import lax
from jax.experimental import pallas as pl
from jax.experimental.pallas import tpu as pltpu
from jax.sharding import PartitionSpec as P

MESH = pl.DeviceIdType.MESH
VMEM = pltpu.VMEM
LANES = 128
HALO = 4
TILE = 8
WIDTH = 512

first_coeffs = (0.8, -0.2, 4.0 / 105.0, -1.0 / 280.0)
second_coeffs = (1.6, -0.2, 8.0 / 315.0, -1.0 / 560.0)
center_coeff = -205.0 / 72.0
diffusivity = 0.15
time_step = 0.4
section_keep = -5.0 / 9.0
section_gain = 15.0 / 16.0


def whole_vmem(count):
    return [pl.BlockSpec(memory_space=VMEM)] * count


def rotate(value, turn):
    re, im = value
    cosine, sine = math.cos(2 * math.pi * turn), math.sin(2 * math.pi * turn)
    quarter = turn * 4 % 4
    if quarter == 0:
        return re, im
    if quarter == 1:
        return -im, re
    if quarter == 2:
        return -re, -im
    if quarter == 3:
        return im, -re
    return re * cosine - im * sine, re * sine + im * cosine


def fft(values):
    count = len(values)
    if count == 1:
        return values
    even = fft(values[0::2])
    odd = fft(values[1::2])
    low, high = [], []
    for x in range(count // 2):
        re, im = rotate(odd[x], x / count)
        low.append((even[x][0] + re, even[x][1] + im))
        high.append((even[x][0] - re, even[x][1] - im))
    return low + high


def split(value):
    top = value.astype(jnp.bfloat16)
    return top, (value - top.astype(jnp.float32)).astype(jnp.bfloat16)


def section_kernel(
    sizes, span,
    offset_ref, length_ref, spec_hbm, theta_hbm, sum_hbm, index_hbm, weight_hbm, twist_hbm, last_hbm,
    theta_out, sum_out,
    spec_ref, theta_ref, sum_ref, index_ref, weight_ref, twist_ref, last_ref,
    modes_send, modes_recv, mixed, velocity, seg_send, seg_recv, matrix_top, matrix_rest, gathered, values,
    grads, part, drift, field, z_back, z_front,
    load_sems, modes_sems, seg_sems, face_sems, deep_sems, meet_sems,
):
    gx, gy, gz = sizes
    here = {axis: lax.axis_index(axis) for axis in ("gx", "gy", "gz")}
    counts = dict(gx=gx, gy=gy, gz=gz)
    ahead = {axis: {axis: lax.rem(here[axis] + 1, counts[axis])} for axis in here}
    behind = {axis: {axis: lax.rem(here[axis] + counts[axis] - 1, counts[axis])} for axis in here}
    me, layer = here["gx"], here["gz"]
    rows, depth, cells = theta_ref.shape
    _, _, own_rows, all_depth, modes = spec_ref.shape
    local_slabs = modes // LANES
    group = own_rows * depth
    slabs = gz * local_slabs
    near = 2 * slabs
    far = 2 * slabs
    taps = index_ref.shape[0]
    lines = rows * depth
    tiles = lines // TILE
    skirt = HALO * depth

    own_columns = pl.ds(pl.multiple_of(me * cells, LANES), cells)
    loads = [
        pltpu.make_async_copy(source, place, load_sems.at[number])
        for number, (source, place) in enumerate(
            [
                (spec_hbm.at[0], spec_ref.at[0]),
                (spec_hbm.at[1], spec_ref.at[1]),
                (spec_hbm.at[2], spec_ref.at[2]),
                (theta_hbm, theta_ref),
                (index_hbm.at[:, own_columns], index_ref),
                (weight_hbm.at[:, own_columns], weight_ref),
                (twist_hbm, twist_ref),
                (last_hbm, last_ref),
                (sum_hbm, sum_ref),
            ]
        )
    ]
    for load in loads:
        load.start()

    barrier = pltpu.get_barrier_semaphore()
    has_up, has_down = layer < gz - 1, layer > 0
    inner = jnp.logical_and(has_up, has_down)
    per_tile = TILE // depth

    def signal(semaphore, target):
        pl.semaphore_signal(semaphore, inc=1, device_id=target, device_id_type=MESH)

    hub = layer == 0
    column = [{"gz": lax.rem(layer + step, gz)} for step in range(1, gz)]
    beside = [{"gx": lax.rem(me + step, gx)} for step in range(1, gx)] + [ahead["gy"], behind["gy"]]
    for target in column:
        signal(barrier, target)

    @pl.when(hub)
    def _():
        for target in beside:
            signal(barrier, target)
        pl.semaphore_wait(barrier, len(column) + len(beside))
        for target in beside:
            signal(meet_sems.at[0], target)

    @pl.when(jnp.logical_not(hub))
    def _():
        pl.semaphore_wait(barrier, len(column))

    def modes_copy(comp, target):
        return pltpu.make_async_remote_copy(
            src_ref=modes_send.at[comp, target],
            dst_ref=modes_recv.at[comp, layer],
            send_sem=modes_sems.at[0, comp, target],
            recv_sem=modes_sems.at[1, comp, layer],
            device_id={"gz": target},
            device_id_type=MESH,
        )

    def modes_wait(comp, other):
        pltpu.make_async_remote_copy(
            src_ref=modes_send.at[comp, other],
            dst_ref=modes_recv.at[comp, other],
            send_sem=modes_sems.at[0, comp, other],
            recv_sem=modes_sems.at[1, comp, other],
            device_id={"gz": other},
            device_id_type=MESH,
        ).wait()

    def send_modes(comp, distance):
        @pl.when(layer + distance < gz)
        def _():
            modes_copy(comp, layer + distance).start()

        @pl.when(layer >= distance)
        def _():
            modes_copy(comp, layer - distance).start()

    def deep_copy(way, tile):
        part_of = pl.ds(tile * per_tile, per_tile)
        return pltpu.make_async_remote_copy(
            src_ref=theta_hbm.at[part_of],
            dst_ref=(z_back, z_front)[way].at[part_of],
            send_sem=deep_sems.at[0, way, tile],
            recv_sem=deep_sems.at[1, way, tile],
            device_id=(ahead, behind)[way]["gz"],
            device_id_type=MESH,
        )

    def send_near(chosen):
        @pl.when(has_up)
        def _():
            for tile in chosen:
                deep_copy(0, tile).start()

        @pl.when(has_down)
        def _():
            for tile in chosen:
                deep_copy(1, tile).start()

    for comp in range(3):
        loads[comp].wait()
        for slab in range(local_slabs):
            for part_of in range(2):
                for row in range(own_rows):
                    held = spec_ref[comp, part_of, row, :, slab * LANES : (slab + 1) * LANES]
                    at = part_of * group + row * depth
                    for peer in range(gz):
                        modes_send[comp, peer, slab, at : at + depth, :] = held[
                            peer * depth : (peer + 1) * depth
                        ]
        for distance in range(gz - 1, 0, -1):
            send_modes(comp, distance)
    send_near(range(tiles))

    @pl.when(jnp.logical_not(inner))
    def _():
        @pl.when(jnp.logical_not(has_up))
        def _():
            for tile in range(tiles):
                deep_copy(0, tile).start()

        @pl.when(jnp.logical_not(has_down))
        def _():
            for tile in range(tiles):
                deep_copy(1, tile).start()

    def seg_copy(comp, step):
        target = lax.rem(me + step, gx)
        return pltpu.make_async_remote_copy(
            src_ref=seg_send.at[comp, target],
            dst_ref=seg_recv.at[comp, me],
            send_sem=seg_sems.at[0, comp, step - 1],
            recv_sem=seg_sems.at[1, comp, step - 1],
            device_id={"gx": target},
            device_id_type=MESH,
        )

    loads[3].wait()
    for tile in range(tiles):
        at = skirt + tile * TILE
        for half in range(per_tile):
            field[at + half * depth : at + (half + 1) * depth, LANES : LANES + cells] = theta_ref[
                tile * (per_tile) + half
            ]

    mine = pl.ds(skirt, lines)
    middle = pl.ds(LANES, cells)
    faces = [
        pltpu.make_async_remote_copy(
            src_ref=field.at[source],
            dst_ref=field.at[place],
            send_sem=face_sems.at[0, number],
            recv_sem=face_sems.at[1, number],
            device_id=device,
            device_id_type=MESH,
        )
        for number, (source, place, device) in enumerate(
            [
                ((mine, pl.ds(cells, LANES)), (mine, pl.ds(0, LANES)), ahead["gx"]),
                ((mine, pl.ds(LANES, LANES)), (mine, pl.ds(LANES + cells, LANES)), behind["gx"]),
                ((pl.ds(lines, skirt), middle), (pl.ds(0, skirt), middle), ahead["gy"]),
                ((pl.ds(skirt, skirt), middle), (pl.ds(skirt + lines, skirt), middle), behind["gy"]),
            ]
        )
    ]

    for comp in range(3):
        modes_recv[comp, layer] = modes_send[comp, layer]

    loads[4].wait()
    loads[5].wait()
    live_count = length_ref[me]
    begin = offset_ref[me] - jnp.minimum(offset_ref[me] // LANES, far - span) * LANES
    counter = lax.broadcasted_iota(jnp.int32, (LANES, LANES), 0).astype(jnp.float32).astype(jnp.bfloat16)
    counters = [counter[step : step + 16] for step in range(0, LANES, 16)]

    def spread(row):
        return jnp.broadcast_to(row, (16, LANES)).astype(jnp.bfloat16)

    def build(chunk, carry):
        columns = pl.ds(pl.multiple_of(chunk * LANES, LANES), LANES)
        index = index_ref[:, columns]
        live = index < live_count
        weight = jnp.where(live, weight_ref[:, columns], 0.0)
        merged = jnp.zeros_like(weight)
        for tap in range(taps):
            merged = merged + jnp.where(index == index[tap : tap + 1], weight[tap : tap + 1], 0.0)
        high, low = split(merged)
        high, low = high.astype(jnp.float32), low.astype(jnp.float32)
        place = jnp.where(live, index + begin, -1)
        owner = (place >> 7).astype(jnp.float32)
        within = (place & (LANES - 1)).astype(jnp.float32)
        tops = [spread(high[tap : tap + 1]) for tap in range(taps)]
        rests = [spread(low[tap : tap + 1]) for tap in range(taps)]
        owners = [spread(owner[tap : tap + 1]) for tap in range(taps)]
        withins = [spread(within[tap : tap + 1]) for tap in range(taps)]

        def slab_of(slab, inner):
            number = jnp.full((16, LANES), slab, jnp.int32).astype(jnp.float32).astype(jnp.bfloat16)
            close = [
                jnp.where(owners[tap] == number, withins[tap], jnp.bfloat16(-1)) for tap in range(taps)
            ]
            for step in range(LANES // 16):
                top = jnp.zeros((16, LANES), jnp.bfloat16)
                rest = jnp.zeros((16, LANES), jnp.bfloat16)
                for tap in range(taps):
                    hit = counters[step] == close[tap]
                    top = jnp.where(hit, tops[tap], top)
                    rest = jnp.where(hit, rests[tap], rest)
                at = pl.ds(pl.multiple_of(slab * LANES + step * 16, 16), 16)
                matrix_top[chunk, at, :] = top
                matrix_rest[chunk, at, :] = rest
            return inner

        return lax.fori_loop(0, span, slab_of, carry)

    chunks = cells // LANES
    step_of = chunks // 8
    early = chunks - 4 * step_of
    first = chunks * 4 // 16
    lax.fori_loop(0, first, build, 0)

    @pl.when(hub)
    def _():
        pl.semaphore_wait(meet_sems.at[0], len(beside))
        for target in column:
            signal(meet_sems.at[1], target)

    lax.fori_loop(first, early, build, 0)

    @pl.when(jnp.logical_not(hub))
    def _():
        pl.semaphore_wait(meet_sems.at[1], 1)

    for face in faces:
        face.start()

    loads[6].wait()
    loads[7].wait()
    last_both = last_ref[...]
    last_top = last_both[:far]
    dims = (((1,), (1,)), ((), ()))

    def twisted(line):
        re, im = mixed[:, line, :], mixed[:, group + line, :]
        pieces = []
        for quarter in range(LANES // near):
            part_of = slice(quarter * near, (quarter + 1) * near)
            cosine, sine = twist_ref[0, part_of, :], twist_ref[1, part_of, :]
            pieces.append(jnp.concatenate([re * cosine - im * sine, re * sine + im * cosine], axis=1))
        return jnp.concatenate(pieces, axis=0)

    def transform(comp, carry):
        lax.fori_loop(early + comp * step_of, early + (comp + 1) * step_of, build, 0)
        for step in range(1, gz):
            modes_wait(comp, lax.rem(layer + step, gz))

        def arrived(k):
            held = modes_recv[comp, k // local_slabs, k % local_slabs]
            return held[:group], held[group:]

        for parity in range(2):
            mixes = fft([rotate(arrived(k), parity * k / near) for k in range(slabs)])
            for x in range(slabs):
                mixed[2 * x + parity, 0:group, :] = mixes[x][0]
                mixed[2 * x + parity, group:, :] = mixes[x][1]
        for pair in range(group // 2):
            turned = jnp.concatenate([twisted(2 * pair), twisted(2 * pair + 1)], axis=0)
            top, rest = split(turned)
            first = lax.dot_general(last_both, top, dims, preferred_element_type=jnp.float32)
            second = lax.dot_general(last_top, rest, dims, preferred_element_type=jnp.float32)
            total = first[:far] + (first[far:] + second)
            velocity[:, 2 * pair, :] = total[:, :LANES]
            velocity[:, 2 * pair + 1, :] = total[:, LANES:]
        for block in range(gx):
            start = jnp.minimum(offset_ref[block] // LANES, far - span)
            seg_send[comp, block] = velocity[pl.ds(start, span)]
        for step in range(1, gx):
            seg_copy(comp, step).start()
        seg_recv[comp, me] = seg_send[comp, me]
        return carry

    lax.fori_loop(0, 3, transform, 0)
    lax.fori_loop(early + 3 * step_of, chunks, build, 0)

    loads[8].wait()
    for tile in range(tiles):
        for half in range(per_tile):
            at = tile * TILE + half * depth
            part[at : at + depth, :] = section_keep * sum_ref[tile * (per_tile) + half]
    for face in faces:
        face.wait()
    width = min(WIDTH, cells)
    wide_width = width + 2 * LANES
    low_half = lax.broadcasted_iota(jnp.int32, (TILE, width), 0) < depth

    def plane(block, carry):
        columns = pl.ds(pl.multiple_of(block * width, LANES), width)
        inner = pl.ds(pl.multiple_of(block * width + LANES, LANES), width)
        around = pl.ds(pl.multiple_of(block * width, LANES), wide_width)
        for tile in range(tiles):
            stack = [field[(tile + step) * TILE : (tile + step + 1) * TILE, inner] for step in range(5)]
            turned = [pltpu.roll(held, depth, 0) for held in stack]
            between = [jnp.where(low_half, turned[step], turned[step + 1]) for step in range(4)]
            behind_y = [between[1], stack[1], between[0], stack[0]]
            ahead_y = [between[2], stack[3], between[3], stack[4]]
            wide = field[skirt + tile * TILE : skirt + (tile + 1) * TILE, around]
            grad_x = jnp.zeros((TILE, width), jnp.float32)
            grad_y = jnp.zeros((TILE, width), jnp.float32)
            partial = 3.0 * center_coeff * stack[2]
            for reach in range(1, 5):
                ahead_x = pltpu.roll(wide, wide_width - reach, 1)[:, LANES : LANES + width]
                behind_x = pltpu.roll(wide, reach, 1)[:, LANES : LANES + width]
                up, down = ahead_y[reach - 1], behind_y[reach - 1]
                grad_x = grad_x + first_coeffs[reach - 1] * (ahead_x - behind_x)
                grad_y = grad_y + first_coeffs[reach - 1] * (up - down)
                partial = partial + second_coeffs[reach - 1] * ((ahead_x + behind_x) + (up + down))
            at = slice(tile * TILE, (tile + 1) * TILE)
            grads[0, at, columns] = grad_x
            grads[1, at, columns] = grad_y
            part[at, columns] = part[at, columns] + (time_step * diffusivity) * partial
        return carry

    lax.fori_loop(0, cells // width, plane, 0)

    for comp in range(3):
        for step in range(1, gx):
            seg_copy(comp, step).wait()
    for comp in range(3):
        for block in range(gx):
            at = (comp * gx + block) * group
            for slab in range(span):
                gathered[at : at + group, slab * LANES : (slab + 1) * LANES] = seg_recv[comp, block, slab]
    total = 3 * lines
    top, rest = split(gathered[...])
    values[0:total, :] = top
    values[total:, :] = rest

    def combine(pair, carry):
        top = jnp.concatenate([matrix_top[2 * pair], matrix_top[2 * pair + 1]], axis=1)
        rest = jnp.concatenate([matrix_rest[2 * pair], matrix_rest[2 * pair + 1]], axis=1)
        first = jnp.dot(values[...], top, preferred_element_type=jnp.float32)
        second = jnp.dot(values[0:total, :], rest, preferred_element_type=jnp.float32)
        moved = first[:total] + (first[total:] + second)
        columns = pl.ds(pl.multiple_of(pair * 2 * LANES, 2 * LANES), 2 * LANES)
        carried = moved[:lines] * grads[0, :, columns] + moved[lines : 2 * lines] * grads[1, :, columns]
        part[:, columns] = part[:, columns] - time_step * carried
        drift[:, columns] = time_step * moved[2 * lines :]
        return carry

    lax.fori_loop(0, cells // (2 * LANES), combine, 0)

    place_of = lax.rem(lax.broadcasted_iota(jnp.int32, (TILE, width), 0), depth)
    for tile in range(tiles):
        for way in range(2):
            deep_copy(way, tile).wait()
        at = slice(tile * TILE, (tile + 1) * TILE)

        def finish(block, carry):
            columns = pl.ds(pl.multiple_of(block * width, LANES), width)
            inner = pl.ds(pl.multiple_of(block * width + LANES, LANES), width)
            own = field[skirt + tile * TILE : skirt + (tile + 1) * TILE, inner]
            back, front = (
                jnp.concatenate([held[tile * per_tile + half, :, columns] for half in range(per_tile)], axis=0)
                for held in (z_back, z_front)
            )
            grad_z = jnp.zeros((TILE, width), jnp.float32)
            partial = jnp.zeros((TILE, width), jnp.float32)
            for reach in range(1, 5):
                up, down = front, back
                if reach < HALO:
                    up = jnp.where(
                        place_of < depth - reach, pltpu.roll(own, TILE - reach, 0), pltpu.roll(front, depth - reach, 0)
                    )
                    down = jnp.where(
                        place_of >= reach, pltpu.roll(own, reach, 0), pltpu.roll(back, depth + reach, 0)
                    )
                grad_z = grad_z + first_coeffs[reach - 1] * (up - down)
                partial = partial + second_coeffs[reach - 1] * (up + down)
            after = (part[at, columns] + (time_step * diffusivity) * partial) - drift[at, columns] * grad_z
            later = own + section_gain * after
            for half in range(per_tile):
                row, piece = tile * (per_tile) + half, slice(half * depth, (half + 1) * depth)
                sum_out[row, :, columns] = after[piece]
                theta_out[row, :, columns] = later[piece]
            return carry

        lax.fori_loop(0, cells // width, finish, 0)


def put(theta_ref, sum_ref, theta_out, sum_out, sems):
    copies = [
        pltpu.make_async_copy(theta_ref, theta_out, sems.at[0]),
        pltpu.make_async_copy(sum_ref, sum_out, sems.at[1]),
    ]
    for copy in copies:
        copy.start()
    for copy in copies:
        copy.wait()


def body(spectrum, theta, section_sum, seg_offset, seg_length, stencil_index, stencil_weight):
    sizes = tuple(lax.axis_size(axis) for axis in ("gx", "gy", "gz"))
    gx, _, gz = sizes
    _, _, own_rows, all_depth, modes = spectrum.shape
    rows, depth, cells = theta.shape
    taps = stencil_index.shape[0]
    assert depth == HALO and rows * depth % TILE == 0 and cells % min(WIDTH, cells) == 0
    group = own_rows * depth
    slabs = gz * modes // LANES
    length = 2 * slabs * LANES
    far = length // LANES
    span = min(3 * length // (2 * gx) // LANES + 1, far)
    k = np.arange(LANES)
    turn = 2 * np.pi * (np.outer(k, k) % length) / length
    twist = np.stack([np.cos(turn), np.sin(turn)]).astype(np.float32)
    turn = 2 * np.pi * (np.outer(np.arange(far), k) % far) / far
    last = np.concatenate([np.cos(turn), -np.sin(turn)], axis=1).astype(np.float32)
    top = last.astype(jnp.bfloat16)
    rest = (last - top.astype(np.float32)).astype(jnp.bfloat16)
    modes_shape = (3, gz, modes // LANES, 2 * group, LANES)
    seg_shape = (3, gx, span, group, LANES)
    lines = rows * depth
    tiles = lines // TILE
    single = jnp.float32
    held = pl.pallas_call(
        functools.partial(section_kernel, sizes, span),
        out_shape=[VMEM(theta.shape, single)] * 2,
        in_specs=[pl.BlockSpec(memory_space=pltpu.SMEM)] * 2 + [pl.BlockSpec(memory_space=pltpu.HBM)] * 7,
        out_specs=whole_vmem(2),
        scratch_shapes=[
            VMEM(spectrum.shape, single),
            VMEM(theta.shape, single),
            VMEM(theta.shape, single),
            VMEM((taps, cells), jnp.int32),
            VMEM((taps, cells), single),
            VMEM(twist.shape, single),
            VMEM((2 * far, 2 * LANES), jnp.bfloat16),
            VMEM(modes_shape, single),
            VMEM(modes_shape, single),
            VMEM((2 * slabs, 2 * group, LANES), single),
            VMEM((far, group, LANES), single),
            VMEM(seg_shape, single),
            VMEM(seg_shape, single),
            VMEM((cells // LANES, span * LANES, LANES), jnp.bfloat16),
            VMEM((cells // LANES, span * LANES, LANES), jnp.bfloat16),
            VMEM((3 * lines, span * LANES), single),
            VMEM((6 * lines, span * LANES), jnp.bfloat16),
            VMEM((2, lines, cells), single),
            VMEM((lines, cells), single),
            VMEM((lines, cells), single),
            VMEM((lines + 2 * HALO * depth, cells + 2 * LANES), single),
            VMEM(theta.shape, single),
            VMEM(theta.shape, single),
            pltpu.SemaphoreType.DMA((9,)),
            pltpu.SemaphoreType.DMA((2, 3, gz)),
            pltpu.SemaphoreType.DMA((2, 3, gx - 1)),
            pltpu.SemaphoreType.DMA((2, 4)),
            pltpu.SemaphoreType.DMA((2, 2, tiles)),
            pltpu.SemaphoreType.REGULAR((2,)),
        ],
        compiler_params=pltpu.CompilerParams(
            collective_id=0, has_side_effects=True, vmem_limit_bytes=60 * 1024 * 1024
        ),
        name="section",
    )(
        seg_offset, seg_length, spectrum, theta, section_sum, stencil_index, stencil_weight,
        jnp.asarray(twist), jnp.asarray(np.concatenate([top, rest], axis=0)),
    )
    return tuple(
        pl.pallas_call(
            put,
            out_shape=[jax.ShapeDtypeStruct(theta.shape, single)] * 2,
            in_specs=[pl.BlockSpec(memory_space=pl.ANY)] * 2,
            out_specs=[pl.BlockSpec(memory_space=pltpu.HBM)] * 2,
            scratch_shapes=[pltpu.SemaphoreType.DMA((2,))],
            compiler_params=pltpu.CompilerParams(vmem_limit_bytes=1024 * 1024),
            name="put",
        )(*held)
    )


def solution(mesh):
    placed = (
        P(None, None, ("gy", "gx"), None, "gz"),
        P("gy", "gz", "gx"),
        P("gy", "gz", "gx"),
        P(),
        P(),
        P(),
        P(),
    )
    return jax.shard_map(
        body,
        mesh=mesh,
        in_specs=placed,
        out_specs=(P("gy", "gz", "gx"), P("gy", "gz", "gx")),
        check_vma=False,
    )
```

```python
import functools
import math

import jax
import jax.numpy as jnp
import numpy as np
from jax import lax
from jax.experimental import pallas as pl
from jax.experimental.pallas import tpu as pltpu
from jax.sharding import PartitionSpec as P

MESH = pl.DeviceIdType.MESH
VMEM = pltpu.VMEM
LANES = 128
HALO = 4
TILE = 8
WIDTH = 512

first_coeffs = (0.8, -0.2, 4.0 / 105.0, -1.0 / 280.0)
second_coeffs = (1.6, -0.2, 8.0 / 315.0, -1.0 / 560.0)
center_coeff = -205.0 / 72.0
diffusivity = 0.15
time_step = 0.4
section_keep = -5.0 / 9.0
section_gain = 15.0 / 16.0


def whole_vmem(count):
    return [pl.BlockSpec(memory_space=VMEM)] * count


def rotate(value, turn):
    re, im = value
    cosine, sine = math.cos(2 * math.pi * turn), math.sin(2 * math.pi * turn)
    quarter = turn * 4 % 4
    if quarter == 0:
        return re, im
    if quarter == 1:
        return -im, re
    if quarter == 2:
        return -re, -im
    if quarter == 3:
        return im, -re
    return re * cosine - im * sine, re * sine + im * cosine


def fft(values):
    count = len(values)
    if count == 1:
        return values
    even = fft(values[0::2])
    odd = fft(values[1::2])
    low, high = [], []
    for x in range(count // 2):
        re, im = rotate(odd[x], x / count)
        low.append((even[x][0] + re, even[x][1] + im))
        high.append((even[x][0] - re, even[x][1] - im))
    return low + high


def split(value):
    top = value.astype(jnp.bfloat16)
    return top, (value - top.astype(jnp.float32)).astype(jnp.bfloat16)


def section_kernel(
    sizes, span,
    offset_ref, length_ref, spec_hbm, theta_hbm, sum_hbm, index_hbm, weight_hbm, twist_hbm, last_hbm,
    theta_out, sum_out,
    spec_ref, theta_ref, sum_ref, index_ref, weight_ref, twist_ref, last_ref,
    modes_send, modes_recv, mixed, velocity, seg_send, seg_recv, matrix_top, matrix_rest, gathered, values,
    grads, part, drift, field, z_back, z_front,
    load_sems, modes_sems, seg_sems, face_sems, deep_sems, meet_sems,
):
    gx, gy, gz = sizes
    here = {axis: lax.axis_index(axis) for axis in ("gx", "gy", "gz")}
    counts = dict(gx=gx, gy=gy, gz=gz)
    ahead = {axis: {axis: lax.rem(here[axis] + 1, counts[axis])} for axis in here}
    behind = {axis: {axis: lax.rem(here[axis] + counts[axis] - 1, counts[axis])} for axis in here}
    me, layer = here["gx"], here["gz"]
    rows, depth, cells = theta_ref.shape
    _, _, own_rows, all_depth, modes = spec_ref.shape
    local_slabs = modes // LANES
    group = own_rows * depth
    slabs = gz * local_slabs
    near = 2 * slabs
    far = 2 * slabs
    taps = index_ref.shape[0]
    lines = rows * depth
    tiles = lines // TILE
    skirt = HALO * depth

    own_columns = pl.ds(pl.multiple_of(me * cells, LANES), cells)
    loads = [
        pltpu.make_async_copy(source, place, load_sems.at[number])
        for number, (source, place) in enumerate(
            [
                (spec_hbm.at[0], spec_ref.at[0]),
                (spec_hbm.at[1], spec_ref.at[1]),
                (spec_hbm.at[2], spec_ref.at[2]),
                (theta_hbm, theta_ref),
                (index_hbm.at[:, own_columns], index_ref),
                (weight_hbm.at[:, own_columns], weight_ref),
                (twist_hbm, twist_ref),
                (last_hbm, last_ref),
                (sum_hbm, sum_ref),
            ]
        )
    ]
    for load in loads:
        load.start()

    barrier = pltpu.get_barrier_semaphore()
    has_up, has_down = layer < gz - 1, layer > 0
    inner = jnp.logical_and(has_up, has_down)
    per_tile = TILE // depth

    def signal(semaphore, target):
        pl.semaphore_signal(semaphore, inc=1, device_id=target, device_id_type=MESH)

    hub = layer == 0
    column = [{"gz": lax.rem(layer + step, gz)} for step in range(1, gz)]
    beside = [{"gx": lax.rem(me + step, gx)} for step in range(1, gx)] + [ahead["gy"], behind["gy"]]
    for target in column:
        signal(barrier, target)

    @pl.when(hub)
    def _():
        for target in beside:
            signal(barrier, target)
        pl.semaphore_wait(barrier, len(column) + len(beside))
        for target in beside:
            signal(meet_sems.at[0], target)

    @pl.when(jnp.logical_not(hub))
    def _():
        pl.semaphore_wait(barrier, len(column))

    def modes_copy(comp, target):
        return pltpu.make_async_remote_copy(
            src_ref=modes_send.at[comp, target],
            dst_ref=modes_recv.at[comp, layer],
            send_sem=modes_sems.at[0, comp, target],
            recv_sem=modes_sems.at[1, comp, layer],
            device_id={"gz": target},
            device_id_type=MESH,
        )

    def modes_wait(comp, other):
        pltpu.make_async_remote_copy(
            src_ref=modes_send.at[comp, other],
            dst_ref=modes_recv.at[comp, other],
            send_sem=modes_sems.at[0, comp, other],
            recv_sem=modes_sems.at[1, comp, other],
            device_id={"gz": other},
            device_id_type=MESH,
        ).wait()

    def send_modes(comp, distance):
        @pl.when(layer + distance < gz)
        def _():
            modes_copy(comp, layer + distance).start()

        @pl.when(layer >= distance)
        def _():
            modes_copy(comp, layer - distance).start()

    def deep_copy(way, tile):
        part_of = pl.ds(tile * per_tile, per_tile)
        return pltpu.make_async_remote_copy(
            src_ref=theta_hbm.at[part_of],
            dst_ref=(z_back, z_front)[way].at[part_of],
            send_sem=deep_sems.at[0, way, tile],
            recv_sem=deep_sems.at[1, way, tile],
            device_id=(ahead, behind)[way]["gz"],
            device_id_type=MESH,
        )

    def send_near(chosen):
        @pl.when(has_up)
        def _():
            for tile in chosen:
                deep_copy(0, tile).start()

        @pl.when(has_down)
        def _():
            for tile in chosen:
                deep_copy(1, tile).start()

    for comp in range(3):
        loads[comp].wait()
        for slab in range(local_slabs):
            for part_of in range(2):
                for row in range(own_rows):
                    held = spec_ref[comp, part_of, row, :, slab * LANES : (slab + 1) * LANES]
                    at = part_of * group + row * depth
                    for peer in range(gz):
                        modes_send[comp, peer, slab, at : at + depth, :] = held[
                            peer * depth : (peer + 1) * depth
                        ]
        for distance in range(gz - 1, 0, -1):
            send_modes(comp, distance)
    send_near(range(tiles))

    @pl.when(jnp.logical_not(inner))
    def _():
        @pl.when(jnp.logical_not(has_up))
        def _():
            for tile in range(tiles):
                deep_copy(0, tile).start()

        @pl.when(jnp.logical_not(has_down))
        def _():
            for tile in range(tiles):
                deep_copy(1, tile).start()

    def seg_copy(comp, step):
        target = lax.rem(me + step, gx)
        return pltpu.make_async_remote_copy(
            src_ref=seg_send.at[comp, target],
            dst_ref=seg_recv.at[comp, me],
            send_sem=seg_sems.at[0, comp, step - 1],
            recv_sem=seg_sems.at[1, comp, step - 1],
            device_id={"gx": target},
            device_id_type=MESH,
        )

    loads[3].wait()
    for tile in range(tiles):
        at = skirt + tile * TILE
        for half in range(per_tile):
            field[at + half * depth : at + (half + 1) * depth, LANES : LANES + cells] = theta_ref[
                tile * (per_tile) + half
            ]

    mine = pl.ds(skirt, lines)
    middle = pl.ds(LANES, cells)
    faces = [
        pltpu.make_async_remote_copy(
            src_ref=field.at[source],
            dst_ref=field.at[place],
            send_sem=face_sems.at[0, number],
            recv_sem=face_sems.at[1, number],
            device_id=device,
            device_id_type=MESH,
        )
        for number, (source, place, device) in enumerate(
            [
                ((mine, pl.ds(cells, LANES)), (mine, pl.ds(0, LANES)), ahead["gx"]),
                ((mine, pl.ds(LANES, LANES)), (mine, pl.ds(LANES + cells, LANES)), behind["gx"]),
                ((pl.ds(lines, skirt), middle), (pl.ds(0, skirt), middle), ahead["gy"]),
                ((pl.ds(skirt, skirt), middle), (pl.ds(skirt + lines, skirt), middle), behind["gy"]),
            ]
        )
    ]

    for comp in range(3):
        modes_recv[comp, layer] = modes_send[comp, layer]

    loads[4].wait()
    loads[5].wait()
    live_count = length_ref[me]
    begin = offset_ref[me] - jnp.minimum(offset_ref[me] // LANES, far - span) * LANES
    counter = lax.broadcasted_iota(jnp.int32, (LANES, LANES), 0).astype(jnp.float32).astype(jnp.bfloat16)
    counters = [counter[step : step + 16] for step in range(0, LANES, 16)]

    def spread(row):
        return jnp.broadcast_to(row, (16, LANES)).astype(jnp.bfloat16)

    def build(chunk, carry):
        columns = pl.ds(pl.multiple_of(chunk * LANES, LANES), LANES)
        index = index_ref[:, columns]
        live = index < live_count
        weight = jnp.where(live, weight_ref[:, columns], 0.0)
        merged = jnp.zeros_like(weight)
        for tap in range(taps):
            merged = merged + jnp.where(index == index[tap : tap + 1], weight[tap : tap + 1], 0.0)
        high, low = split(merged)
        high, low = high.astype(jnp.float32), low.astype(jnp.float32)
        place = jnp.where(live, index + begin, -1)
        owner = (place >> 7).astype(jnp.float32)
        within = (place & (LANES - 1)).astype(jnp.float32)
        tops = [spread(high[tap : tap + 1]) for tap in range(taps)]
        rests = [spread(low[tap : tap + 1]) for tap in range(taps)]
        owners = [spread(owner[tap : tap + 1]) for tap in range(taps)]
        withins = [spread(within[tap : tap + 1]) for tap in range(taps)]

        def slab_of(slab, inner):
            number = jnp.full((16, LANES), slab, jnp.int32).astype(jnp.float32).astype(jnp.bfloat16)
            close = [
                jnp.where(owners[tap] == number, withins[tap], jnp.bfloat16(-1)) for tap in range(taps)
            ]
            for step in range(LANES // 16):
                top = jnp.zeros((16, LANES), jnp.bfloat16)
                rest = jnp.zeros((16, LANES), jnp.bfloat16)
                for tap in range(taps):
                    hit = counters[step] == close[tap]
                    top = jnp.where(hit, tops[tap], top)
                    rest = jnp.where(hit, rests[tap], rest)
                at = pl.ds(pl.multiple_of(slab * LANES + step * 16, 16), 16)
                matrix_top[chunk, at, :] = top
                matrix_rest[chunk, at, :] = rest
            return inner

        return lax.fori_loop(0, span, slab_of, carry)

    chunks = cells // LANES
    step_of = chunks // 8
    early = chunks - 5 * step_of
    first = chunks * 4 // 16
    lax.fori_loop(0, first, build, 0)

    @pl.when(hub)
    def _():
        pl.semaphore_wait(meet_sems.at[0], len(beside))
        for target in column:
            signal(meet_sems.at[1], target)

    lax.fori_loop(first, early, build, 0)

    @pl.when(jnp.logical_not(hub))
    def _():
        pl.semaphore_wait(meet_sems.at[1], 1)

    for face in faces:
        face.start()

    loads[6].wait()
    loads[7].wait()
    last_both = last_ref[...]
    last_top = last_both[:far]
    dims = (((1,), (1,)), ((), ()))

    def twisted(line):
        re, im = mixed[:, line, :], mixed[:, group + line, :]
        pieces = []
        for quarter in range(LANES // near):
            part_of = slice(quarter * near, (quarter + 1) * near)
            cosine, sine = twist_ref[0, part_of, :], twist_ref[1, part_of, :]
            pieces.append(jnp.concatenate([re * cosine - im * sine, re * sine + im * cosine], axis=1))
        return jnp.concatenate(pieces, axis=0)

    def transform(comp, carry):
        lax.fori_loop(early + comp * step_of, early + (comp + 1) * step_of, build, 0)
        for step in range(1, gz):
            modes_wait(comp, lax.rem(layer + step, gz))

        def arrived(k):
            held = modes_recv[comp, k // local_slabs, k % local_slabs]
            return held[:group], held[group:]

        for parity in range(2):
            mixes = fft([rotate(arrived(k), parity * k / near) for k in range(slabs)])
            for x in range(slabs):
                mixed[2 * x + parity, 0:group, :] = mixes[x][0]
                mixed[2 * x + parity, group:, :] = mixes[x][1]
        for pair in range(group // 2):
            turned = jnp.concatenate([twisted(2 * pair), twisted(2 * pair + 1)], axis=0)
            top, rest = split(turned)
            first = lax.dot_general(last_both, top, dims, preferred_element_type=jnp.float32)
            second = lax.dot_general(last_top, rest, dims, preferred_element_type=jnp.float32)
            total = first[:far] + (first[far:] + second)
            velocity[:, 2 * pair, :] = total[:, :LANES]
            velocity[:, 2 * pair + 1, :] = total[:, LANES:]
        for block in range(gx):
            start = jnp.minimum(offset_ref[block] // LANES, far - span)
            seg_send[comp, block] = velocity[pl.ds(start, span)]
        for step in range(1, gx):
            seg_copy(comp, step).start()
        seg_recv[comp, me] = seg_send[comp, me]
        return carry

    lax.fori_loop(0, 3, transform, 0)
    lax.fori_loop(early + 3 * step_of, chunks, build, 0)

    loads[8].wait()
    for tile in range(tiles):
        for half in range(per_tile):
            at = tile * TILE + half * depth
            part[at : at + depth, :] = section_keep * sum_ref[tile * (per_tile) + half]
    for face in faces:
        face.wait()
    width = min(WIDTH, cells)
    wide_width = width + 2 * LANES
    low_half = lax.broadcasted_iota(jnp.int32, (TILE, width), 0) < depth

    def plane(block, carry):
        columns = pl.ds(pl.multiple_of(block * width, LANES), width)
        inner = pl.ds(pl.multiple_of(block * width + LANES, LANES), width)
        around = pl.ds(pl.multiple_of(block * width, LANES), wide_width)
        for tile in range(tiles):
            stack = [field[(tile + step) * TILE : (tile + step + 1) * TILE, inner] for step in range(5)]
            turned = [pltpu.roll(held, depth, 0) for held in stack]
            between = [jnp.where(low_half, turned[step], turned[step + 1]) for step in range(4)]
            behind_y = [between[1], stack[1], between[0], stack[0]]
            ahead_y = [between[2], stack[3], between[3], stack[4]]
            wide = field[skirt + tile * TILE : skirt + (tile + 1) * TILE, around]
            grad_x = jnp.zeros((TILE, width), jnp.float32)
            grad_y = jnp.zeros((TILE, width), jnp.float32)
            partial = 3.0 * center_coeff * stack[2]
            for reach in range(1, 5):
                ahead_x = pltpu.roll(wide, wide_width - reach, 1)[:, LANES : LANES + width]
                behind_x = pltpu.roll(wide, reach, 1)[:, LANES : LANES + width]
                up, down = ahead_y[reach - 1], behind_y[reach - 1]
                grad_x = grad_x + first_coeffs[reach - 1] * (ahead_x - behind_x)
                grad_y = grad_y + first_coeffs[reach - 1] * (up - down)
                partial = partial + second_coeffs[reach - 1] * ((ahead_x + behind_x) + (up + down))
            at = slice(tile * TILE, (tile + 1) * TILE)
            grads[0, at, columns] = grad_x
            grads[1, at, columns] = grad_y
            part[at, columns] = part[at, columns] + (time_step * diffusivity) * partial
        return carry

    lax.fori_loop(0, cells // width, plane, 0)

    for comp in range(3):
        for step in range(1, gx):
            seg_copy(comp, step).wait()
    for comp in range(3):
        for block in range(gx):
            at = (comp * gx + block) * group
            for slab in range(span):
                gathered[at : at + group, slab * LANES : (slab + 1) * LANES] = seg_recv[comp, block, slab]
    total = 3 * lines
    top, rest = split(gathered[...])
    values[0:total, :] = top
    values[total:, :] = rest

    def combine(pair, carry):
        top = jnp.concatenate([matrix_top[2 * pair], matrix_top[2 * pair + 1]], axis=1)
        rest = jnp.concatenate([matrix_rest[2 * pair], matrix_rest[2 * pair + 1]], axis=1)
        first = jnp.dot(values[...], top, preferred_element_type=jnp.float32)
        second = jnp.dot(values[0:total, :], rest, preferred_element_type=jnp.float32)
        moved = first[:total] + (first[total:] + second)
        columns = pl.ds(pl.multiple_of(pair * 2 * LANES, 2 * LANES), 2 * LANES)
        carried = moved[:lines] * grads[0, :, columns] + moved[lines : 2 * lines] * grads[1, :, columns]
        part[:, columns] = part[:, columns] - time_step * carried
        drift[:, columns] = time_step * moved[2 * lines :]
        return carry

    lax.fori_loop(0, cells // (2 * LANES), combine, 0)

    place_of = lax.rem(lax.broadcasted_iota(jnp.int32, (TILE, width), 0), depth)
    for tile in range(tiles):
        for way in range(2):
            deep_copy(way, tile).wait()
        at = slice(tile * TILE, (tile + 1) * TILE)

        def finish(block, carry):
            columns = pl.ds(pl.multiple_of(block * width, LANES), width)
            inner = pl.ds(pl.multiple_of(block * width + LANES, LANES), width)
            own = field[skirt + tile * TILE : skirt + (tile + 1) * TILE, inner]
            back, front = (
                jnp.concatenate([held[tile * per_tile + half, :, columns] for half in range(per_tile)], axis=0)
                for held in (z_back, z_front)
            )
            grad_z = jnp.zeros((TILE, width), jnp.float32)
            partial = jnp.zeros((TILE, width), jnp.float32)
            for reach in range(1, 5):
                up, down = front, back
                if reach < HALO:
                    up = jnp.where(
                        place_of < depth - reach, pltpu.roll(own, TILE - reach, 0), pltpu.roll(front, depth - reach, 0)
                    )
                    down = jnp.where(
                        place_of >= reach, pltpu.roll(own, reach, 0), pltpu.roll(back, depth + reach, 0)
                    )
                grad_z = grad_z + first_coeffs[reach - 1] * (up - down)
                partial = partial + second_coeffs[reach - 1] * (up + down)
            after = (part[at, columns] + (time_step * diffusivity) * partial) - drift[at, columns] * grad_z
            later = own + section_gain * after
            for half in range(per_tile):
                row, piece = tile * (per_tile) + half, slice(half * depth, (half + 1) * depth)
                sum_out[row, :, columns] = after[piece]
                theta_out[row, :, columns] = later[piece]
            return carry

        lax.fori_loop(0, cells // width, finish, 0)


def put(theta_ref, sum_ref, theta_out, sum_out, sems):
    copies = [
        pltpu.make_async_copy(theta_ref, theta_out, sems.at[0]),
        pltpu.make_async_copy(sum_ref, sum_out, sems.at[1]),
    ]
    for copy in copies:
        copy.start()
    for copy in copies:
        copy.wait()


def body(spectrum, theta, section_sum, seg_offset, seg_length, stencil_index, stencil_weight):
    sizes = tuple(lax.axis_size(axis) for axis in ("gx", "gy", "gz"))
    gx, _, gz = sizes
    _, _, own_rows, all_depth, modes = spectrum.shape
    rows, depth, cells = theta.shape
    taps = stencil_index.shape[0]
    assert depth == HALO and rows * depth % TILE == 0 and cells % min(WIDTH, cells) == 0
    group = own_rows * depth
    slabs = gz * modes // LANES
    length = 2 * slabs * LANES
    far = length // LANES
    span = min(3 * length // (2 * gx) // LANES + 1, far)
    k = np.arange(LANES)
    turn = 2 * np.pi * (np.outer(k, k) % length) / length
    twist = np.stack([np.cos(turn), np.sin(turn)]).astype(np.float32)
    turn = 2 * np.pi * (np.outer(np.arange(far), k) % far) / far
    last = np.concatenate([np.cos(turn), -np.sin(turn)], axis=1).astype(np.float32)
    top = last.astype(jnp.bfloat16)
    rest = (last - top.astype(np.float32)).astype(jnp.bfloat16)
    modes_shape = (3, gz, modes // LANES, 2 * group, LANES)
    seg_shape = (3, gx, span, group, LANES)
    lines = rows * depth
    tiles = lines // TILE
    single = jnp.float32
    held = pl.pallas_call(
        functools.partial(section_kernel, sizes, span),
        out_shape=[VMEM(theta.shape, single)] * 2,
        in_specs=[pl.BlockSpec(memory_space=pltpu.SMEM)] * 2 + [pl.BlockSpec(memory_space=pltpu.HBM)] * 7,
        out_specs=whole_vmem(2),
        scratch_shapes=[
            VMEM(spectrum.shape, single),
            VMEM(theta.shape, single),
            VMEM(theta.shape, single),
            VMEM((taps, cells), jnp.int32),
            VMEM((taps, cells), single),
            VMEM(twist.shape, single),
            VMEM((2 * far, 2 * LANES), jnp.bfloat16),
            VMEM(modes_shape, single),
            VMEM(modes_shape, single),
            VMEM((2 * slabs, 2 * group, LANES), single),
            VMEM((far, group, LANES), single),
            VMEM(seg_shape, single),
            VMEM(seg_shape, single),
            VMEM((cells // LANES, span * LANES, LANES), jnp.bfloat16),
            VMEM((cells // LANES, span * LANES, LANES), jnp.bfloat16),
            VMEM((3 * lines, span * LANES), single),
            VMEM((6 * lines, span * LANES), jnp.bfloat16),
            VMEM((2, lines, cells), single),
            VMEM((lines, cells), single),
            VMEM((lines, cells), single),
            VMEM((lines + 2 * HALO * depth, cells + 2 * LANES), single),
            VMEM(theta.shape, single),
            VMEM(theta.shape, single),
            pltpu.SemaphoreType.DMA((9,)),
            pltpu.SemaphoreType.DMA((2, 3, gz)),
            pltpu.SemaphoreType.DMA((2, 3, gx - 1)),
            pltpu.SemaphoreType.DMA((2, 4)),
            pltpu.SemaphoreType.DMA((2, 2, tiles)),
            pltpu.SemaphoreType.REGULAR((2,)),
        ],
        compiler_params=pltpu.CompilerParams(
            collective_id=0, has_side_effects=True, vmem_limit_bytes=60 * 1024 * 1024
        ),
        name="section",
    )(
        seg_offset, seg_length, spectrum, theta, section_sum, stencil_index, stencil_weight,
        jnp.asarray(twist), jnp.asarray(np.concatenate([top, rest], axis=0)),
    )
    return tuple(
        pl.pallas_call(
            put,
            out_shape=[jax.ShapeDtypeStruct(theta.shape, single)] * 2,
            in_specs=[pl.BlockSpec(memory_space=pl.ANY)] * 2,
            out_specs=[pl.BlockSpec(memory_space=pltpu.HBM)] * 2,
            scratch_shapes=[pltpu.SemaphoreType.DMA((2,))],
            compiler_params=pltpu.CompilerParams(vmem_limit_bytes=1024 * 1024),
            name="put",
        )(*held)
    )


def solution(mesh):
    placed = (
        P(None, None, ("gy", "gx"), None, "gz"),
        P("gy", "gz", "gx"),
        P("gy", "gz", "gx"),
        P(),
        P(),
        P(),
        P(),
    )
    return jax.shard_map(
        body,
        mesh=mesh,
        in_specs=placed,
        out_specs=(P("gy", "gz", "gx"), P("gy", "gz", "gx")),
        check_vma=False,
    )
```

```python
import functools
import math

import jax
import jax.numpy as jnp
import numpy as np
from jax import lax
from jax.experimental import pallas as pl
from jax.experimental.pallas import tpu as pltpu
from jax.sharding import PartitionSpec as P

MESH = pl.DeviceIdType.MESH
VMEM = pltpu.VMEM
LANES = 128
HALO = 4
TILE = 8
WIDTH = 512

first_coeffs = (0.8, -0.2, 4.0 / 105.0, -1.0 / 280.0)
second_coeffs = (1.6, -0.2, 8.0 / 315.0, -1.0 / 560.0)
center_coeff = -205.0 / 72.0
diffusivity = 0.15
time_step = 0.4
section_keep = -5.0 / 9.0
section_gain = 15.0 / 16.0


def whole_vmem(count):
    return [pl.BlockSpec(memory_space=VMEM)] * count


def rotate(value, turn):
    re, im = value
    cosine, sine = math.cos(2 * math.pi * turn), math.sin(2 * math.pi * turn)
    quarter = turn * 4 % 4
    if quarter == 0:
        return re, im
    if quarter == 1:
        return -im, re
    if quarter == 2:
        return -re, -im
    if quarter == 3:
        return im, -re
    return re * cosine - im * sine, re * sine + im * cosine


def fft(values):
    count = len(values)
    if count == 1:
        return values
    even = fft(values[0::2])
    odd = fft(values[1::2])
    low, high = [], []
    for x in range(count // 2):
        re, im = rotate(odd[x], x / count)
        low.append((even[x][0] + re, even[x][1] + im))
        high.append((even[x][0] - re, even[x][1] - im))
    return low + high


def split(value):
    top = value.astype(jnp.bfloat16)
    return top, (value - top.astype(jnp.float32)).astype(jnp.bfloat16)


def section_kernel(
    sizes, span,
    offset_hbm, length_hbm, spec_hbm, theta_hbm, sum_hbm, index_hbm, weight_hbm, twist_hbm, last_hbm,
    theta_out, sum_out,
    offset_ref, length_ref, spec_ref, theta_ref, sum_ref, index_ref, weight_ref, twist_ref, last_ref,
    modes_send, modes_recv, mixed, velocity, seg_send, seg_recv, matrix_top, matrix_rest, gathered, values,
    grads, part, drift, field, z_back, z_front,
    load_sems, modes_sems, seg_sems, face_sems, deep_sems, meet_sems,
):
    gx, gy, gz = sizes
    here = {axis: lax.axis_index(axis) for axis in ("gx", "gy", "gz")}
    counts = dict(gx=gx, gy=gy, gz=gz)
    ahead = {axis: {axis: lax.rem(here[axis] + 1, counts[axis])} for axis in here}
    behind = {axis: {axis: lax.rem(here[axis] + counts[axis] - 1, counts[axis])} for axis in here}
    me, layer = here["gx"], here["gz"]
    rows, depth, cells = theta_ref.shape
    _, _, own_rows, all_depth, modes = spec_ref.shape
    local_slabs = modes // LANES
    group = own_rows * depth
    slabs = gz * local_slabs
    near = 2 * slabs
    far = 2 * slabs
    taps = index_ref.shape[0]
    lines = rows * depth
    tiles = lines // TILE
    skirt = HALO * depth

    barrier = pltpu.get_barrier_semaphore()
    has_up, has_down = layer < gz - 1, layer > 0
    inner = jnp.logical_and(has_up, has_down)
    per_tile = TILE // depth

    def signal(semaphore, target):
        pl.semaphore_signal(semaphore, inc=1, device_id=target, device_id_type=MESH)

    hub = layer == 0
    column = [{"gz": lax.rem(layer + step, gz)} for step in range(1, gz)]
    beside = [{"gx": lax.rem(me + step, gx)} for step in range(1, gx)] + [ahead["gy"], behind["gy"]]
    for target in column:
        signal(barrier, target)

    @pl.when(hub)
    def _():
        for target in beside:
            signal(barrier, target)

    own_columns = pl.ds(pl.multiple_of(me * cells, LANES), cells)
    loads = [
        pltpu.make_async_copy(source, place, load_sems.at[number])
        for number, (source, place) in enumerate(
            [
                (spec_hbm.at[0], spec_ref.at[0]),
                (spec_hbm.at[1], spec_ref.at[1]),
                (spec_hbm.at[2], spec_ref.at[2]),
                (theta_hbm, theta_ref),
                (index_hbm.at[:, own_columns], index_ref),
                (weight_hbm.at[:, own_columns], weight_ref),
                (twist_hbm, twist_ref),
                (last_hbm, last_ref),
                (sum_hbm, sum_ref),
                (offset_hbm, offset_ref),
                (length_hbm, length_ref),
            ]
        )
    ]
    for load in loads:
        load.start()

    @pl.when(hub)
    def _():
        pl.semaphore_wait(barrier, len(column) + len(beside))
        for target in beside:
            signal(meet_sems.at[0], target)

    @pl.when(jnp.logical_not(hub))
    def _():
        pl.semaphore_wait(barrier, len(column))

    def modes_copy(comp, target):
        return pltpu.make_async_remote_copy(
            src_ref=modes_send.at[comp, target],
            dst_ref=modes_recv.at[comp, layer],
            send_sem=modes_sems.at[0, comp, target],
            recv_sem=modes_sems.at[1, comp, layer],
            device_id={"gz": target},
            device_id_type=MESH,
        )

    def modes_wait(comp, other):
        pltpu.make_async_remote_copy(
            src_ref=modes_send.at[comp, other],
            dst_ref=modes_recv.at[comp, other],
            send_sem=modes_sems.at[0, comp, other],
            recv_sem=modes_sems.at[1, comp, other],
            device_id={"gz": other},
            device_id_type=MESH,
        ).wait()

    def send_modes(comp, distance):
        @pl.when(layer + distance < gz)
        def _():
            modes_copy(comp, layer + distance).start()

        @pl.when(layer >= distance)
        def _():
            modes_copy(comp, layer - distance).start()

    def deep_copy(way, tile):
        part_of = pl.ds(tile * per_tile, per_tile)
        return pltpu.make_async_remote_copy(
            src_ref=theta_hbm.at[part_of],
            dst_ref=(z_back, z_front)[way].at[part_of],
            send_sem=deep_sems.at[0, way, tile],
            recv_sem=deep_sems.at[1, way, tile],
            device_id=(ahead, behind)[way]["gz"],
            device_id_type=MESH,
        )

    def send_near(chosen):
        @pl.when(has_up)
        def _():
            for tile in chosen:
                deep_copy(0, tile).start()

        @pl.when(has_down)
        def _():
            for tile in chosen:
                deep_copy(1, tile).start()

    for comp in range(3):
        loads[comp].wait()
        for slab in range(local_slabs):
            for part_of in range(2):
                for row in range(own_rows):
                    held = spec_ref[comp, part_of, row, :, slab * LANES : (slab + 1) * LANES]
                    at = part_of * group + row * depth
                    for peer in range(gz):
                        modes_send[comp, peer, slab, at : at + depth, :] = held[
                            peer * depth : (peer + 1) * depth
                        ]
        for distance in range(gz - 1, 0, -1):
            send_modes(comp, distance)
    send_near(range(tiles))

    @pl.when(jnp.logical_not(inner))
    def _():
        @pl.when(jnp.logical_not(has_up))
        def _():
            for tile in range(tiles):
                deep_copy(0, tile).start()

        @pl.when(jnp.logical_not(has_down))
        def _():
            for tile in range(tiles):
                deep_copy(1, tile).start()

    def seg_copy(comp, step):
        target = lax.rem(me + step, gx)
        return pltpu.make_async_remote_copy(
            src_ref=seg_send.at[comp, target],
            dst_ref=seg_recv.at[comp, me],
            send_sem=seg_sems.at[0, comp, step - 1],
            recv_sem=seg_sems.at[1, comp, step - 1],
            device_id={"gx": target},
            device_id_type=MESH,
        )

    loads[3].wait()
    for tile in range(tiles):
        at = skirt + tile * TILE
        for half in range(per_tile):
            field[at + half * depth : at + (half + 1) * depth, LANES : LANES + cells] = theta_ref[
                tile * (per_tile) + half
            ]

    mine = pl.ds(skirt, lines)
    middle = pl.ds(LANES, cells)
    faces = [
        pltpu.make_async_remote_copy(
            src_ref=field.at[source],
            dst_ref=field.at[place],
            send_sem=face_sems.at[0, number],
            recv_sem=face_sems.at[1, number],
            device_id=device,
            device_id_type=MESH,
        )
        for number, (source, place, device) in enumerate(
            [
                ((mine, pl.ds(cells, LANES)), (mine, pl.ds(0, LANES)), ahead["gx"]),
                ((mine, pl.ds(LANES, LANES)), (mine, pl.ds(LANES + cells, LANES)), behind["gx"]),
                ((pl.ds(lines, skirt), middle), (pl.ds(0, skirt), middle), ahead["gy"]),
                ((pl.ds(skirt, skirt), middle), (pl.ds(skirt + lines, skirt), middle), behind["gy"]),
            ]
        )
    ]

    for comp in range(3):
        modes_recv[comp, layer] = modes_send[comp, layer]

    loads[4].wait()
    loads[5].wait()
    loads[9].wait()
    loads[10].wait()
    live_count = length_ref[me]
    begin = offset_ref[me] - jnp.minimum(offset_ref[me] // LANES, far - span) * LANES
    counter = lax.broadcasted_iota(jnp.int32, (LANES, LANES), 0).astype(jnp.float32).astype(jnp.bfloat16)
    counters = [counter[step : step + 16] for step in range(0, LANES, 16)]

    def spread(row):
        return jnp.broadcast_to(row, (16, LANES)).astype(jnp.bfloat16)

    def build(chunk, carry):
        columns = pl.ds(pl.multiple_of(chunk * LANES, LANES), LANES)
        index = index_ref[:, columns]
        live = index < live_count
        weight = jnp.where(live, weight_ref[:, columns], 0.0)
        merged = jnp.zeros_like(weight)
        for tap in range(taps):
            merged = merged + jnp.where(index == index[tap : tap + 1], weight[tap : tap + 1], 0.0)
        high, low = split(merged)
        high, low = high.astype(jnp.float32), low.astype(jnp.float32)
        place = jnp.where(live, index + begin, -1)
        owner = (place >> 7).astype(jnp.float32)
        within = (place & (LANES - 1)).astype(jnp.float32)
        tops = [spread(high[tap : tap + 1]) for tap in range(taps)]
        rests = [spread(low[tap : tap + 1]) for tap in range(taps)]
        owners = [spread(owner[tap : tap + 1]) for tap in range(taps)]
        withins = [spread(within[tap : tap + 1]) for tap in range(taps)]

        def slab_of(slab, inner):
            number = jnp.full((16, LANES), slab, jnp.int32).astype(jnp.float32).astype(jnp.bfloat16)
            close = [
                jnp.where(owners[tap] == number, withins[tap], jnp.bfloat16(-1)) for tap in range(taps)
            ]
            for step in range(LANES // 16):
                top = jnp.zeros((16, LANES), jnp.bfloat16)
                rest = jnp.zeros((16, LANES), jnp.bfloat16)
                for tap in range(taps):
                    hit = counters[step] == close[tap]
                    top = jnp.where(hit, tops[tap], top)
                    rest = jnp.where(hit, rests[tap], rest)
                at = pl.ds(pl.multiple_of(slab * LANES + step * 16, 16), 16)
                matrix_top[chunk, at, :] = top
                matrix_rest[chunk, at, :] = rest
            return inner

        return lax.fori_loop(0, span, slab_of, carry)

    chunks = cells // LANES
    step_of = chunks // 8
    early = chunks - 5 * step_of
    first = chunks * 4 // 16
    lax.fori_loop(0, first, build, 0)

    @pl.when(hub)
    def _():
        pl.semaphore_wait(meet_sems.at[0], len(beside))
        for target in column:
            signal(meet_sems.at[1], target)

    lax.fori_loop(first, early, build, 0)

    @pl.when(jnp.logical_not(hub))
    def _():
        pl.semaphore_wait(meet_sems.at[1], 1)

    for face in faces:
        face.start()

    loads[6].wait()
    loads[7].wait()
    last_both = last_ref[...]
    last_top = last_both[:far]
    dims = (((1,), (1,)), ((), ()))

    def twisted(line):
        re, im = mixed[:, line, :], mixed[:, group + line, :]
        pieces = []
        for quarter in range(LANES // near):
            part_of = slice(quarter * near, (quarter + 1) * near)
            cosine, sine = twist_ref[0, part_of, :], twist_ref[1, part_of, :]
            pieces.append(jnp.concatenate([re * cosine - im * sine, re * sine + im * cosine], axis=1))
        return jnp.concatenate(pieces, axis=0)

    def transform(comp, carry):
        lax.fori_loop(early + comp * step_of, early + (comp + 1) * step_of, build, 0)
        for step in range(1, gz):
            modes_wait(comp, lax.rem(layer + step, gz))

        def arrived(k):
            held = modes_recv[comp, k // local_slabs, k % local_slabs]
            return held[:group], held[group:]

        for parity in range(2):
            mixes = fft([rotate(arrived(k), parity * k / near) for k in range(slabs)])
            for x in range(slabs):
                mixed[2 * x + parity, 0:group, :] = mixes[x][0]
                mixed[2 * x + parity, group:, :] = mixes[x][1]
        for pair in range(group // 2):
            turned = jnp.concatenate([twisted(2 * pair), twisted(2 * pair + 1)], axis=0)
            top, rest = split(turned)
            first = lax.dot_general(last_both, top, dims, preferred_element_type=jnp.float32)
            second = lax.dot_general(last_top, rest, dims, preferred_element_type=jnp.float32)
            total = first[:far] + (first[far:] + second)
            velocity[:, 2 * pair, :] = total[:, :LANES]
            velocity[:, 2 * pair + 1, :] = total[:, LANES:]
        for block in range(gx):
            start = jnp.minimum(offset_ref[block] // LANES, far - span)
            seg_send[comp, block] = velocity[pl.ds(start, span)]
        for step in range(1, gx):
            seg_copy(comp, step).start()
        seg_recv[comp, me] = seg_send[comp, me]
        return carry

    lax.fori_loop(0, 3, transform, 0)
    lax.fori_loop(early + 3 * step_of, chunks, build, 0)

    loads[8].wait()
    for tile in range(tiles):
        for half in range(per_tile):
            at = tile * TILE + half * depth
            part[at : at + depth, :] = section_keep * sum_ref[tile * (per_tile) + half]
    for face in faces:
        face.wait()
    width = min(WIDTH, cells)
    wide_width = width + 2 * LANES
    low_half = lax.broadcasted_iota(jnp.int32, (TILE, width), 0) < depth

    def plane(block, carry):
        columns = pl.ds(pl.multiple_of(block * width, LANES), width)
        inner = pl.ds(pl.multiple_of(block * width + LANES, LANES), width)
        around = pl.ds(pl.multiple_of(block * width, LANES), wide_width)
        for tile in range(tiles):
            stack = [field[(tile + step) * TILE : (tile + step + 1) * TILE, inner] for step in range(5)]
            turned = [pltpu.roll(held, depth, 0) for held in stack]
            between = [jnp.where(low_half, turned[step], turned[step + 1]) for step in range(4)]
            behind_y = [between[1], stack[1], between[0], stack[0]]
            ahead_y = [between[2], stack[3], between[3], stack[4]]
            wide = field[skirt + tile * TILE : skirt + (tile + 1) * TILE, around]
            grad_x = jnp.zeros((TILE, width), jnp.float32)
            grad_y = jnp.zeros((TILE, width), jnp.float32)
            partial = 3.0 * center_coeff * stack[2]
            for reach in range(1, 5):
                ahead_x = pltpu.roll(wide, wide_width - reach, 1)[:, LANES : LANES + width]
                behind_x = pltpu.roll(wide, reach, 1)[:, LANES : LANES + width]
                up, down = ahead_y[reach - 1], behind_y[reach - 1]
                grad_x = grad_x + first_coeffs[reach - 1] * (ahead_x - behind_x)
                grad_y = grad_y + first_coeffs[reach - 1] * (up - down)
                partial = partial + second_coeffs[reach - 1] * ((ahead_x + behind_x) + (up + down))
            at = slice(tile * TILE, (tile + 1) * TILE)
            grads[0, at, columns] = grad_x
            grads[1, at, columns] = grad_y
            part[at, columns] = part[at, columns] + (time_step * diffusivity) * partial
        return carry

    lax.fori_loop(0, cells // width, plane, 0)

    for comp in range(3):
        for step in range(1, gx):
            seg_copy(comp, step).wait()
    for comp in range(3):
        for block in range(gx):
            at = (comp * gx + block) * group
            for slab in range(span):
                gathered[at : at + group, slab * LANES : (slab + 1) * LANES] = seg_recv[comp, block, slab]
    total = 3 * lines
    top, rest = split(gathered[...])
    values[0:total, :] = top
    values[total:, :] = rest

    def combine(pair, carry):
        top = jnp.concatenate([matrix_top[2 * pair], matrix_top[2 * pair + 1]], axis=1)
        rest = jnp.concatenate([matrix_rest[2 * pair], matrix_rest[2 * pair + 1]], axis=1)
        first = jnp.dot(values[...], top, preferred_element_type=jnp.float32)
        second = jnp.dot(values[0:total, :], rest, preferred_element_type=jnp.float32)
        moved = first[:total] + (first[total:] + second)
        columns = pl.ds(pl.multiple_of(pair * 2 * LANES, 2 * LANES), 2 * LANES)
        carried = moved[:lines] * grads[0, :, columns] + moved[lines : 2 * lines] * grads[1, :, columns]
        part[:, columns] = part[:, columns] - time_step * carried
        drift[:, columns] = time_step * moved[2 * lines :]
        return carry

    lax.fori_loop(0, cells // (2 * LANES), combine, 0)

    place_of = lax.rem(lax.broadcasted_iota(jnp.int32, (TILE, width), 0), depth)
    for tile in range(tiles):
        for way in range(2):
            deep_copy(way, tile).wait()
        at = slice(tile * TILE, (tile + 1) * TILE)

        def finish(block, carry):
            columns = pl.ds(pl.multiple_of(block * width, LANES), width)
            inner = pl.ds(pl.multiple_of(block * width + LANES, LANES), width)
            own = field[skirt + tile * TILE : skirt + (tile + 1) * TILE, inner]
            back, front = (
                jnp.concatenate([held[tile * per_tile + half, :, columns] for half in range(per_tile)], axis=0)
                for held in (z_back, z_front)
            )
            grad_z = jnp.zeros((TILE, width), jnp.float32)
            partial = jnp.zeros((TILE, width), jnp.float32)
            for reach in range(1, 5):
                up, down = front, back
                if reach < HALO:
                    up = jnp.where(
                        place_of < depth - reach, pltpu.roll(own, TILE - reach, 0), pltpu.roll(front, depth - reach, 0)
                    )
                    down = jnp.where(
                        place_of >= reach, pltpu.roll(own, reach, 0), pltpu.roll(back, depth + reach, 0)
                    )
                grad_z = grad_z + first_coeffs[reach - 1] * (up - down)
                partial = partial + second_coeffs[reach - 1] * (up + down)
            after = (part[at, columns] + (time_step * diffusivity) * partial) - drift[at, columns] * grad_z
            later = own + section_gain * after
            for half in range(per_tile):
                row, piece = tile * (per_tile) + half, slice(half * depth, (half + 1) * depth)
                sum_out[row, :, columns] = after[piece]
                theta_out[row, :, columns] = later[piece]
            return carry

        lax.fori_loop(0, cells // width, finish, 0)


def put(theta_ref, sum_ref, theta_out, sum_out, sems):
    copies = [
        pltpu.make_async_copy(theta_ref, theta_out, sems.at[0]),
        pltpu.make_async_copy(sum_ref, sum_out, sems.at[1]),
    ]
    for copy in copies:
        copy.start()
    for copy in copies:
        copy.wait()


def body(spectrum, theta, section_sum, seg_offset, seg_length, stencil_index, stencil_weight):
    sizes = tuple(lax.axis_size(axis) for axis in ("gx", "gy", "gz"))
    gx, _, gz = sizes
    _, _, own_rows, all_depth, modes = spectrum.shape
    rows, depth, cells = theta.shape
    taps = stencil_index.shape[0]
    assert depth == HALO and rows * depth % TILE == 0 and cells % min(WIDTH, cells) == 0
    group = own_rows * depth
    slabs = gz * modes // LANES
    length = 2 * slabs * LANES
    far = length // LANES
    span = min(3 * length // (2 * gx) // LANES + 1, far)
    k = np.arange(LANES)
    turn = 2 * np.pi * (np.outer(k, k) % length) / length
    twist = np.stack([np.cos(turn), np.sin(turn)]).astype(np.float32)
    turn = 2 * np.pi * (np.outer(np.arange(far), k) % far) / far
    last = np.concatenate([np.cos(turn), -np.sin(turn)], axis=1).astype(np.float32)
    top = last.astype(jnp.bfloat16)
    rest = (last - top.astype(np.float32)).astype(jnp.bfloat16)
    modes_shape = (3, gz, modes // LANES, 2 * group, LANES)
    seg_shape = (3, gx, span, group, LANES)
    lines = rows * depth
    tiles = lines // TILE
    single = jnp.float32
    held = pl.pallas_call(
        functools.partial(section_kernel, sizes, span),
        out_shape=[VMEM(theta.shape, single)] * 2,
        in_specs=[pl.BlockSpec(memory_space=pltpu.HBM)] * 9,
        out_specs=whole_vmem(2),
        scratch_shapes=[
            pltpu.SMEM(seg_offset.shape, jnp.int32),
            pltpu.SMEM(seg_length.shape, jnp.int32),
            VMEM(spectrum.shape, single),
            VMEM(theta.shape, single),
            VMEM(theta.shape, single),
            VMEM((taps, cells), jnp.int32),
            VMEM((taps, cells), single),
            VMEM(twist.shape, single),
            VMEM((2 * far, 2 * LANES), jnp.bfloat16),
            VMEM(modes_shape, single),
            VMEM(modes_shape, single),
            VMEM((2 * slabs, 2 * group, LANES), single),
            VMEM((far, group, LANES), single),
            VMEM(seg_shape, single),
            VMEM(seg_shape, single),
            VMEM((cells // LANES, span * LANES, LANES), jnp.bfloat16),
            VMEM((cells // LANES, span * LANES, LANES), jnp.bfloat16),
            VMEM((3 * lines, span * LANES), single),
            VMEM((6 * lines, span * LANES), jnp.bfloat16),
            VMEM((2, lines, cells), single),
            VMEM((lines, cells), single),
            VMEM((lines, cells), single),
            VMEM((lines + 2 * HALO * depth, cells + 2 * LANES), single),
            VMEM(theta.shape, single),
            VMEM(theta.shape, single),
            pltpu.SemaphoreType.DMA((11,)),
            pltpu.SemaphoreType.DMA((2, 3, gz)),
            pltpu.SemaphoreType.DMA((2, 3, gx - 1)),
            pltpu.SemaphoreType.DMA((2, 4)),
            pltpu.SemaphoreType.DMA((2, 2, tiles)),
            pltpu.SemaphoreType.REGULAR((2,)),
        ],
        compiler_params=pltpu.CompilerParams(
            collective_id=0, has_side_effects=True, vmem_limit_bytes=60 * 1024 * 1024
        ),
        name="section",
    )(
        seg_offset, seg_length, spectrum, theta, section_sum, stencil_index, stencil_weight,
        jnp.asarray(twist), jnp.asarray(np.concatenate([top, rest], axis=0)),
    )
    return tuple(
        pl.pallas_call(
            put,
            out_shape=[jax.ShapeDtypeStruct(theta.shape, single)] * 2,
            in_specs=[pl.BlockSpec(memory_space=pl.ANY)] * 2,
            out_specs=[pl.BlockSpec(memory_space=pltpu.HBM)] * 2,
            scratch_shapes=[pltpu.SemaphoreType.DMA((2,))],
            compiler_params=pltpu.CompilerParams(vmem_limit_bytes=1024 * 1024),
            name="put",
        )(*held)
    )


def solution(mesh):
    placed = (
        P(None, None, ("gy", "gx"), None, "gz"),
        P("gy", "gz", "gx"),
        P("gy", "gz", "gx"),
        P(),
        P(),
        P(),
        P(),
    )
    return jax.shard_map(
        body,
        mesh=mesh,
        in_specs=placed,
        out_specs=(P("gy", "gz", "gx"), P("gy", "gz", "gx")),
        check_vma=False,
    )
```

```python
import functools
import math

import jax
import jax.numpy as jnp
import numpy as np
from jax import lax
from jax.experimental import pallas as pl
from jax.experimental.pallas import tpu as pltpu
from jax.sharding import PartitionSpec as P

MESH = pl.DeviceIdType.MESH
VMEM = pltpu.VMEM
LANES = 128
HALO = 4
TILE = 8
WIDTH = 512

first_coeffs = (0.8, -0.2, 4.0 / 105.0, -1.0 / 280.0)
second_coeffs = (1.6, -0.2, 8.0 / 315.0, -1.0 / 560.0)
center_coeff = -205.0 / 72.0
diffusivity = 0.15
time_step = 0.4
section_keep = -5.0 / 9.0
section_gain = 15.0 / 16.0


def whole_vmem(count):
    return [pl.BlockSpec(memory_space=VMEM)] * count


def rotate(value, turn):
    re, im = value
    cosine, sine = math.cos(2 * math.pi * turn), math.sin(2 * math.pi * turn)
    quarter = turn * 4 % 4
    if quarter == 0:
        return re, im
    if quarter == 1:
        return -im, re
    if quarter == 2:
        return -re, -im
    if quarter == 3:
        return im, -re
    return re * cosine - im * sine, re * sine + im * cosine


def fft(values):
    count = len(values)
    if count == 1:
        return values
    even = fft(values[0::2])
    odd = fft(values[1::2])
    low, high = [], []
    for x in range(count // 2):
        re, im = rotate(odd[x], x / count)
        low.append((even[x][0] + re, even[x][1] + im))
        high.append((even[x][0] - re, even[x][1] - im))
    return low + high


def split(value):
    top = value.astype(jnp.bfloat16)
    return top, (value - top.astype(jnp.float32)).astype(jnp.bfloat16)


def section_kernel(
    sizes, span,
    offset_hbm, length_hbm, spec_hbm, theta_hbm, sum_hbm, index_hbm, weight_hbm, twist_hbm, last_hbm,
    theta_out, sum_out,
    offset_ref, length_ref, spec_ref, theta_ref, sum_ref, index_ref, weight_ref, twist_ref, last_ref,
    modes_send, modes_recv, mixed, velocity, seg_send, seg_recv, matrix_top, matrix_rest, gathered, values,
    grads, part, drift, field, z_back, z_front,
    load_sems, modes_sems, seg_sems, face_sems, deep_sems, meet_sems,
):
    gx, gy, gz = sizes
    here = {axis: lax.axis_index(axis) for axis in ("gx", "gy", "gz")}
    counts = dict(gx=gx, gy=gy, gz=gz)
    ahead = {axis: {axis: lax.rem(here[axis] + 1, counts[axis])} for axis in here}
    behind = {axis: {axis: lax.rem(here[axis] + counts[axis] - 1, counts[axis])} for axis in here}
    me, layer = here["gx"], here["gz"]
    rows, depth, cells = theta_ref.shape
    _, _, own_rows, all_depth, modes = spec_ref.shape
    local_slabs = modes // LANES
    group = own_rows * depth
    slabs = gz * local_slabs
    near = 2 * slabs
    far = 2 * slabs
    taps = index_ref.shape[0]
    lines = rows * depth
    tiles = lines // TILE
    skirt = HALO * depth

    barrier = pltpu.get_barrier_semaphore()
    has_up, has_down = layer < gz - 1, layer > 0
    inner = jnp.logical_and(has_up, has_down)
    per_tile = TILE // depth

    def signal(semaphore, target):
        pl.semaphore_signal(semaphore, inc=1, device_id=target, device_id_type=MESH)

    hub = layer == 0
    column = [{"gz": lax.rem(layer + step, gz)} for step in range(1, gz)]
    beside = [{"gx": lax.rem(me + step, gx)} for step in range(1, gx)] + [ahead["gy"], behind["gy"]]
    for target in column:
        signal(barrier, target)

    @pl.when(hub)
    def _():
        for target in beside:
            signal(barrier, target)

    own_columns = pl.ds(pl.multiple_of(me * cells, LANES), cells)
    loads = [
        pltpu.make_async_copy(source, place, load_sems.at[number])
        for number, (source, place) in enumerate(
            [
                (spec_hbm.at[0], spec_ref.at[0]),
                (spec_hbm.at[1], spec_ref.at[1]),
                (spec_hbm.at[2], spec_ref.at[2]),
                (theta_hbm, theta_ref),
                (index_hbm.at[:, own_columns], index_ref),
                (weight_hbm.at[:, own_columns], weight_ref),
                (twist_hbm, twist_ref),
                (last_hbm, last_ref),
                (sum_hbm, sum_ref),
                (offset_hbm, offset_ref),
                (length_hbm, length_ref),
            ]
        )
    ]
    for load in loads:
        load.start()

    def repack(comp):
        loads[comp].wait()
        for slab in range(local_slabs):
            for part_of in range(2):
                for row in range(own_rows):
                    held = spec_ref[comp, part_of, row, :, slab * LANES : (slab + 1) * LANES]
                    at = part_of * group + row * depth
                    for peer in range(gz):
                        modes_send[comp, peer, slab, at : at + depth, :] = held[
                            peer * depth : (peer + 1) * depth
                        ]

    @pl.when(hub)
    def _():
        pl.semaphore_wait(barrier, len(column) + len(beside))
        for target in beside:
            signal(meet_sems.at[0], target)

    @pl.when(jnp.logical_not(hub))
    def _():
        pl.semaphore_wait(barrier, len(column))

    def modes_copy(comp, target):
        return pltpu.make_async_remote_copy(
            src_ref=modes_send.at[comp, target],
            dst_ref=modes_recv.at[comp, layer],
            send_sem=modes_sems.at[0, comp, target],
            recv_sem=modes_sems.at[1, comp, layer],
            device_id={"gz": target},
            device_id_type=MESH,
        )

    def modes_wait(comp, other):
        pltpu.make_async_remote_copy(
            src_ref=modes_send.at[comp, other],
            dst_ref=modes_recv.at[comp, other],
            send_sem=modes_sems.at[0, comp, other],
            recv_sem=modes_sems.at[1, comp, other],
            device_id={"gz": other},
            device_id_type=MESH,
        ).wait()

    def send_modes(comp, distance):
        @pl.when(layer + distance < gz)
        def _():
            modes_copy(comp, layer + distance).start()

        @pl.when(layer >= distance)
        def _():
            modes_copy(comp, layer - distance).start()

    def deep_copy(way, tile):
        part_of = pl.ds(tile * per_tile, per_tile)
        return pltpu.make_async_remote_copy(
            src_ref=theta_hbm.at[part_of],
            dst_ref=(z_back, z_front)[way].at[part_of],
            send_sem=deep_sems.at[0, way, tile],
            recv_sem=deep_sems.at[1, way, tile],
            device_id=(ahead, behind)[way]["gz"],
            device_id_type=MESH,
        )

    def send_near(chosen):
        @pl.when(has_up)
        def _():
            for tile in chosen:
                deep_copy(0, tile).start()

        @pl.when(jnp.logical_and(has_down, has_up))
        def _():
            for tile in chosen:
                deep_copy(1, tile).start()

        @pl.when(jnp.logical_not(has_up))
        def _():
            for tile in chosen:
                if tile > 0:
                    deep_copy(1, tile).start()

    @pl.when(layer == gz - 1)
    def _():
        deep_copy(1, 0).start()

    for comp in range(3):
        if comp >= 0:
            repack(comp)
        for distance in range(gz - 1, 0, -1):
            send_modes(comp, distance)
    send_near(range(tiles - 1))

    @pl.when(jnp.logical_not(inner))
    def _():
        @pl.when(jnp.logical_not(has_up))
        def _():
            for tile in range(tiles):
                deep_copy(0, tile).start()

        @pl.when(jnp.logical_not(has_down))
        def _():
            for tile in range(tiles):
                deep_copy(1, tile).start()

    send_near(range(tiles - 1, tiles))

    def seg_copy(comp, step):
        target = lax.rem(me + step, gx)
        return pltpu.make_async_remote_copy(
            src_ref=seg_send.at[comp, target],
            dst_ref=seg_recv.at[comp, me],
            send_sem=seg_sems.at[0, comp, step - 1],
            recv_sem=seg_sems.at[1, comp, step - 1],
            device_id={"gx": target},
            device_id_type=MESH,
        )

    loads[3].wait()
    for tile in range(tiles):
        at = skirt + tile * TILE
        for half in range(per_tile):
            field[at + half * depth : at + (half + 1) * depth, LANES : LANES + cells] = theta_ref[
                tile * (per_tile) + half
            ]

    mine = pl.ds(skirt, lines)
    middle = pl.ds(LANES, cells)
    faces = [
        pltpu.make_async_remote_copy(
            src_ref=field.at[source],
            dst_ref=field.at[place],
            send_sem=face_sems.at[0, number],
            recv_sem=face_sems.at[1, number],
            device_id=device,
            device_id_type=MESH,
        )
        for number, (source, place, device) in enumerate(
            [
                ((mine, pl.ds(cells, LANES)), (mine, pl.ds(0, LANES)), ahead["gx"]),
                ((mine, pl.ds(LANES, LANES)), (mine, pl.ds(LANES + cells, LANES)), behind["gx"]),
                ((pl.ds(lines, skirt), middle), (pl.ds(0, skirt), middle), ahead["gy"]),
                ((pl.ds(skirt, skirt), middle), (pl.ds(skirt + lines, skirt), middle), behind["gy"]),
            ]
        )
    ]

    for comp in range(3):
        modes_recv[comp, layer] = modes_send[comp, layer]

    loads[4].wait()
    loads[5].wait()
    loads[9].wait()
    loads[10].wait()
    live_count = length_ref[me]
    begin = offset_ref[me] - jnp.minimum(offset_ref[me] // LANES, far - span) * LANES
    counter = lax.broadcasted_iota(jnp.int32, (LANES, LANES), 0).astype(jnp.float32).astype(jnp.bfloat16)
    counters = [counter[step : step + 16] for step in range(0, LANES, 16)]

    def spread(row):
        return jnp.broadcast_to(row, (16, LANES)).astype(jnp.bfloat16)

    def build(chunk, carry):
        columns = pl.ds(pl.multiple_of(chunk * LANES, LANES), LANES)
        index = index_ref[:, columns]
        live = index < live_count
        weight = jnp.where(live, weight_ref[:, columns], 0.0)
        merged = jnp.zeros_like(weight)
        for tap in range(taps):
            merged = merged + jnp.where(index == index[tap : tap + 1], weight[tap : tap + 1], 0.0)
        high, low = split(merged)
        high, low = high.astype(jnp.float32), low.astype(jnp.float32)
        place = jnp.where(live, index + begin, -1)
        owner = (place >> 7).astype(jnp.float32)
        within = (place & (LANES - 1)).astype(jnp.float32)
        tops = [spread(high[tap : tap + 1]) for tap in range(taps)]
        rests = [spread(low[tap : tap + 1]) for tap in range(taps)]
        owners = [spread(owner[tap : tap + 1]) for tap in range(taps)]
        withins = [spread(within[tap : tap + 1]) for tap in range(taps)]

        def slab_of(slab, inner):
            number = jnp.full((16, LANES), slab, jnp.int32).astype(jnp.float32).astype(jnp.bfloat16)
            close = [
                jnp.where(owners[tap] == number, withins[tap], jnp.bfloat16(-1)) for tap in range(taps)
            ]
            for step in range(LANES // 16):
                top = jnp.zeros((16, LANES), jnp.bfloat16)
                rest = jnp.zeros((16, LANES), jnp.bfloat16)
                for tap in range(taps):
                    hit = counters[step] == close[tap]
                    top = jnp.where(hit, tops[tap], top)
                    rest = jnp.where(hit, rests[tap], rest)
                at = pl.ds(pl.multiple_of(slab * LANES + step * 16, 16), 16)
                matrix_top[chunk, at, :] = top
                matrix_rest[chunk, at, :] = rest
            return inner

        return lax.fori_loop(0, span, slab_of, carry)

    chunks = cells // LANES
    step_of = chunks // 8
    early = chunks - 5 * step_of
    first = chunks * 4 // 16
    lax.fori_loop(0, first, build, 0)

    @pl.when(hub)
    def _():
        pl.semaphore_wait(meet_sems.at[0], len(beside))
        for target in column:
            signal(meet_sems.at[1], target)

    lax.fori_loop(first, early, build, 0)

    @pl.when(jnp.logical_not(hub))
    def _():
        pl.semaphore_wait(meet_sems.at[1], 1)

    for face in faces:
        face.start()

    loads[6].wait()
    loads[7].wait()
    last_both = last_ref[...]
    last_top = last_both[:far]
    dims = (((1,), (1,)), ((), ()))

    def twisted(line):
        re, im = mixed[:, line, :], mixed[:, group + line, :]
        pieces = []
        for quarter in range(LANES // near):
            part_of = slice(quarter * near, (quarter + 1) * near)
            cosine, sine = twist_ref[0, part_of, :], twist_ref[1, part_of, :]
            pieces.append(jnp.concatenate([re * cosine - im * sine, re * sine + im * cosine], axis=1))
        return jnp.concatenate(pieces, axis=0)

    def transform(comp, carry):
        lax.fori_loop(early + comp * step_of, early + (comp + 1) * step_of, build, 0)
        for step in range(1, gz):
            modes_wait(comp, lax.rem(layer + step, gz))

        def arrived(k):
            held = modes_recv[comp, k // local_slabs, k % local_slabs]
            return held[:group], held[group:]

        for parity in range(2):
            mixes = fft([rotate(arrived(k), parity * k / near) for k in range(slabs)])
            for x in range(slabs):
                mixed[2 * x + parity, 0:group, :] = mixes[x][0]
                mixed[2 * x + parity, group:, :] = mixes[x][1]
        for pair in range(group // 2):
            turned = jnp.concatenate([twisted(2 * pair), twisted(2 * pair + 1)], axis=0)
            top, rest = split(turned)
            first = lax.dot_general(last_both, top, dims, preferred_element_type=jnp.float32)
            second = lax.dot_general(last_top, rest, dims, preferred_element_type=jnp.float32)
            total = first[:far] + (first[far:] + second)
            velocity[:, 2 * pair, :] = total[:, :LANES]
            velocity[:, 2 * pair + 1, :] = total[:, LANES:]
        for block in range(gx):
            start = jnp.minimum(offset_ref[block] // LANES, far - span)
            seg_send[comp, block] = velocity[pl.ds(start, span)]
        for step in range(1, gx):
            seg_copy(comp, step).start()
        seg_recv[comp, me] = seg_send[comp, me]
        return carry

    lax.fori_loop(0, 3, transform, 0)
    lax.fori_loop(early + 3 * step_of, chunks, build, 0)

    loads[8].wait()
    for tile in range(tiles):
        for half in range(per_tile):
            at = tile * TILE + half * depth
            part[at : at + depth, :] = section_keep * sum_ref[tile * (per_tile) + half]
    for face in faces:
        face.wait()
    width = min(WIDTH, cells)
    wide_width = width + 2 * LANES
    low_half = lax.broadcasted_iota(jnp.int32, (TILE, width), 0) < depth

    def plane(block, carry):
        columns = pl.ds(pl.multiple_of(block * width, LANES), width)
        inner = pl.ds(pl.multiple_of(block * width + LANES, LANES), width)
        around = pl.ds(pl.multiple_of(block * width, LANES), wide_width)
        for tile in range(tiles):
            stack = [field[(tile + step) * TILE : (tile + step + 1) * TILE, inner] for step in range(5)]
            turned = [pltpu.roll(held, depth, 0) for held in stack]
            between = [jnp.where(low_half, turned[step], turned[step + 1]) for step in range(4)]
            behind_y = [between[1], stack[1], between[0], stack[0]]
            ahead_y = [between[2], stack[3], between[3], stack[4]]
            wide = field[skirt + tile * TILE : skirt + (tile + 1) * TILE, around]
            grad_x = jnp.zeros((TILE, width), jnp.float32)
            grad_y = jnp.zeros((TILE, width), jnp.float32)
            partial = 3.0 * center_coeff * stack[2]
            for reach in range(1, 5):
                ahead_x = pltpu.roll(wide, wide_width - reach, 1)[:, LANES : LANES + width]
                behind_x = pltpu.roll(wide, reach, 1)[:, LANES : LANES + width]
                up, down = ahead_y[reach - 1], behind_y[reach - 1]
                grad_x = grad_x + first_coeffs[reach - 1] * (ahead_x - behind_x)
                grad_y = grad_y + first_coeffs[reach - 1] * (up - down)
                partial = partial + second_coeffs[reach - 1] * ((ahead_x + behind_x) + (up + down))
            at = slice(tile * TILE, (tile + 1) * TILE)
            grads[0, at, columns] = grad_x
            grads[1, at, columns] = grad_y
            part[at, columns] = part[at, columns] + (time_step * diffusivity) * partial
        return carry

    lax.fori_loop(0, cells // width, plane, 0)

    for comp in range(3):
        for step in range(1, gx):
            seg_copy(comp, step).wait()
    for comp in range(3):
        for block in range(gx):
            at = (comp * gx + block) * group
            for slab in range(span):
                gathered[at : at + group, slab * LANES : (slab + 1) * LANES] = seg_recv[comp, block, slab]
    total = 3 * lines
    top, rest = split(gathered[...])
    values[0:total, :] = top
    values[total:, :] = rest

    def combine(pair, carry):
        top = jnp.concatenate([matrix_top[2 * pair], matrix_top[2 * pair + 1]], axis=1)
        rest = jnp.concatenate([matrix_rest[2 * pair], matrix_rest[2 * pair + 1]], axis=1)
        first = jnp.dot(values[...], top, preferred_element_type=jnp.float32)
        second = jnp.dot(values[0:total, :], rest, preferred_element_type=jnp.float32)
        moved = first[:total] + (first[total:] + second)
        columns = pl.ds(pl.multiple_of(pair * 2 * LANES, 2 * LANES), 2 * LANES)
        carried = moved[:lines] * grads[0, :, columns] + moved[lines : 2 * lines] * grads[1, :, columns]
        part[:, columns] = part[:, columns] - time_step * carried
        drift[:, columns] = time_step * moved[2 * lines :]
        return carry

    lax.fori_loop(0, cells // (2 * LANES), combine, 0)

    place_of = lax.rem(lax.broadcasted_iota(jnp.int32, (TILE, width), 0), depth)
    for tile in range(tiles):
        for way in range(2):
            deep_copy(way, tile).wait()
        at = slice(tile * TILE, (tile + 1) * TILE)

        def finish(block, carry):
            columns = pl.ds(pl.multiple_of(block * width, LANES), width)
            inner = pl.ds(pl.multiple_of(block * width + LANES, LANES), width)
            own = field[skirt + tile * TILE : skirt + (tile + 1) * TILE, inner]
            back, front = (
                jnp.concatenate([held[tile * per_tile + half, :, columns] for half in range(per_tile)], axis=0)
                for held in (z_back, z_front)
            )
            grad_z = jnp.zeros((TILE, width), jnp.float32)
            partial = jnp.zeros((TILE, width), jnp.float32)
            for reach in range(1, 5):
                up, down = front, back
                if reach < HALO:
                    up = jnp.where(
                        place_of < depth - reach, pltpu.roll(own, TILE - reach, 0), pltpu.roll(front, depth - reach, 0)
                    )
                    down = jnp.where(
                        place_of >= reach, pltpu.roll(own, reach, 0), pltpu.roll(back, depth + reach, 0)
                    )
                grad_z = grad_z + first_coeffs[reach - 1] * (up - down)
                partial = partial + second_coeffs[reach - 1] * (up + down)
            after = (part[at, columns] + (time_step * diffusivity) * partial) - drift[at, columns] * grad_z
            later = own + section_gain * after
            for half in range(per_tile):
                row, piece = tile * (per_tile) + half, slice(half * depth, (half + 1) * depth)
                sum_out[row, :, columns] = after[piece]
                theta_out[row, :, columns] = later[piece]
            return carry

        lax.fori_loop(0, cells // width, finish, 0)


def put(theta_ref, sum_ref, theta_out, sum_out, sems):
    copies = [
        pltpu.make_async_copy(theta_ref, theta_out, sems.at[0]),
        pltpu.make_async_copy(sum_ref, sum_out, sems.at[1]),
    ]
    for copy in copies:
        copy.start()
    for copy in copies:
        copy.wait()


def body(spectrum, theta, section_sum, seg_offset, seg_length, stencil_index, stencil_weight):
    sizes = tuple(lax.axis_size(axis) for axis in ("gx", "gy", "gz"))
    gx, _, gz = sizes
    _, _, own_rows, all_depth, modes = spectrum.shape
    rows, depth, cells = theta.shape
    taps = stencil_index.shape[0]
    assert depth == HALO and rows * depth % TILE == 0 and cells % min(WIDTH, cells) == 0
    group = own_rows * depth
    slabs = gz * modes // LANES
    length = 2 * slabs * LANES
    far = length // LANES
    span = min(3 * length // (2 * gx) // LANES + 1, far)
    k = np.arange(LANES)
    turn = 2 * np.pi * (np.outer(k, k) % length) / length
    twist = np.stack([np.cos(turn), np.sin(turn)]).astype(np.float32)
    turn = 2 * np.pi * (np.outer(np.arange(far), k) % far) / far
    last = np.concatenate([np.cos(turn), -np.sin(turn)], axis=1).astype(np.float32)
    top = last.astype(jnp.bfloat16)
    rest = (last - top.astype(np.float32)).astype(jnp.bfloat16)
    modes_shape = (3, gz, modes // LANES, 2 * group, LANES)
    seg_shape = (3, gx, span, group, LANES)
    lines = rows * depth
    tiles = lines // TILE
    single = jnp.float32
    held = pl.pallas_call(
        functools.partial(section_kernel, sizes, span),
        out_shape=[VMEM(theta.shape, single)] * 2,
        in_specs=[pl.BlockSpec(memory_space=pltpu.HBM)] * 9,
        out_specs=whole_vmem(2),
        scratch_shapes=[
            pltpu.SMEM(seg_offset.shape, jnp.int32),
            pltpu.SMEM(seg_length.shape, jnp.int32),
            VMEM(spectrum.shape, single),
            VMEM(theta.shape, single),
            VMEM(theta.shape, single),
            VMEM((taps, cells), jnp.int32),
            VMEM((taps, cells), single),
            VMEM(twist.shape, single),
            VMEM((2 * far, 2 * LANES), jnp.bfloat16),
            VMEM(modes_shape, single),
            VMEM(modes_shape, single),
            VMEM((2 * slabs, 2 * group, LANES), single),
            VMEM((far, group, LANES), single),
            VMEM(seg_shape, single),
            VMEM(seg_shape, single),
            VMEM((cells // LANES, span * LANES, LANES), jnp.bfloat16),
            VMEM((cells // LANES, span * LANES, LANES), jnp.bfloat16),
            VMEM((3 * lines, span * LANES), single),
            VMEM((6 * lines, span * LANES), jnp.bfloat16),
            VMEM((2, lines, cells), single),
            VMEM((lines, cells), single),
            VMEM((lines, cells), single),
            VMEM((lines + 2 * HALO * depth, cells + 2 * LANES), single),
            VMEM(theta.shape, single),
            VMEM(theta.shape, single),
            pltpu.SemaphoreType.DMA((11,)),
            pltpu.SemaphoreType.DMA((2, 3, gz)),
            pltpu.SemaphoreType.DMA((2, 3, gx - 1)),
            pltpu.SemaphoreType.DMA((2, 4)),
            pltpu.SemaphoreType.DMA((2, 2, tiles)),
            pltpu.SemaphoreType.REGULAR((2,)),
        ],
        compiler_params=pltpu.CompilerParams(
            collective_id=0, has_side_effects=True, vmem_limit_bytes=60 * 1024 * 1024
        ),
        name="section",
    )(
        seg_offset, seg_length, spectrum, theta, section_sum, stencil_index, stencil_weight,
        jnp.asarray(twist), jnp.asarray(np.concatenate([top, rest], axis=0)),
    )
    return tuple(
        pl.pallas_call(
            put,
            out_shape=[jax.ShapeDtypeStruct(theta.shape, single)] * 2,
            in_specs=[pl.BlockSpec(memory_space=pl.ANY)] * 2,
            out_specs=[pl.BlockSpec(memory_space=pltpu.HBM)] * 2,
            scratch_shapes=[pltpu.SemaphoreType.DMA((2,))],
            compiler_params=pltpu.CompilerParams(vmem_limit_bytes=1024 * 1024),
            name="put",
        )(*held)
    )


def solution(mesh):
    placed = (
        P(None, None, ("gy", "gx"), None, "gz"),
        P("gy", "gz", "gx"),
        P("gy", "gz", "gx"),
        P(),
        P(),
        P(),
        P(),
    )
    return jax.shard_map(
        body,
        mesh=mesh,
        in_specs=placed,
        out_specs=(P("gy", "gz", "gx"), P("gy", "gz", "gx")),
        check_vma=False,
    )
```

```python
import functools
import math

import jax
import jax.numpy as jnp
import numpy as np
from jax import lax
from jax.experimental import pallas as pl
from jax.experimental.pallas import tpu as pltpu
from jax.sharding import PartitionSpec as P

MESH = pl.DeviceIdType.MESH
VMEM = pltpu.VMEM
LANES = 128
HALO = 4
TILE = 8
WIDTH = 1024

first_coeffs = (0.8, -0.2, 4.0 / 105.0, -1.0 / 280.0)
second_coeffs = (1.6, -0.2, 8.0 / 315.0, -1.0 / 560.0)
center_coeff = -205.0 / 72.0
diffusivity = 0.15
time_step = 0.4
section_keep = -5.0 / 9.0
section_gain = 15.0 / 16.0


def whole_vmem(count):
    return [pl.BlockSpec(memory_space=VMEM)] * count


def rotate(value, turn):
    re, im = value
    cosine, sine = math.cos(2 * math.pi * turn), math.sin(2 * math.pi * turn)
    quarter = turn * 4 % 4
    if quarter == 0:
        return re, im
    if quarter == 1:
        return -im, re
    if quarter == 2:
        return -re, -im
    if quarter == 3:
        return im, -re
    return re * cosine - im * sine, re * sine + im * cosine


def fft(values):
    count = len(values)
    if count == 1:
        return values
    even = fft(values[0::2])
    odd = fft(values[1::2])
    low, high = [], []
    for x in range(count // 2):
        re, im = rotate(odd[x], x / count)
        low.append((even[x][0] + re, even[x][1] + im))
        high.append((even[x][0] - re, even[x][1] - im))
    return low + high


def split(value):
    top = value.astype(jnp.bfloat16)
    return top, (value - top.astype(jnp.float32)).astype(jnp.bfloat16)


def section_kernel(
    sizes, span,
    offset_hbm, length_hbm, spec_hbm, theta_hbm, sum_hbm, index_hbm, weight_hbm, twist_hbm, last_hbm,
    theta_out, sum_out,
    offset_ref, length_ref, spec_ref, theta_ref, sum_ref, index_ref, weight_ref, twist_ref, last_ref,
    modes_send, modes_recv, mixed, velocity, seg_send, seg_recv, matrix_top, matrix_rest, gathered, values,
    grads, part, drift, field, z_back, z_front,
    load_sems, modes_sems, seg_sems, face_sems, deep_sems, meet_sems,
):
    gx, gy, gz = sizes
    here = {axis: lax.axis_index(axis) for axis in ("gx", "gy", "gz")}
    counts = dict(gx=gx, gy=gy, gz=gz)
    ahead = {axis: {axis: lax.rem(here[axis] + 1, counts[axis])} for axis in here}
    behind = {axis: {axis: lax.rem(here[axis] + counts[axis] - 1, counts[axis])} for axis in here}
    me, layer = here["gx"], here["gz"]
    rows, depth, cells = theta_ref.shape
    _, _, own_rows, all_depth, modes = spec_ref.shape
    local_slabs = modes // LANES
    group = own_rows * depth
    slabs = gz * local_slabs
    near = 2 * slabs
    far = 2 * slabs
    taps = index_ref.shape[0]
    lines = rows * depth
    tiles = lines // TILE
    skirt = HALO * depth

    barrier = pltpu.get_barrier_semaphore()
    has_up, has_down = layer < gz - 1, layer > 0
    inner = jnp.logical_and(has_up, has_down)
    per_tile = TILE // depth

    def signal(semaphore, target):
        pl.semaphore_signal(semaphore, inc=1, device_id=target, device_id_type=MESH)

    hub = layer == 0
    column = [{"gz": lax.rem(layer + step, gz)} for step in range(1, gz)]
    beside = [{"gx": lax.rem(me + step, gx)} for step in range(1, gx)] + [ahead["gy"], behind["gy"]]
    for target in column:
        signal(barrier, target)

    @pl.when(hub)
    def _():
        for target in beside:
            signal(barrier, target)

    own_columns = pl.ds(pl.multiple_of(me * cells, LANES), cells)
    loads = [
        pltpu.make_async_copy(source, place, load_sems.at[number])
        for number, (source, place) in enumerate(
            [
                (spec_hbm.at[0], spec_ref.at[0]),
                (spec_hbm.at[1], spec_ref.at[1]),
                (spec_hbm.at[2], spec_ref.at[2]),
                (theta_hbm, theta_ref),
                (index_hbm.at[:, own_columns], index_ref),
                (weight_hbm.at[:, own_columns], weight_ref),
                (twist_hbm, twist_ref),
                (last_hbm, last_ref),
                (sum_hbm, sum_ref),
                (offset_hbm, offset_ref),
                (length_hbm, length_ref),
            ]
        )
    ]
    for load in loads:
        load.start()

    def repack(comp):
        loads[comp].wait()
        for slab in range(local_slabs):
            for part_of in range(2):
                for row in range(own_rows):
                    held = spec_ref[comp, part_of, row, :, slab * LANES : (slab + 1) * LANES]
                    at = part_of * group + row * depth
                    for peer in range(gz):
                        modes_send[comp, peer, slab, at : at + depth, :] = held[
                            peer * depth : (peer + 1) * depth
                        ]

    @pl.when(hub)
    def _():
        pl.semaphore_wait(barrier, len(column) + len(beside))
        for target in beside:
            signal(meet_sems.at[0], target)

    @pl.when(jnp.logical_not(hub))
    def _():
        pl.semaphore_wait(barrier, len(column))

    def modes_copy(comp, target):
        return pltpu.make_async_remote_copy(
            src_ref=modes_send.at[comp, target],
            dst_ref=modes_recv.at[comp, layer],
            send_sem=modes_sems.at[0, comp, target],
            recv_sem=modes_sems.at[1, comp, layer],
            device_id={"gz": target},
            device_id_type=MESH,
        )

    def modes_wait(comp, other):
        pltpu.make_async_remote_copy(
            src_ref=modes_send.at[comp, other],
            dst_ref=modes_recv.at[comp, other],
            send_sem=modes_sems.at[0, comp, other],
            recv_sem=modes_sems.at[1, comp, other],
            device_id={"gz": other},
            device_id_type=MESH,
        ).wait()

    def send_modes(comp, distance):
        @pl.when(layer + distance < gz)
        def _():
            modes_copy(comp, layer + distance).start()

        @pl.when(layer >= distance)
        def _():
            modes_copy(comp, layer - distance).start()

    def deep_copy(way, tile):
        part_of = pl.ds(tile * per_tile, per_tile)
        return pltpu.make_async_remote_copy(
            src_ref=theta_hbm.at[part_of],
            dst_ref=(z_back, z_front)[way].at[part_of],
            send_sem=deep_sems.at[0, way, tile],
            recv_sem=deep_sems.at[1, way, tile],
            device_id=(ahead, behind)[way]["gz"],
            device_id_type=MESH,
        )

    def send_near(chosen):
        @pl.when(has_up)
        def _():
            for tile in chosen:
                deep_copy(0, tile).start()

        @pl.when(jnp.logical_and(has_down, has_up))
        def _():
            for tile in chosen:
                deep_copy(1, tile).start()

        @pl.when(jnp.logical_not(has_up))
        def _():
            for tile in chosen:
                if tile > 0:
                    deep_copy(1, tile).start()

    @pl.when(layer == gz - 1)
    def _():
        deep_copy(1, 0).start()

    for comp in range(3):
        if comp >= 0:
            repack(comp)
        for distance in range(gz - 1, 0, -1):
            send_modes(comp, distance)
    send_near(range(tiles - 1))

    @pl.when(jnp.logical_not(inner))
    def _():
        @pl.when(jnp.logical_not(has_up))
        def _():
            for tile in range(tiles):
                deep_copy(0, tile).start()

        @pl.when(jnp.logical_not(has_down))
        def _():
            for tile in range(tiles):
                deep_copy(1, tile).start()

    send_near(range(tiles - 1, tiles))

    def seg_copy(comp, step):
        target = lax.rem(me + step, gx)
        return pltpu.make_async_remote_copy(
            src_ref=seg_send.at[comp, target],
            dst_ref=seg_recv.at[comp, me],
            send_sem=seg_sems.at[0, comp, step - 1],
            recv_sem=seg_sems.at[1, comp, step - 1],
            device_id={"gx": target},
            device_id_type=MESH,
        )

    loads[3].wait()
    for tile in range(tiles):
        at = skirt + tile * TILE
        for half in range(per_tile):
            field[at + half * depth : at + (half + 1) * depth, LANES : LANES + cells] = theta_ref[
                tile * (per_tile) + half
            ]

    mine = pl.ds(skirt, lines)
    middle = pl.ds(LANES, cells)
    faces = [
        pltpu.make_async_remote_copy(
            src_ref=field.at[source],
            dst_ref=field.at[place],
            send_sem=face_sems.at[0, number],
            recv_sem=face_sems.at[1, number],
            device_id=device,
            device_id_type=MESH,
        )
        for number, (source, place, device) in enumerate(
            [
                ((mine, pl.ds(cells, LANES)), (mine, pl.ds(0, LANES)), ahead["gx"]),
                ((mine, pl.ds(LANES, LANES)), (mine, pl.ds(LANES + cells, LANES)), behind["gx"]),
                ((pl.ds(lines, skirt), middle), (pl.ds(0, skirt), middle), ahead["gy"]),
                ((pl.ds(skirt, skirt), middle), (pl.ds(skirt + lines, skirt), middle), behind["gy"]),
            ]
        )
    ]

    for comp in range(3):
        modes_recv[comp, layer] = modes_send[comp, layer]

    loads[4].wait()
    loads[5].wait()
    loads[9].wait()
    loads[10].wait()
    live_count = length_ref[me]
    begin = offset_ref[me] - jnp.minimum(offset_ref[me] // LANES, far - span) * LANES
    counter = lax.broadcasted_iota(jnp.int32, (LANES, LANES), 0).astype(jnp.float32).astype(jnp.bfloat16)
    counters = [counter[step : step + 16] for step in range(0, LANES, 16)]

    def spread(row):
        return jnp.broadcast_to(row, (16, LANES)).astype(jnp.bfloat16)

    def build(chunk, carry):
        columns = pl.ds(pl.multiple_of(chunk * LANES, LANES), LANES)
        index = index_ref[:, columns]
        live = index < live_count
        weight = jnp.where(live, weight_ref[:, columns], 0.0)
        merged = jnp.zeros_like(weight)
        for tap in range(taps):
            merged = merged + jnp.where(index == index[tap : tap + 1], weight[tap : tap + 1], 0.0)
        high, low = split(merged)
        high, low = high.astype(jnp.float32), low.astype(jnp.float32)
        place = jnp.where(live, index + begin, -1)
        owner = (place >> 7).astype(jnp.float32)
        within = (place & (LANES - 1)).astype(jnp.float32)
        tops = [spread(high[tap : tap + 1]) for tap in range(taps)]
        rests = [spread(low[tap : tap + 1]) for tap in range(taps)]
        owners = [spread(owner[tap : tap + 1]) for tap in range(taps)]
        withins = [spread(within[tap : tap + 1]) for tap in range(taps)]

        def slab_of(slab, inner):
            number = jnp.full((16, LANES), slab, jnp.int32).astype(jnp.float32).astype(jnp.bfloat16)
            close = [
                jnp.where(owners[tap] == number, withins[tap], jnp.bfloat16(-1)) for tap in range(taps)
            ]
            for step in range(LANES // 16):
                top = jnp.zeros((16, LANES), jnp.bfloat16)
                rest = jnp.zeros((16, LANES), jnp.bfloat16)
                for tap in range(taps):
                    hit = counters[step] == close[tap]
                    top = jnp.where(hit, tops[tap], top)
                    rest = jnp.where(hit, rests[tap], rest)
                at = pl.ds(pl.multiple_of(slab * LANES + step * 16, 16), 16)
                matrix_top[chunk, at, :] = top
                matrix_rest[chunk, at, :] = rest
            return inner

        return lax.fori_loop(0, span, slab_of, carry)

    chunks = cells // LANES
    step_of = chunks // 8
    early = chunks - 5 * step_of
    first = chunks * 4 // 16
    lax.fori_loop(0, first, build, 0)

    @pl.when(hub)
    def _():
        pl.semaphore_wait(meet_sems.at[0], len(beside))
        for target in column:
            signal(meet_sems.at[1], target)

    lax.fori_loop(first, early, build, 0)

    @pl.when(jnp.logical_not(hub))
    def _():
        pl.semaphore_wait(meet_sems.at[1], 1)

    for face in faces:
        face.start()

    loads[6].wait()
    loads[7].wait()
    last_both = last_ref[...]
    last_top = last_both[:far]
    dims = (((1,), (1,)), ((), ()))

    def twisted(line):
        re, im = mixed[:, line, :], mixed[:, group + line, :]
        pieces = []
        for quarter in range(LANES // near):
            part_of = slice(quarter * near, (quarter + 1) * near)
            cosine, sine = twist_ref[0, part_of, :], twist_ref[1, part_of, :]
            pieces.append(jnp.concatenate([re * cosine - im * sine, re * sine + im * cosine], axis=1))
        return jnp.concatenate(pieces, axis=0)

    def transform(comp, carry):
        lax.fori_loop(early + comp * step_of, early + (comp + 1) * step_of, build, 0)
        for step in range(1, gz):
            modes_wait(comp, lax.rem(layer + step, gz))

        def arrived(k):
            held = modes_recv[comp, k // local_slabs, k % local_slabs]
            return held[:group], held[group:]

        for parity in range(2):
            mixes = fft([rotate(arrived(k), parity * k / near) for k in range(slabs)])
            for x in range(slabs):
                mixed[2 * x + parity, 0:group, :] = mixes[x][0]
                mixed[2 * x + parity, group:, :] = mixes[x][1]
        for pair in range(group // 2):
            turned = jnp.concatenate([twisted(2 * pair), twisted(2 * pair + 1)], axis=0)
            top, rest = split(turned)
            first = lax.dot_general(last_both, top, dims, preferred_element_type=jnp.float32)
            second = lax.dot_general(last_top, rest, dims, preferred_element_type=jnp.float32)
            total = first[:far] + (first[far:] + second)
            velocity[:, 2 * pair, :] = total[:, :LANES]
            velocity[:, 2 * pair + 1, :] = total[:, LANES:]
        for block in range(gx):
            start = jnp.minimum(offset_ref[block] // LANES, far - span)
            seg_send[comp, block] = velocity[pl.ds(start, span)]
        for step in range(1, gx):
            seg_copy(comp, step).start()
        seg_recv[comp, me] = seg_send[comp, me]
        return carry

    lax.fori_loop(0, 3, transform, 0)
    lax.fori_loop(early + 3 * step_of, chunks, build, 0)

    loads[8].wait()
    for tile in range(tiles):
        for half in range(per_tile):
            at = tile * TILE + half * depth
            part[at : at + depth, :] = section_keep * sum_ref[tile * (per_tile) + half]
    for face in faces:
        face.wait()
    width = min(WIDTH, cells)
    wide_width = width + 2 * LANES
    low_half = lax.broadcasted_iota(jnp.int32, (TILE, width), 0) < depth

    def plane(block, carry):
        columns = pl.ds(pl.multiple_of(block * width, LANES), width)
        inner = pl.ds(pl.multiple_of(block * width + LANES, LANES), width)
        around = pl.ds(pl.multiple_of(block * width, LANES), wide_width)
        for tile in range(tiles):
            stack = [field[(tile + step) * TILE : (tile + step + 1) * TILE, inner] for step in range(5)]
            turned = [pltpu.roll(held, depth, 0) for held in stack]
            between = [jnp.where(low_half, turned[step], turned[step + 1]) for step in range(4)]
            behind_y = [between[1], stack[1], between[0], stack[0]]
            ahead_y = [between[2], stack[3], between[3], stack[4]]
            wide = field[skirt + tile * TILE : skirt + (tile + 1) * TILE, around]
            grad_x = jnp.zeros((TILE, width), jnp.float32)
            grad_y = jnp.zeros((TILE, width), jnp.float32)
            partial = 3.0 * center_coeff * stack[2]
            for reach in range(1, 5):
                ahead_x = pltpu.roll(wide, wide_width - reach, 1)[:, LANES : LANES + width]
                behind_x = pltpu.roll(wide, reach, 1)[:, LANES : LANES + width]
                up, down = ahead_y[reach - 1], behind_y[reach - 1]
                grad_x = grad_x + first_coeffs[reach - 1] * (ahead_x - behind_x)
                grad_y = grad_y + first_coeffs[reach - 1] * (up - down)
                partial = partial + second_coeffs[reach - 1] * ((ahead_x + behind_x) + (up + down))
            at = slice(tile * TILE, (tile + 1) * TILE)
            grads[0, at, columns] = grad_x
            grads[1, at, columns] = grad_y
            part[at, columns] = part[at, columns] + (time_step * diffusivity) * partial
        return carry

    lax.fori_loop(0, cells // width, plane, 0)

    for comp in range(3):
        for step in range(1, gx):
            seg_copy(comp, step).wait()
    for comp in range(3):
        for block in range(gx):
            at = (comp * gx + block) * group
            for slab in range(span):
                gathered[at : at + group, slab * LANES : (slab + 1) * LANES] = seg_recv[comp, block, slab]
    total = 3 * lines
    top, rest = split(gathered[...])
    values[0:total, :] = top
    values[total:, :] = rest

    def combine(pair, carry):
        top = jnp.concatenate([matrix_top[2 * pair], matrix_top[2 * pair + 1]], axis=1)
        rest = jnp.concatenate([matrix_rest[2 * pair], matrix_rest[2 * pair + 1]], axis=1)
        first = jnp.dot(values[...], top, preferred_element_type=jnp.float32)
        second = jnp.dot(values[0:total, :], rest, preferred_element_type=jnp.float32)
        moved = first[:total] + (first[total:] + second)
        columns = pl.ds(pl.multiple_of(pair * 2 * LANES, 2 * LANES), 2 * LANES)
        carried = moved[:lines] * grads[0, :, columns] + moved[lines : 2 * lines] * grads[1, :, columns]
        part[:, columns] = part[:, columns] - time_step * carried
        drift[:, columns] = time_step * moved[2 * lines :]
        return carry

    lax.fori_loop(0, cells // (2 * LANES), combine, 0)

    place_of = lax.rem(lax.broadcasted_iota(jnp.int32, (TILE, width), 0), depth)
    for tile in range(tiles):
        for way in range(2):
            deep_copy(way, tile).wait()
        at = slice(tile * TILE, (tile + 1) * TILE)

        def finish(block, carry):
            columns = pl.ds(pl.multiple_of(block * width, LANES), width)
            inner = pl.ds(pl.multiple_of(block * width + LANES, LANES), width)
            own = field[skirt + tile * TILE : skirt + (tile + 1) * TILE, inner]
            back, front = (
                jnp.concatenate([held[tile * per_tile + half, :, columns] for half in range(per_tile)], axis=0)
                for held in (z_back, z_front)
            )
            grad_z = jnp.zeros((TILE, width), jnp.float32)
            partial = jnp.zeros((TILE, width), jnp.float32)
            for reach in range(1, 5):
                up, down = front, back
                if reach < HALO:
                    up = jnp.where(
                        place_of < depth - reach, pltpu.roll(own, TILE - reach, 0), pltpu.roll(front, depth - reach, 0)
                    )
                    down = jnp.where(
                        place_of >= reach, pltpu.roll(own, reach, 0), pltpu.roll(back, depth + reach, 0)
                    )
                grad_z = grad_z + first_coeffs[reach - 1] * (up - down)
                partial = partial + second_coeffs[reach - 1] * (up + down)
            after = (part[at, columns] + (time_step * diffusivity) * partial) - drift[at, columns] * grad_z
            later = own + section_gain * after
            for half in range(per_tile):
                row, piece = tile * (per_tile) + half, slice(half * depth, (half + 1) * depth)
                sum_out[row, :, columns] = after[piece]
                theta_out[row, :, columns] = later[piece]
            return carry

        lax.fori_loop(0, cells // width, finish, 0)


def put(theta_ref, sum_ref, theta_out, sum_out, sems):
    copies = [
        pltpu.make_async_copy(theta_ref, theta_out, sems.at[0]),
        pltpu.make_async_copy(sum_ref, sum_out, sems.at[1]),
    ]
    for copy in copies:
        copy.start()
    for copy in copies:
        copy.wait()


def body(spectrum, theta, section_sum, seg_offset, seg_length, stencil_index, stencil_weight):
    sizes = tuple(lax.axis_size(axis) for axis in ("gx", "gy", "gz"))
    gx, _, gz = sizes
    _, _, own_rows, all_depth, modes = spectrum.shape
    rows, depth, cells = theta.shape
    taps = stencil_index.shape[0]
    assert depth == HALO and rows * depth % TILE == 0 and cells % min(WIDTH, cells) == 0
    group = own_rows * depth
    slabs = gz * modes // LANES
    length = 2 * slabs * LANES
    far = length // LANES
    span = min(3 * length // (2 * gx) // LANES + 1, far)
    k = np.arange(LANES)
    turn = 2 * np.pi * (np.outer(k, k) % length) / length
    twist = np.stack([np.cos(turn), np.sin(turn)]).astype(np.float32)
    turn = 2 * np.pi * (np.outer(np.arange(far), k) % far) / far
    last = np.concatenate([np.cos(turn), -np.sin(turn)], axis=1).astype(np.float32)
    top = last.astype(jnp.bfloat16)
    rest = (last - top.astype(np.float32)).astype(jnp.bfloat16)
    modes_shape = (3, gz, modes // LANES, 2 * group, LANES)
    seg_shape = (3, gx, span, group, LANES)
    lines = rows * depth
    tiles = lines // TILE
    single = jnp.float32
    held = pl.pallas_call(
        functools.partial(section_kernel, sizes, span),
        out_shape=[VMEM(theta.shape, single)] * 2,
        in_specs=[pl.BlockSpec(memory_space=pltpu.HBM)] * 9,
        out_specs=whole_vmem(2),
        scratch_shapes=[
            pltpu.SMEM(seg_offset.shape, jnp.int32),
            pltpu.SMEM(seg_length.shape, jnp.int32),
            VMEM(spectrum.shape, single),
            VMEM(theta.shape, single),
            VMEM(theta.shape, single),
            VMEM((taps, cells), jnp.int32),
            VMEM((taps, cells), single),
            VMEM(twist.shape, single),
            VMEM((2 * far, 2 * LANES), jnp.bfloat16),
            VMEM(modes_shape, single),
            VMEM(modes_shape, single),
            VMEM((2 * slabs, 2 * group, LANES), single),
            VMEM((far, group, LANES), single),
            VMEM(seg_shape, single),
            VMEM(seg_shape, single),
            VMEM((cells // LANES, span * LANES, LANES), jnp.bfloat16),
            VMEM((cells // LANES, span * LANES, LANES), jnp.bfloat16),
            VMEM((3 * lines, span * LANES), single),
            VMEM((6 * lines, span * LANES), jnp.bfloat16),
            VMEM((2, lines, cells), single),
            VMEM((lines, cells), single),
            VMEM((lines, cells), single),
            VMEM((lines + 2 * HALO * depth, cells + 2 * LANES), single),
            VMEM(theta.shape, single),
            VMEM(theta.shape, single),
            pltpu.SemaphoreType.DMA((11,)),
            pltpu.SemaphoreType.DMA((2, 3, gz)),
            pltpu.SemaphoreType.DMA((2, 3, gx - 1)),
            pltpu.SemaphoreType.DMA((2, 4)),
            pltpu.SemaphoreType.DMA((2, 2, tiles)),
            pltpu.SemaphoreType.REGULAR((2,)),
        ],
        compiler_params=pltpu.CompilerParams(
            collective_id=0, has_side_effects=True, vmem_limit_bytes=60 * 1024 * 1024
        ),
        name="section",
    )(
        seg_offset, seg_length, spectrum, theta, section_sum, stencil_index, stencil_weight,
        jnp.asarray(twist), jnp.asarray(np.concatenate([top, rest], axis=0)),
    )
    return tuple(
        pl.pallas_call(
            put,
            out_shape=[jax.ShapeDtypeStruct(theta.shape, single)] * 2,
            in_specs=[pl.BlockSpec(memory_space=pl.ANY)] * 2,
            out_specs=[pl.BlockSpec(memory_space=pltpu.HBM)] * 2,
            scratch_shapes=[pltpu.SemaphoreType.DMA((2,))],
            compiler_params=pltpu.CompilerParams(vmem_limit_bytes=1024 * 1024),
            name="put",
        )(*held)
    )


def solution(mesh):
    placed = (
        P(None, None, ("gy", "gx"), None, "gz"),
        P("gy", "gz", "gx"),
        P("gy", "gz", "gx"),
        P(),
        P(),
        P(),
        P(),
    )
    return jax.shard_map(
        body,
        mesh=mesh,
        in_specs=placed,
        out_specs=(P("gy", "gz", "gx"), P("gy", "gz", "gx")),
        check_vma=False,
    )
```
